256 devices in a mesh: seq: 32 (over x_hi, z, core), zero: 8 (over x_lo, y).
Axes of the slice: x: 4 (x_hi: 2, x_lo: 2; x = x_hi * 2 + x_lo), y: 4, z: 8, core: 2. Of those that a mesh axis runs over, the one named last changes fastest.
Arguments:
- tokens: bfloat16 [8, 4096, 2048], P('zero', 'seq'), may hold values from -6 to 6
- w_in: bfloat16 [2048, 2336], P('zero'), may hold values from -0.0625 to 0.0625
- a_log: float32 [32], replicated, may hold values from -8 to 0
- dt_bias: float32 [32], replicated, may hold values from -4.5 to -3.5
- d_skip: float32 [32], replicated, may hold values from 0.5 to 1.5
- grad_y: bfloat16 [8, 4096, 2048], P('zero', 'seq'), may hold values from -6 to 6
Outputs:
- y_out: bfloat16 [8, 4096, 2048], P('zero', 'seq')
- grad_tokens: bfloat16 [8, 4096, 2048], P('zero', 'seq')
- grad_w: float32 [2048, 2336], P(('seq', 'zero'))
The draws below stay inside these ranges and needn't reach their ends.
All inputs are finite; a program needn't handle non-finite values.
Results may differ from the reference program's by a relative error of at most 0.013.
Values may be sent and summed in bfloat16 or wider, within the bound.
A program may use at most 128 MiB of HBM per device.

```python
import jax
import jax.numpy as jnp
from jax import lax

D = 2048
STATE = 128
HEADS = 32
HEAD_SIZE = 64
TOK_DEV = 128
INNER = 2048
PROJ = 2336
BATCH = 8
LENGTH = 4096
N_SEQ = 32


def block_scale(own_key, extent, shards, least, top_value):
    level, own = 1.0, jax.random.fold_in(own_key, 6)
    for axis_at, shards_of in shards:
        draws = jnp.exp(jax.random.uniform(jax.random.fold_in(own, axis_at), (shards_of,), jnp.float32, least / len(shards), top_value / len(shards)))
        level = level * jnp.repeat(draws, extent[axis_at] // shards_of).reshape([-1 if axis == axis_at else 1 for axis in range(len(extent))])
    return level


def noise(own_key, shape, scale, reach, cuts=(), kind=jnp.bfloat16):
    gain = block_scale(own_key, shape, cuts, -0.22, 0.18) if cuts else 1.0
    result = jax.random.normal(own_key, shape, jnp.float32) * scale * gain
    return jnp.minimum(jnp.maximum(result, -reach), reach).astype(kind)


def setup_inputs(seed: int = 0) -> dict:
    keys = jax.random.split(jax.random.key(seed), 7)
    return {
        "tokens": noise(keys[0], (BATCH, LENGTH, D), 1.0, 6.0, ((0, 8), (1, 32))),
        "w_in": noise(keys[1], (D, PROJ), (4 * D) ** -0.5, 0.0625, ((0, 8),)),
        "a_log": jnp.clip(jax.random.uniform(keys[2], (HEADS,), jnp.float32, -8.0, 0.0), -8.0, 0.0),
        "dt_bias": jnp.clip(jax.random.uniform(keys[3], (HEADS,), jnp.float32, -4.5, -3.5), -4.5, -3.5),
        "d_skip": jnp.clip(jax.random.uniform(keys[4], (HEADS,), jnp.float32, 0.5, 1.5), 0.5, 1.5),
        "grad_y": noise(keys[5], (BATCH, LENGTH, INNER), 1.0, 6.0, ((0, 8), (1, 32))),
    }


def block_ssd(xs, bm, cm, raw, start, a_log, dt_bias, d_skip):
    high = lax.Precision.HIGHEST
    dt = jax.nn.softplus(raw + dt_bias)
    loga = -jnp.exp(a_log) * dt
    cum = jnp.cumsum(loga, axis=0)
    count = xs.shape[0]
    later = (jnp.arange(count)[:, None] >= jnp.arange(count)[None, :])[:, :, None]
    spans = cum[:, None, :] - cum[None, :, :]
    decay = jnp.where(later, jnp.exp(jnp.where(later, spans, 0.0)), 0.0)
    scores = jnp.dot(cm, bm.T, precision=high)
    mixing = scores[:, :, None] * decay * dt[None, :, :]
    ssd = jnp.einsum('tsh,shp->thp', mixing, xs, precision=high)
    ssd = ssd + jnp.einsum('tn,th,hpn->thp', cm, jnp.exp(cum), start, precision=high)
    out = ssd + d_skip[None, :, None] * xs
    tail = jnp.exp(cum[-1:] - cum) * dt
    state = jnp.exp(cum[-1])[:, None, None] * start + jnp.einsum('sh,sn,shp->hpn', tail, bm, xs, precision=high)
    return (out, state)

def reference(tokens, w_in, a_log, dt_bias, d_skip, grad_y):
    proj = jnp.dot(tokens.reshape(BATCH * LENGTH, D), w_in, preferred_element_type=jnp.float32)
    proj = proj.reshape(BATCH, LENGTH, PROJ)
    xs = lax.optimization_barrier(proj[:, :, :INNER].astype(jnp.bfloat16)).astype(jnp.float32)
    bm = lax.optimization_barrier(proj[:, :, INNER:INNER + STATE].astype(jnp.bfloat16)).astype(jnp.float32)
    cm = lax.optimization_barrier(proj[:, :, INNER + STATE:INNER + 2 * STATE].astype(jnp.bfloat16)).astype(jnp.float32)
    raw = proj[:, :, INNER + 2 * STATE:]
    blocks = LENGTH // TOK_DEV

    def forward(xseq, bseq, cseq, rseq):
        xb = xseq.reshape(blocks, TOK_DEV, HEADS, HEAD_SIZE)
        bb = bseq.reshape(blocks, TOK_DEV, STATE)
        cb = cseq.reshape(blocks, TOK_DEV, STATE)
        rb = rseq.reshape(blocks, TOK_DEV, HEADS)

        def step(carry, item):
            out, state = block_ssd(item[0], item[1], item[2], item[3], carry, a_log, dt_bias, d_skip)
            return (state, out)
        initial = jnp.zeros((HEADS, HEAD_SIZE, STATE), jnp.float32)
        final, outs = lax.scan(step, initial, (xb, bb, cb, rb))
        return outs.reshape(LENGTH, INNER)

    def one_sequence(item):
        xseq, bseq, cseq, rseq, gseq = item
        out, pullback = jax.vjp(forward, xseq, bseq, cseq, rseq)
        gx, gb, gc, gr = pullback(gseq.astype(jnp.float32))
        return (out, jnp.concatenate([gx, gb, gc, gr], axis=1))
    outs, grads = lax.map(one_sequence, (xs, bm, cm, raw, grad_y))
    y_out = outs.astype(jnp.bfloat16)
    gproj = grads.astype(jnp.bfloat16)
    grad_tokens = jnp.dot(gproj.reshape(BATCH * LENGTH, PROJ), w_in.T, preferred_element_type=jnp.float32)
    grad_tokens = grad_tokens.astype(jnp.bfloat16).reshape(BATCH, LENGTH, D)
    ublocks = tokens.reshape(BATCH * N_SEQ, TOK_DEV, D)
    gblocks = gproj.reshape(BATCH * N_SEQ, TOK_DEV, PROJ)

    def add_part(total, item):
        part = jnp.dot(item[0].T, item[1], preferred_element_type=jnp.float32)
        part = lax.optimization_barrier(part.astype(jnp.bfloat16)).astype(jnp.float32)
        return (total + part, None)
    grad_w, unused = lax.scan(add_part, jnp.zeros((D, PROJ), jnp.float32), (ublocks, gblocks))
    return (y_out, grad_tokens, grad_w)
```

```python
import jax
import jax.numpy as jnp
from jax import lax
from jax.experimental import pallas as pl
from jax.experimental.pallas import tpu as pltpu
from jax.sharding import Mesh
from jax.sharding import PartitionSpec as P

SEQ = ("xh", "z", "c")
ZERO = ("xl", "y")
MESH = pl.DeviceIdType.MESH
F32 = jnp.float32
BF16 = jnp.bfloat16
LIMIT = 60 * 1024 * 1024
VM = pl.BlockSpec(memory_space=pltpu.VMEM)
ANY = pl.BlockSpec(memory_space=pl.ANY)


def remote(src, dst, send, recv, target):
    return pltpu.make_async_remote_copy(
        src_ref=src, dst_ref=dst, send_sem=send, recv_sem=recv, device_id=target, device_id_type=MESH
    )


def greet(targets):
    barrier = pltpu.get_barrier_semaphore()
    for target in targets:
        pl.semaphore_signal(barrier, inc=1, device_id=target, device_id_type=MESH)
    pl.semaphore_wait(barrier, len(targets))


def place():
    return tuple(lax.axis_index(a) for a in ("xh", "z", "c", "xl", "y"))


def along_x(x):
    return {"xh": x // 2, "xl": x % 2}


def dot(a, b, precision=None):
    return jnp.dot(a, b, preferred_element_type=F32, precision=precision)


def dot_nt(a, b):
    return lax.dot_general(a, b, (((1,), (1,)), ((), ())), preferred_element_type=F32)


def gather_kernel(tok, w, x_o, bc_o, raw_o, wf_o, t1_o, t2_o, wbuf, acc, tt, tb, tr, ici_s, ici_r, d2d_s, d2d_r, tok_sem, hbm_sem, own_sem):
    xh, z, c, xl, y = place()
    x = xh * 2 + xl
    right, left = along_x((x + 1) % 4), along_x((x + 3) % 4)
    up, down = {"y": (y + 1) % 4}, {"y": (y + 3) % 4}
    mate = {"c": 1 - c}
    greet((mate, right, left, up, down))
    inner = x_o.shape[1]
    depth = w.shape[0]
    piece = depth // 4
    sends = []

    def shard(flip, dy):
        return (xl + flip) % 2 * 4 + (y + dy) % 4

    rel = [shard(0, 3), shard(0, 1), shard(0, 2), shard(1, 0), shard(1, 3), shard(1, 1), shard(1, 2)]
    mine = shard(0, 0)

    def rows(core, part):
        return pl.ds(pl.multiple_of((core * 2 + part) * piece, piece), piece)

    def send(k, part, to, slot, src=None):
        block = wbuf.at[k, rows(c, part)]
        n = len(sends)
        copy = remote(block if src is None else src, block, ici_s.at[n], ici_r.at[slot, part], to)
        copy.start()
        sends.append(copy)

    own = [w.at[rows(c, part)] for part in range(2)]
    send(mine, 0, up, 0, own[0])
    send(mine, 1, down, 1, own[1])
    send(mine, 0, left, 3, own[0])
    send(mine, 1, right, 3, own[1])
    send(mine, 1, up, 0, own[1])
    send(mine, 0, down, 1, own[0])
    local = pltpu.make_async_copy(w, wbuf.at[mine], own_sem)
    local.start()

    for i in range(16):
        block = tok[:, i * 128 : (i + 1) * 128].astype(F32).T
        for r in range(16):
            core, xlow, yy = r // 8, r // 4 % 2, r % 4
            tt[core, i // 8 * 2 + xlow, yy, i % 8 * 8 : i % 8 * 8 + 8, :] = block[r * 8 : r * 8 + 8, :]
    tb[...] = tt[...].astype(BF16)
    swap = remote(tb.at[1 - c], tr, tok_sem.at[0], tok_sem.at[1], mate)
    swap.start()
    half = tb[pl.ds(c, 1)][0]
    t1_o[:, :, :, :128] = half
    for a in range(4):
        for b in range(4):
            t2_o[b, a, :, :128] = half[a, b]
    acc[...] = jnp.zeros_like(acc)
    local.wait()

    outs = []

    def out(k):
        copy = pltpu.make_async_copy(wbuf.at[k], wf_o.at[k], hbm_sem.at[len(outs)])
        copy.start()
        outs.append(copy)

    def arrive(slot, part):
        k = rel[slot]
        block = wbuf.at[k, rows(c, part)]
        remote(block, block, ici_s.at[0], ici_r.at[slot, part], mate).wait_recv()
        copy = remote(block, block, d2d_s.at[slot, part], d2d_r.at[slot, part], mate)
        copy.start()
        sends.append(copy)

    def whole(slot):
        for part in range(2):
            block = wbuf.at[rel[slot], rows(1 - c, part)]
            remote(block, block, d2d_s.at[slot, part], d2d_r.at[slot, part], mate).wait_recv()
        out(rel[slot])

    def forward(slot, part, to, there):
        k = rel[slot]
        block = wbuf.at[k, rows(c, part)]
        copy = remote(block, block, ici_s.at[count[0]], ici_r.at[there, part], to)
        count[0] += 1
        copy.start()
        sends.append(copy)

    count = [len(sends)]

    def multiply(ks):
        def body(i, carry):
            k = ks[0]
            for n in range(1, len(ks)):
                k = jnp.where(i == n, ks[n], k)
            acc[...] += dot(tok[:, pl.ds(pl.multiple_of(k * depth, depth), depth)], wbuf[k])
            return carry

        lax.fori_loop(0, len(ks), body, 0)

    out(mine)
    multiply([mine])
    arrive(0, 0)
    forward(0, 0, up, 2)
    forward(0, 0, left, 4)
    arrive(1, 1)
    forward(1, 1, down, 2)
    forward(1, 1, right, 5)
    arrive(3, 0)
    arrive(3, 1)
    arrive(0, 1)
    forward(0, 1, right, 4)
    arrive(1, 0)
    forward(1, 0, left, 5)
    arrive(4, 0)
    arrive(5, 1)
    whole(3)
    whole(0)
    whole(1)
    multiply([rel[3], rel[0], rel[1]])
    arrive(2, 0)
    forward(2, 0, left, 6)
    arrive(2, 1)
    forward(2, 1, right, 6)
    arrive(4, 1)
    arrive(5, 0)
    whole(2)
    whole(4)
    whole(5)
    multiply([rel[2], rel[4], rel[5]])
    swap.wait()
    other = tr[...]
    t1_o[:, :, :, 128:] = other
    for a in range(4):
        for b in range(4):
            t2_o[b, a, :, 128:] = other[a, b]
    arrive(6, 0)
    arrive(6, 1)
    whole(6)
    multiply([rel[6]])
    x_o[...] = acc[:, :inner].astype(BF16)
    wide = bc_o.shape[1]
    bc_o[...] = acc[:, inner : inner + wide].astype(BF16)
    raw_o[...] = acc[:, inner + wide :]
    for copy in sends:
        copy.wait_send()
    for copy in outs:
        copy.wait()


def gather(tokens, w):
    count, width = tokens.shape
    depth, cols = w.shape
    sd = jax.ShapeDtypeStruct
    return pl.pallas_call(
        gather_kernel,
        out_shape=(
            sd((count, 2048), BF16),
            sd((count, 256), BF16),
            sd((count, 32), F32),
            sd((8, depth, cols), BF16),
            sd((4, 4, 64, 2 * count), BF16),
            sd((4, 4, 64, 2 * count), BF16),
        ),
        in_specs=[VM, VM],
        out_specs=(VM, VM, VM, ANY, VM, VM),
        scratch_shapes=[
            pltpu.VMEM((8, depth, cols), BF16),
            pltpu.VMEM((count, cols), F32),
            pltpu.VMEM((2, 4, 4, 64, count), F32),
            pltpu.VMEM((2, 4, 4, 64, count), BF16),
            pltpu.VMEM((4, 4, 64, count), BF16),
            pltpu.SemaphoreType.DMA((14,)),
            pltpu.SemaphoreType.DMA((7, 2)),
            pltpu.SemaphoreType.DMA((7, 2)),
            pltpu.SemaphoreType.DMA((7, 2)),
            pltpu.SemaphoreType.DMA((2,)),
            pltpu.SemaphoreType.DMA((8,)),
            pltpu.SemaphoreType.DMA,
        ],
        compiler_params=pltpu.CompilerParams(collective_id=0, has_side_effects=True, vmem_limit_bytes=LIMIT),
    )(tokens, w)


def spread(row):
    lane = lax.broadcasted_iota(jnp.int32, (row.shape[0], 128), 1)
    out = []
    for j in range(16):
        out.append(jnp.where(lane < 64, row[:, 2 * j : 2 * j + 1], row[:, 2 * j + 1 : 2 * j + 2]))
    return out


def scan_kernel(
    x_r, bc_r, raw_r, al_r, bias_r, skip_r, g_r, y_o, ga_o, gb_o,
    dte, ece, tle, cume, cumt, xdt, xt, gec, yi, dxi, ds_acc,
    stf, sst, pst, tot_s, tot_r, te, msg, rmsg, dmsg, dr, res, rres, se, hs, ske,
    d_sem, s0, r0, s1, r1, s2, r2,
):
    xh, z, c, xl, y = place()
    chip = xh * 8 + z
    mate = {"c": 1 - c}
    others = []
    for d in range(1, 16):
        t = (chip + d) % 16
        others.append((d, t, (chip + 16 - d) % 16, {"xh": t // 8, "z": t % 8}))
    greet([mate] + [o[3] for o in others])

    count = x_r.shape[0]
    zeros = jnp.zeros((count, 96), F32)
    rowz = jnp.zeros((1, 96), F32)
    decay_rate = jnp.concatenate([-jnp.exp(al_r[...]), rowz], axis=1)
    bias = jnp.concatenate([bias_r[...], rowz], axis=1)
    u = jnp.concatenate([raw_r[...], zeros], axis=1) + bias
    small = jnp.exp(-jnp.abs(u))
    dt = jnp.maximum(u, 0.0) + jnp.log1p(small)
    sig = jnp.where(u >= 0, 1.0, small) / (1.0 + small)
    ti = lax.broadcasted_iota(jnp.int32, (128, 128), 0)
    si = lax.broadcasted_iota(jnp.int32, (128, 128), 1)
    keep = ti >= si
    keep_t = ti <= si
    lower = jnp.where(keep, 1.0, 0.0).astype(F32)
    upper = jnp.where(keep_t, 1.0, 0.0).astype(F32)
    cum = dot(lower, decay_rate * dt, lax.Precision.HIGHEST)
    total = cum[127:128, :]
    tot_s[...] = jnp.broadcast_to(total, (8, 128))
    tot_copy = remote(tot_s, tot_r, d_sem.at[0], d_sem.at[1], mate)
    tot_copy.start()
    growth = jnp.exp(cum)
    tail = jnp.exp(total - cum)
    cumt[...] = cum.T
    lane = lax.broadcasted_iota(jnp.int32, (count, 128), 1)
    for arr, dst in ((dt, dte), (growth, ece), (tail, tle)):
        for j, e in enumerate(spread(arr)):
            dst[:, j * 128 : (j + 1) * 128] = e
    for j, e in enumerate(spread(jnp.broadcast_to(jnp.concatenate([skip_r[...], rowz], axis=1), (8, 128)))):
        ske[:, j * 128 : (j + 1) * 128] = e
    xf = x_r[...].astype(F32)
    gf = g_r[...].astype(F32)
    xd = xf * dte[...]
    xdt[...] = xd.astype(BF16)
    xt[...] = (xd * tle[...]).astype(BF16)
    gec[...] = (gf * ece[...]).astype(BF16)
    bm = bc_r[:, :128]
    cm = bc_r[:, 128:]
    bt = bm.astype(F32).T.astype(BF16)
    ct = cm.astype(F32).T.astype(BF16)
    for half in range(2):
        cols = slice(half * 1024, half * 1024 + 1024)
        stf[half, 0] = dot(bt, xt[:, cols])
        stf[half, 1] = dot(ct, gec[:, cols])
    sst[...] = stf[pl.ds(1 - c, 1)][0].astype(BF16)
    st_copy = remote(sst, pst, d_sem.at[2], d_sem.at[3], mate)
    st_copy.start()
    tot_copy.wait()
    for n, arr in enumerate((tot_s, tot_r)):
        for j, e in enumerate(spread(arr[...])):
            te[n, j // 8, :, j % 8 * 128 : j % 8 * 128 + 128] = e
    t_own = te[0, pl.ds(c, 1)][0][0:1]
    t_mate = te[1, pl.ds(c, 1)][0][0:1]
    first = c == 0
    for j in range(8):
        dmsg[j] = te[0, pl.ds(c, 1), :, j * 128 : j * 128 + 128][0] + te[1, pl.ds(c, 1), :, j * 128 : j * 128 + 128][0]
    dr[pl.ds(chip, 1)] = dmsg[pl.ds(chip // 2, 1)]
    copies = []
    for d, t, source, target in others:
        copy = remote(dmsg.at[t // 2], dr.at[chip], s0.at[d], r0.at[d], target)
        copy.start()
        copies.append(copy)
    e_own, e_mate = jnp.exp(t_own), jnp.exp(t_mate)
    e0 = jnp.where(first, e_own, e_mate)
    e1 = jnp.where(first, e_mate, e_own)
    st_copy.wait()
    own_f, own_b = stf[pl.ds(c, 1), 0][0], stf[pl.ds(c, 1), 1][0]
    mate_f, mate_b = pst[0].astype(F32), pst[1].astype(F32)
    f0 = jnp.where(first, own_f, mate_f)
    f1 = jnp.where(first, mate_f, own_f)
    b0 = jnp.where(first, own_b, mate_b)
    b1 = jnp.where(first, mate_b, own_b)
    chip_f = (e1 * f0 + f1).astype(BF16)
    chip_b = (b0 + e0 * b1).astype(BF16)
    for i in range(16):
        r, l = slice(i % 2 * 64, i % 2 * 64 + 64), slice(i // 2 * 128, i // 2 * 128 + 128)
        msg[i, 0] = chip_f[r, l]
        msg[i, 1] = chip_b[r, l]
    for d, t, source, target in others:
        copy = remote(msg.at[t], rmsg.at[chip], s1.at[d], r1.at[d], target)
        copy.start()
        copies.append(copy)
    rmsg[pl.ds(chip, 1)] = msg[pl.ds(chip, 1)]

    scores = dot_nt(cm, bm)
    scores_t = dot_nt(bm, cm)
    ds_acc[...] = jnp.zeros_like(ds_acc)
    for h in range(32):
        cume[:, h * 128 : h * 128 + 128] = jnp.broadcast_to(cum[:, h : h + 1], (count, 128))

    def pair(j, carry):
        cols = pl.ds(pl.multiple_of(j * 128, 128), 128)
        lows = pl.ds(pl.multiple_of(j * 256, 128), 128)
        highs = pl.ds(pl.multiple_of(j * 256 + 128, 128), 128)
        xj = xdt[:, cols]
        gj = g_r[:, cols]
        none = jnp.zeros_like(xj)
        xx = jnp.concatenate([jnp.where(lane < 64, xj, none), jnp.where(lane < 64, none, xj)], axis=0)
        gg = jnp.concatenate([jnp.where(lane < 64, gj, none), jnp.where(lane < 64, none, gj)], axis=0)
        ww = dot_nt(gg, xj)
        mix, mix_t = [], []
        total_ds = ds_acc[...]
        for n, where in enumerate((lows, highs)):
            span = cume[:, where] - cumt[pl.ds(2 * j + n, 1), :]
            decay = jnp.exp(jnp.where(keep, span, -1e30))
            decay_t = jnp.exp(jnp.where(keep_t, -span, -1e30))
            mix.append((scores * decay).astype(BF16))
            mix_t.append((scores_t * decay_t).astype(BF16))
            total_ds += ww[n * 128 : n * 128 + 128] * decay
        ds_acc[...] = total_ds
        yi[:, cols] = dot(jnp.concatenate(mix, axis=1), xx)
        dxi[:, cols] = dot(jnp.concatenate(mix_t, axis=1), gg)
        return carry

    lax.fori_loop(0, 8, pair, 0)

    for n, (d, t, source, target) in enumerate(others):
        remote(dmsg.at[0], dr.at[source], s0.at[d], r0.at[d], target).wait_recv()
        remote(msg.at[t], rmsg.at[source], s1.at[d], r1.at[d], target).wait_recv()
    state = jnp.zeros((64, 128), F32)
    for i in range(16):
        res[i, 0] = state.astype(BF16)
        state = jnp.exp(dr[i][0:1]) * state + rmsg[i, 0].astype(F32)
    state = jnp.zeros((64, 128), F32)
    for i in reversed(range(16)):
        res[i, 1] = state.astype(BF16)
        state = jnp.exp(dr[i][0:1]) * state + rmsg[i, 1].astype(F32)
    for d, t, source, target in others:
        copy = remote(res.at[t], rres.at[chip], s2.at[d], r2.at[d], target)
        copy.start()
        copies.append(copy)
    rres[pl.ds(chip, 1)] = res[pl.ds(chip, 1)]

    lax.fori_loop(8, 16, pair, 0)

    for d, t, source, target in others:
        remote(res.at[t], rres.at[source], s2.at[d], r2.at[d], target).wait_recv()
    for j in range(8):
        l = slice(j * 128, j * 128 + 128)
        at = pl.ds(c, 1)
        eo = jnp.exp(te[0, at, :, l][0][0:1])
        em = jnp.exp(te[1, at, :, l][0][0:1])
        own_f, own_b = stf[at, 0, :, l][0], stf[at, 1, :, l][0]
        mate_f, mate_b = pst[0, :, l].astype(F32), pst[1, :, l].astype(F32)
        start0 = jnp.concatenate([rres[2 * j, 0], rres[2 * j + 1, 0]], axis=0).astype(F32)
        end1 = jnp.concatenate([rres[2 * j, 1], rres[2 * j + 1, 1]], axis=0).astype(F32)
        start1 = jnp.where(first, eo, em) * start0 + jnp.where(first, own_f, mate_f)
        end0 = jnp.where(first, mate_b, own_b) + jnp.where(first, em, eo) * end1
        se[at, 0, :, l] = jnp.where(first, start0, start1).astype(BF16)[None]
        se[at, 1, :, l] = jnp.where(first, end0, end1).astype(BF16)[None]
        hs[0, :, l] = jnp.where(first, start1, start0).astype(BF16)
        hs[1, :, l] = jnp.where(first, end1, end0).astype(BF16)
    back = remote(hs, se.at[c], d_sem.at[4], d_sem.at[5], mate)
    back.start()
    ds = ds_acc[...]
    ds_t = ds.T.astype(BF16)
    ds = ds.astype(BF16)
    segment = jnp.where(
        lax.broadcasted_iota(jnp.int32, (2048, 128), 0) // 64 == lax.broadcasted_iota(jnp.int32, (2048, 128), 1), 1.0, 0.0
    ).astype(BF16)

    def by_head(values):
        high = values.astype(BF16)
        low = (values - high.astype(F32)).astype(BF16)
        part = segment[: values.shape[1]]
        return high, low

    grad_c = dot(ds, bm)
    grad_b = dot(ds_t, cm)
    back.wait_send()
    remote(hs, se.at[1 - c], d_sem.at[4], d_sem.at[5], mate).wait_recv()
    p1 = jnp.zeros((count, 128), F32)
    p2 = jnp.zeros((count, 128), F32)
    p3 = jnp.zeros((count, 128), F32)
    he = jnp.zeros((8, 128), F32)

    def heads(values, part):
        high = values.astype(BF16)
        low = (values - high.astype(F32)).astype(BF16)
        return dot(high, part) + dot(low, part)

    for q in range(4):
        half, l = q // 2, slice(q % 2 * 512, q % 2 * 512 + 512)
        cols = slice(q * 512, q * 512 + 512)
        part = segment[cols]
        st, en = se[half, 0, :, l], se[half, 1, :, l]
        xs = x_r[:, cols].astype(F32)
        gs = g_r[:, cols].astype(F32)
        skip = ske[0:1, cols]
        yo = yi[:, cols] + ece[:, cols] * dot(cm, st)
        dxs = tle[:, cols] * dot(bm, en)
        dxn = dxi[:, cols] + dxs
        y_o[:, cols] = (yo + skip * xs).astype(BF16)
        dx = (dte[:, cols] * dxn + skip * gs).astype(BF16)
        lo, hi = q * 512, q * 512 + 512
        if hi <= 1152:
            ga_o[:, lo:hi] = dx
        elif lo >= 1152:
            gb_o[:, lo - 1152 : hi - 1152] = dx
        else:
            ga_o[:, lo:1152] = dx[:, : 1152 - lo]
            gb_o[:, : hi - 1152] = dx[:, 1152 - lo :]
        p1 += heads(gs * yo, part)
        p2 += heads(xs * dxn, part)
        p3 += heads(xs * dxs, part)
        both = jnp.sum(st.astype(F32) * en.astype(F32), axis=0, keepdims=True)
        he += heads(jnp.broadcast_to(both, (8, 512)), part)
        grad_c += dot_nt(gec[:, cols], st)
        grad_b += dot_nt(xt[:, cols], en)
    last = jnp.sum(dt * p3, axis=0, keepdims=True) + jnp.exp(total) * he[0:1]
    dloga = dot(upper, p1 - dt * p2, lax.Precision.HIGHEST) + last
    draw = (p2 + decay_rate * dloga) * sig
    gb_o[:, 896:1024] = grad_b.astype(BF16)
    gb_o[:, 1024:1152] = grad_c.astype(BF16)
    gb_o[:, 1152:1184] = draw[:, :32].astype(BF16)
    for copy in copies:
        copy.wait_send()


def layer(x, bc, raw, a_log, dt_bias, d_skip, g):
    count, inner = x.shape
    sd = jax.ShapeDtypeStruct
    vm = pltpu.VMEM
    dma = pltpu.SemaphoreType.DMA
    return pl.pallas_call(
        scan_kernel,
        out_shape=(sd((count, inner), BF16), sd((count, 1152), BF16), sd((count, 1184), BF16)),
        in_specs=[VM] * 7,
        out_specs=(VM, VM, VM),
        scratch_shapes=[
            vm((count, inner), F32), vm((count, inner), F32), vm((count, inner), F32),
            vm((count, 2 * inner), F32), vm((128, count), F32),
            vm((count, inner), BF16), vm((count, inner), BF16), vm((count, inner), BF16),
            vm((count, inner), F32), vm((count, inner), F32), vm((128, 128), F32),
            vm((2, 2, 128, 1024), F32), vm((2, 128, 1024), BF16), vm((2, 128, 1024), BF16),
            vm((8, 128), F32), vm((8, 128), F32), vm((2, 2, 8, 1024), F32),
            vm((16, 2, 64, 128), BF16), vm((16, 2, 64, 128), BF16),
            vm((8, 8, 128), F32), vm((16, 8, 128), F32),
            vm((16, 2, 64, 128), BF16), vm((16, 2, 64, 128), BF16),
            vm((2, 2, 128, 1024), BF16), vm((2, 128, 1024), BF16), vm((8, inner), F32),
            dma((6,)), dma((16,)), dma((16,)), dma((16,)), dma((16,)), dma((16,)), dma((16,)),
        ],
        compiler_params=pltpu.CompilerParams(collective_id=1, has_side_effects=True, vmem_limit_bytes=LIMIT),
    )(x, bc, raw, a_log.reshape(1, -1), dt_bias.reshape(1, -1), d_skip.reshape(1, -1), g)


class Ring:
    def __init__(self, me, plus, minus, src, got, send, recv):
        self.me, self.plus, self.minus, self.src, self.got = me, plus, minus, src, got
        self.send, self.recv = send, recv
        self.h = src.shape[1] // 2
        self.copies = []

    def part(self, step, half):
        return self.src.at[(self.me + step) % 4, pl.ds(half * self.h, self.h)]

    def go(self, n, block, target):
        copy = remote(block, self.got.at[n], self.send.at[n], self.recv.at[n], target)
        copy.start()
        self.copies.append(copy)

    def far(self):
        self.go(0, self.part(2, 0), self.plus)
        self.go(1, self.part(2, 1), self.minus)

    def near(self, step):
        if step == 1:
            self.go(2, self.part(1, 1), self.plus)
        else:
            self.go(3, self.part(3, 0), self.minus)

    def landed(self, n):
        remote(self.part(0, 0), self.got.at[n], self.send.at[n], self.recv.at[n], self.plus).wait_recv()
        return self.got[n].astype(F32)

    def add(self, step, half, n):
        at = (self.me + step) % 4
        rows = slice(half * self.h, half * self.h + self.h)
        self.src[at, rows] = (self.src[at, rows].astype(F32) + self.landed(n)).astype(BF16)

    def middle(self):
        self.add(1, 0, 0)
        self.go(4, self.part(1, 0), self.plus)
        self.add(3, 1, 1)
        self.go(5, self.part(3, 1), self.minus)

    def end(self):
        low = self.src[self.me, : self.h].astype(F32) + self.landed(3)
        high = self.src[self.me, self.h :].astype(F32) + self.landed(2)
        return low + self.landed(4), high + self.landed(5)


def grad_kernel(
    ga, gb, wf, t1, t2, gt_o, gw_o,
    wbuf, a2, b2, p1, p2, g1, g2, q1, q2, h1, h2, z1, z2, y1, y2,
    w_sem, d_sem, s1, r1, s2, r2, s3, r3, s4, r4, s5, r5, s6, r6,
):
    xh, z, c, xl, y = place()
    x = xh * 2 + xl
    right, left = along_x((x + 1) % 4), along_x((x + 3) % 4)
    up, down = {"y": (y + 1) % 4}, {"y": (y + 3) % 4}
    mate = {"c": 1 - c}
    zs = [(d, (z + d) % 8, {"z": (z + d) % 8}) for d in range(1, 8)]
    load = pltpu.make_async_copy(wf, wbuf, w_sem)
    load.start()
    greet([mate, right, left, up, down] + [o[2] for o in zs])
    count = ga.shape[0]
    ca = remote(ga, a2.at[1], d_sem.at[0], d_sem.at[1], mate)
    cb = remote(gb, b2.at[1], d_sem.at[2], d_sem.at[3], mate)
    ca.start()
    cb.start()
    a2[0] = ga[...]
    b2[0] = gb[...]
    ring1 = Ring(x, right, left, p1, g1, s1, r1)
    ring2 = Ring(y, up, down, p2, g2, s2, r2)

    def partial(p, t, both, at):
        lhs = t[at].reshape(256, 2 * count)
        p[at] = (dot(lhs[:, :count], both[0]) + dot(lhs[:, count:], both[1])).astype(BF16)

    ca.wait()
    partial(p1, t1, a2, (x + 2) % 4)
    ring1.far()
    cb.wait()
    partial(p2, t2, b2, (y + 2) % 4)
    ring2.far()
    for step in (1, 3):
        partial(p1, t1, a2, (x + step) % 4)
        ring1.near(step)
        partial(p2, t2, b2, (y + step) % 4)
        ring2.near(step)
    partial(p1, t1, a2, x)
    partial(p2, t2, b2, y)

    load.wait()

    def tokens(k, carry):
        w = wbuf[k]
        cols = pl.ds(pl.multiple_of(k * 256, 256), 256)
        gt_o[:, cols] = (dot_nt(ga[...], w[:, :1152]) + dot_nt(gb[...], w[:, 1152:])).astype(BF16)
        return carry

    lax.fori_loop(0, 4, tokens, 0)
    ring1.middle()
    ring2.middle()
    lax.fori_loop(4, 8, tokens, 0)

    ring3 = Ring(y, up, down, q1, h1, s3, r3)
    ring4 = Ring(x, right, left, q2, h2, s4, r4)
    for ring, nxt, q in ((ring1, ring3, q1), (ring2, ring4, q2)):
        low, high = ring.end()
        for k in range(2):
            q[k] = low[k * 64 : k * 64 + 64].astype(BF16)
            q[k + 2] = high[k * 64 : k * 64 + 64].astype(BF16)
        nxt.far()
        nxt.near(1)
        nxt.near(3)
    ring3.middle()
    ring4.middle()
    copies = []
    for ring, zb, yb, s, r in ((ring3, z1, y1, s5, r5), (ring4, z2, y2, s6, r6)):
        low, high = ring.end()
        for k in range(4):
            zb[k] = low[k * 8 : k * 8 + 8].astype(BF16)
            zb[k + 4] = high[k * 8 : k * 8 + 8].astype(BF16)
        for d, t, target in zs:
            copy = remote(zb.at[t], yb.at[d], s.at[d], r.at[d], target)
            copy.start()
            copies.append(copy)
    for zb, yb, s, r, lo in ((z1, y1, s5, r5, 0), (z2, y2, s6, r6, 1152)):
        out = zb[z].astype(F32)
        for d, t, target in zs:
            remote(zb.at[t], yb.at[d], s.at[d], r.at[d], target).wait_recv()
            out += yb[d].astype(F32)
        gw_o[:, lo : lo + out.shape[1]] = out
    for ring in (ring1, ring2, ring3, ring4):
        for copy in ring.copies:
            copy.wait_send()
    for copy in copies:
        copy.wait_send()


def weight_grads(ga, gb, wf, t1, t2):
    count = ga.shape[0]
    wa, wb = ga.shape[1], gb.shape[1]
    sd = jax.ShapeDtypeStruct
    vm = pltpu.VMEM
    dma = pltpu.SemaphoreType.DMA
    return pl.pallas_call(
        grad_kernel,
        out_shape=(sd((count, 2048), BF16), sd((8, wa + wb), F32)),
        in_specs=[VM, VM, ANY, VM, VM],
        out_specs=(VM, VM),
        scratch_shapes=[
            vm(wf.shape, BF16),
            vm((2, count, wa), BF16), vm((2, count, wb), BF16),
            vm((4, 256, wa), BF16), vm((4, 256, wb), BF16),
            vm((6, 128, wa), BF16), vm((6, 128, wb), BF16),
            vm((4, 64, wa), BF16), vm((4, 64, wb), BF16),
            vm((6, 32, wa), BF16), vm((6, 32, wb), BF16),
            vm((8, 8, wa), BF16), vm((8, 8, wb), BF16),
            vm((8, 8, wa), BF16), vm((8, 8, wb), BF16),
            dma, dma((4,)),
        ]
        + [dma((6,))] * 8
        + [dma((8,))] * 4,
        compiler_params=pltpu.CompilerParams(collective_id=2, has_side_effects=True, vmem_limit_bytes=LIMIT),
    )(ga, gb, wf, t1, t2)


def per_device(tokens, w_in, a_log, dt_bias, d_skip, grad_y):
    count, width = tokens.shape[1:]
    inner = grad_y.shape[2]
    x, bc, raw, wf, t1, t2 = gather(tokens.reshape(count, width), w_in)
    y, ga, gb = layer(x, bc, raw, a_log, dt_bias, d_skip, grad_y.reshape(count, inner))
    gt, gw = weight_grads(ga, gb, wf, t1, t2)
    return (y.reshape(1, count, inner), gt.reshape(1, count, width), gw)


def solution(mesh):
    torus = Mesh(mesh.devices.reshape(2, 8, 2, 2, 4), ("xh", "z", "c", "xl", "y"))
    placed = (P(ZERO, SEQ, None), P(ZERO, None), P(), P(), P(), P(ZERO, SEQ, None))
    return jax.shard_map(
        per_device,
        mesh=torus,
        in_specs=placed,
        out_specs=(P(ZERO, SEQ, None), P(ZERO, SEQ, None), P(SEQ + ZERO, None)),
        check_vma=False,
    )
```

```python
import jax
import jax.numpy as jnp
from jax import lax
from jax.experimental import pallas as pl
from jax.experimental.pallas import tpu as pltpu
from jax.sharding import Mesh
from jax.sharding import PartitionSpec as P

SEQ = ("xh", "z", "c")
ZERO = ("xl", "y")
MESH = pl.DeviceIdType.MESH
F32 = jnp.float32
BF16 = jnp.bfloat16
LIMIT = 62 * 1024 * 1024
VM = pl.BlockSpec(memory_space=pltpu.VMEM)
ANY = pl.BlockSpec(memory_space=pl.ANY)
INNER = 2048
EDGE_SMALL, EDGE_LARGE = 384, 400
WX, WZ, WY = 768, 768, 800


def remote(src, dst, send, recv, target):
    return pltpu.make_async_remote_copy(
        src_ref=src, dst_ref=dst, send_sem=send, recv_sem=recv, device_id=target, device_id_type=MESH
    )


def along_x(x):
    return {"xh": x // 2, "xl": x % 2}


def dot(a, b, precision=None):
    return jnp.dot(a, b, preferred_element_type=F32, precision=precision)


def dot_nt(a, b):
    return lax.dot_general(a, b, (((1,), (1,)), ((), ())), preferred_element_type=F32)


class Place:
    def __init__(self):
        self.xh, self.z, self.c, self.xl, self.y = (lax.axis_index(a) for a in ("xh", "z", "c", "xl", "y"))
        self.x = self.xh * 2 + self.xl
        self.chip = self.xh * 8 + self.z
        self.right, self.left = along_x((self.x + 1) % 4), along_x((self.x + 3) % 4)
        self.up, self.down = {"y": (self.y + 1) % 4}, {"y": (self.y + 3) % 4}
        self.fore, self.aft = {"z": (self.z + 1) % 8}, {"z": (self.z + 7) % 8}
        self.mate = {"c": 1 - self.c}
        self.others = []
        for d in range(1, 16):
            t = (self.chip + d) % 16
            self.others.append((d, t, (self.chip + 16 - d) % 16, {"xh": t // 8, "z": t % 8}))

    def greet(self):
        barrier = pltpu.get_barrier_semaphore()
        targets = [self.mate, self.right, self.left, self.up, self.down] + [o[3] for o in self.others]
        for target in targets:
            pl.semaphore_signal(barrier, inc=1, device_id=target, device_id_type=MESH)
        pl.semaphore_wait(barrier, len(targets))


class Gather:
    def __init__(self, at, w, wbuf, s):
        self.at, self.w, self.wbuf, self.s = at, w, wbuf, s
        self.sends, self.n = [], 0
        self.rel = [self.shard(0, 3), self.shard(0, 1), self.shard(0, 2)] + [self.shard(1, d) for d in (0, 3, 1, 2)]
        self.mine = self.shard(0, 0)

    def shard(self, flip, dy):
        return (self.at.xl + flip) % 2 * 4 + (self.at.y + dy) % 4

    def rows(self, part, core=None):
        core = self.at.c if core is None else core
        odd = self.at.z % 2
        base = core * (2 * EDGE_SMALL + EDGE_LARGE)
        far = EDGE_SMALL + EDGE_LARGE
        if part == "a":
            start, size = base + odd * far, EDGE_SMALL
        elif part == "b":
            start, size = base + EDGE_SMALL, EDGE_LARGE
        elif part in ("a0", "a1"):
            start, size = base + odd * far + (part == "a1") * (EDGE_SMALL // 2), EDGE_SMALL // 2
        else:
            start, size = base + (1 - odd) * far + (part == "m1") * (EDGE_SMALL // 2), EDGE_SMALL // 2
        return pl.ds(pl.multiple_of(start, 16), size)

    def block(self, k, part, core=None):
        return self.wbuf.at[k, self.rows(part, core)]

    def send(self, k, part, to, slot, lane):
        block = self.block(k, part)
        copy = remote(block, block, self.s["send"].at[self.n], self.s["ici"].at[slot, lane], to)
        self.n += 1
        copy.start()
        self.sends.append(copy)

    def depth_send(self, k, slot):
        self.send(k, "a0", self.at.fore, slot, 2)
        self.send(k, "a1", self.at.aft, slot, 3)

    def begin(self):
        at = self.at
        self.send(self.mine, "a", at.up, 0, 0)
        self.send(self.mine, "b", at.down, 1, 1)
        self.send(self.mine, "a", at.left, 3, 0)
        self.send(self.mine, "b", at.right, 3, 1)
        self.send(self.mine, "b", at.up, 0, 1)
        self.send(self.mine, "a", at.down, 1, 0)

    def arrive(self, slot, lane):
        part = ("a", "b", "m0", "m1")[lane]
        block = self.block(self.rel[slot], part)
        remote(block, block, self.s["send"].at[0], self.s["ici"].at[slot, lane], self.at.mate).wait_recv()
        copy = remote(block, block, self.s["d2d_send"].at[slot, lane], self.s["d2d"].at[slot, lane], self.at.mate)
        copy.start()
        self.sends.append(copy)

    def a(self, slot, *onward):
        self.arrive(slot, 0)
        for to, there in onward:
            self.send(self.rel[slot], "a", to, there, 0)
        self.depth_send(self.rel[slot], slot)

    def b(self, slot, *onward):
        self.arrive(slot, 1)
        for to, there in onward:
            self.send(self.rel[slot], "b", to, there, 1)

    def m(self, slot):
        self.arrive(slot, 2)
        self.arrive(slot, 3)

    def whole(self, slot):
        for lane, part in enumerate(("a", "b", "m0", "m1")):
            block = self.block(self.rel[slot], part, 1 - self.at.c)
            remote(block, block, self.s["d2d_send"].at[slot, lane], self.s["d2d"].at[slot, lane], self.at.mate).wait_recv()


def spread(row):
    lane = lax.broadcasted_iota(jnp.int32, (row.shape[0], 128), 1)
    out = []
    for j in range(16):
        out.append(jnp.where(lane < 64, row[:, 2 * j : 2 * j + 1], row[:, 2 * j + 1 : 2 * j + 2]))
    return out


def heads(values, part):
    high = values.astype(BF16)
    low = (values - high.astype(F32)).astype(BF16)
    return dot(high, part) + dot(low, part)


class Ring4:
    def __init__(self, me, plus, minus, src, got, send, recv):
        self.me, self.plus, self.minus, self.src, self.got = me, plus, minus, src, got
        self.sem, self.recv = send, recv
        self.h = src.shape[1] // 2
        self.copies = []

    def part(self, step, half):
        return self.src.at[(self.me + step) % 4, pl.ds(half * self.h, self.h)]

    def go(self, n, block, target):
        copy = remote(block, self.got.at[n], self.sem.at[n], self.recv.at[n], target)
        copy.start()
        self.copies.append(copy)

    def far(self):
        self.go(0, self.part(2, 0), self.plus)
        self.go(1, self.part(2, 1), self.minus)

    def near(self, step):
        if step == 1:
            self.go(2, self.part(1, 1), self.plus)
        else:
            self.go(3, self.part(3, 0), self.minus)

    def landed(self, n):
        remote(self.part(0, 0), self.got.at[n], self.sem.at[n], self.recv.at[n], self.plus).wait_recv()
        return self.got[n].astype(F32)

    def add(self, step, half, n):
        at = (self.me + step) % 4
        rows = slice(half * self.h, half * self.h + self.h)
        self.src[at, rows] = (self.src[at, rows].astype(F32) + self.landed(n)).astype(BF16)

    def middle(self):
        self.add(1, 0, 0)
        self.go(4, self.part(1, 0), self.plus)
        self.add(3, 1, 1)
        self.go(5, self.part(3, 1), self.minus)

    def end(self):
        low = self.src[self.me, : self.h].astype(F32) + self.landed(3)
        high = self.src[self.me, self.h :].astype(F32) + self.landed(2)
        return low + self.landed(4), high + self.landed(5)


class Ring8:
    def __init__(self, me, plus, minus, src, got, send, recv):
        self.me, self.src, self.got, self.sem, self.recv = me, src, got, send, recv
        self.to = (plus, minus)
        self.h = src.shape[1] // 2
        self.copies = []

    def piece(self, way, s):
        return (self.me + (s if way == 0 else 8 - s)) % 8

    def slot(self, way, half, s):
        return (way * 2 + half) * 4 + s

    def go(self, way, half, s):
        block = self.src.at[self.piece(way, s), pl.ds(half * self.h, self.h)]
        n = self.slot(way, half, s - 1)
        copy = remote(block, self.got.at[n], self.sem.at[n], self.recv.at[n], self.to[way])
        copy.start()
        self.copies.append(copy)

    def landed(self, way, half, s):
        n = self.slot(way, half, s)
        block = self.src.at[self.me, pl.ds(0, self.h)]
        remote(block, self.got.at[n], self.sem.at[n], self.recv.at[n], self.to[way]).wait_recv()
        return self.got[n].astype(F32)

    def on(self, way, half, s):
        at = self.piece(way, s)
        rows = slice(half * self.h, half * self.h + self.h)
        self.src[at, rows] = (self.src[at, rows].astype(F32) + self.landed(way, half, s)).astype(BF16)
        self.go(way, half, s)

    def far(self):
        self.go(0, 0, 4)
        self.go(1, 1, 4)

    def next_far(self, way):
        self.go(way, 1 - way, 3)

    def long(self, s):
        self.on(0, 0, s)
        self.on(1, 1, s)

    def short(self, s):
        self.on(0, 1, s)
        self.on(1, 0, s)

    def end(self):
        low = self.src[self.me, : self.h].astype(F32) + self.landed(1, 0, 0)
        high = self.src[self.me, self.h :].astype(F32) + self.landed(0, 1, 0)
        return low + self.landed(0, 0, 0), high + self.landed(1, 1, 0)


def kernel(names, *refs):
    r = dict(zip(names, refs))
    at = Place()
    c, x, y, z, chip, mate = at.c, at.x, at.y, at.z, at.chip, at.mate
    first = c == 0
    own = pl.ds(c, 1)

    tok, acc, wbuf = r["tok"], r["acc"], r["wbuf"]
    count = tok.shape[0]
    depth = wbuf.shape[2]
    gather = Gather(at, r["w"], wbuf, {"send": r["g_send"], "ici": r["g_ici"], "d2d_send": r["g_d2d_send"], "d2d": r["g_d2d"]})
    w_copy = pltpu.make_async_copy(r["w"], wbuf.at[gather.mine], r["in_sem"].at[0])
    tok_copy = pltpu.make_async_copy(r["tokens"], tok, r["in_sem"].at[1])
    g_copy = pltpu.make_async_copy(r["grad_y"], r["g"], r["in_sem"].at[2])
    w_copy.start()
    tok_copy.start()
    g_copy.start()
    at.greet()
    w_copy.wait()
    gather.begin()
    tok_copy.wait()
    tt, tt3 = r["tt"], r["tt3"]
    for i in range(16):
        block = tok[:, i * 128 : (i + 1) * 128].astype(F32).T
        for n in range(16):
            core, xlow, yy = n // 8, n // 4 % 2, n % 4
            rows = block[n * 8 : n * 8 + 8, :]
            xx, zz = i // 8 * 2 + xlow, i % 8
            tt[core, xx, yy, zz * 8 : zz * 8 + 8, :] = rows
            tt3[core, zz, xx * 32 + yy * 8 : xx * 32 + yy * 8 + 8, :] = rows
    tb, tb3, tr, tr3 = r["tb"], r["tb3"], r["tr"], r["tr3"]
    tb[...] = tt[...].astype(BF16)
    tb3[...] = tt3[...].astype(BF16)
    swap = remote(tb.at[1 - c], tr, r["tok_sem"].at[0], r["tok_sem"].at[1], mate)
    swap3 = remote(tb3.at[1 - c], tr3, r["tok_sem"].at[2], r["tok_sem"].at[3], mate)
    swap.start()
    swap3.start()
    t1, t2, t3 = r["t1"], r["t2"], r["t3"]

    def place_rows(lo, one, three):
        t1[:, :, :, lo : lo + 128] = one
        t3[:, :, lo : lo + 128] = three
        for i in range(4):
            for j in range(4):
                t2[j, i, :, lo : lo + 128] = one[i, j]

    place_rows(0, tb[own][0], tb3[own][0])
    acc[...] = jnp.zeros_like(acc)

    def multiply(*ks):
        def body(i, carry):
            k = ks[0]
            for n in range(1, len(ks)):
                k = jnp.where(i == n, ks[n], k)
            acc[...] += dot_nt(tok[:, pl.ds(pl.multiple_of(k * depth, depth), depth)], wbuf[k])
            return carry

        lax.fori_loop(0, len(ks), body, 0)

    ga, gb, gm, rel = gather.a, gather.b, gather.m, gather.rel
    with jax.named_scope("g1"):
        ga(0, (at.up, 2), (at.left, 4))
        gb(1, (at.down, 2), (at.right, 5))
        ga(3)
        gb(3)
    with jax.named_scope("g2"):
        gb(0, (at.right, 4))
        ga(1, (at.left, 5))
        ga(4)
        gb(5)
        gm(0)
        gm(3)
    with jax.named_scope("g3"):
        ga(2, (at.left, 6))
        gb(2, (at.right, 6))
        gb(4)
        ga(5)
        gather.whole(0)
        gather.whole(3)
        multiply(gather.mine, rel[0], rel[3])
    with jax.named_scope("g4"):
        gm(1)
        gm(4)
        ga(6)
        gb(6)
        gm(2)
        gm(5)
        for slot in (1, 4, 2, 5):
            gather.whole(slot)
    with jax.named_scope("g5"):
        multiply(rel[1], rel[4], rel[2], rel[5])
    with jax.named_scope("g6"):
        swap.wait()
        swap3.wait()
        place_rows(128, tr[...], tr3[...])
        gm(6)
        gather.whole(6)
    with jax.named_scope("g7"):
        multiply(rel[6])

    x_r, g_r = r["x"], r["g"]
    dte, ece, tle, cume, cumt = r["dte"], r["ece"], r["tle"], r["cume"], r["cumt"]
    xdt, xt, gec, yi, dxi, ds_acc = r["xdt"], r["xt"], r["gec"], r["yi"], r["dxi"], r["ds_acc"]
    stf, sst, pst, te, ske = r["stf"], r["sst"], r["pst"], r["te"], r["ske"]
    tot_s, tot_r, dmsg, dr = r["tot_s"], r["tot_r"], r["dmsg"], r["dr"]
    msg, rmsg, res, rres, se, hs = r["msg"], r["rmsg"], r["res"], r["rres"], r["se"], r["hs"]
    d_sem = r["d_sem"]
    copies = []
    with jax.named_scope("prep"):
        x_r[...] = acc[:, :INNER].astype(BF16)
        bm = acc[:, INNER : INNER + 128].astype(BF16)
        cm = acc[:, INNER + 128 : INNER + 256].astype(BF16)
        rowz = jnp.zeros((1, 96), F32)
        decay_rate = jnp.concatenate([-jnp.exp(r["a_log"][...]), rowz], axis=1)
        bias = jnp.concatenate([r["dt_bias"][...], rowz], axis=1)
        u = jnp.concatenate([acc[:, INNER + 256 :], jnp.zeros((count, 96), F32)], axis=1) + bias
        small = jnp.exp(-jnp.abs(u))
        dt = jnp.maximum(u, 0.0) + jnp.log1p(small)
        sig = jnp.where(u >= 0, 1.0, small) / (1.0 + small)
        ti = lax.broadcasted_iota(jnp.int32, (128, 128), 0)
        si = lax.broadcasted_iota(jnp.int32, (128, 128), 1)
        keep, keep_t = ti >= si, ti <= si
        lower = jnp.where(keep, 1.0, 0.0).astype(F32)
        upper = jnp.where(keep_t, 1.0, 0.0).astype(F32)
        cum = dot(lower, decay_rate * dt, lax.Precision.HIGHEST)
        total = cum[127:128, :]
        tot_s[...] = jnp.broadcast_to(total, (8, 128))
        tot_copy = remote(tot_s, tot_r, d_sem.at[0], d_sem.at[1], mate)
        tot_copy.start()
        growth = jnp.exp(cum)
        tail = jnp.exp(total - cum)
        cumt[...] = cum.T
        lane = lax.broadcasted_iota(jnp.int32, (count, 128), 1)
        for arr, dst in ((dt, dte), (tail, tle), (growth, ece)):
            for j, e in enumerate(spread(arr)):
                dst[:, j * 128 : (j + 1) * 128] = e
        xd = x_r[...].astype(F32) * dte[...]
        xdt[...] = xd.astype(BF16)
        xt[...] = (xd * tle[...]).astype(BF16)
        bt = bm.astype(F32).T.astype(BF16)
        ct = cm.astype(F32).T.astype(BF16)

    def local_states(kind, lhs, rhs):
        for half in range(2):
            stf[kind, half] = dot(lhs, rhs[:, half * 1024 : half * 1024 + 1024])
        sst[kind] = stf[kind, pl.ds(1 - c, 1)][0].astype(BF16)
        copy = remote(sst.at[kind], pst.at[kind], d_sem.at[2 + 2 * kind], d_sem.at[3 + 2 * kind], mate)
        copy.start()
        return copy

    with jax.named_scope("states"):
        st_copies = [local_states(0, bt, xt)]
        g_copy.wait()
        gec[...] = (g_r[...].astype(F32) * ece[...]).astype(BF16)
        st_copies.append(local_states(1, ct, gec))
        tot_copy.wait()
        for n, arr in enumerate((tot_s, tot_r)):
            for j, e in enumerate(spread(arr[...])):
                te[n, j // 8, :, j % 8 * 128 : j % 8 * 128 + 128] = e
        for j in range(8):
            l = slice(j * 128, j * 128 + 128)
            dmsg[j] = te[0, own, :, l][0] + te[1, own, :, l][0]
        dr[pl.ds(chip, 1)] = dmsg[pl.ds(chip // 2, 1)]
        for d, t, source, target in at.others:
            copy = remote(dmsg.at[t // 2], dr.at[chip], r["s0"].at[d], r["r0"].at[d], target)
            copy.start()
            copies.append(copy)
        e_own, e_mate = jnp.exp(te[0, own][0][0:1]), jnp.exp(te[1, own][0][0:1])
        e0 = jnp.where(first, e_own, e_mate)
        e1 = jnp.where(first, e_mate, e_own)

    def send_states(kind):
        st_copies[kind].wait()
        mine, theirs = stf[kind, own][0], pst[kind].astype(F32)
        early = jnp.where(first, mine, theirs)
        late = jnp.where(first, theirs, mine)
        whole = (e1 * early + late if kind == 0 else early + e0 * late).astype(BF16)
        for i in range(16):
            msg[kind, i] = whole[i % 2 * 64 : i % 2 * 64 + 64, i // 2 * 128 : i // 2 * 128 + 128]
        for d, t, source, target in at.others:
            copy = remote(msg.at[kind, t], rmsg.at[kind, chip], r["s1"].at[kind, d], r["r1"].at[kind, d], target)
            copy.start()
            copies.append(copy)
        rmsg[kind, pl.ds(chip, 1)] = msg[kind, pl.ds(chip, 1)]

    def scan_states(kind):
        for d, t, source, target in at.others:
            if kind == 0:
                remote(dmsg.at[0], dr.at[source], r["s0"].at[d], r["r0"].at[d], target).wait_recv()
            remote(msg.at[kind, t], rmsg.at[kind, source], r["s1"].at[kind, d], r["r1"].at[kind, d], target).wait_recv()
        state = jnp.zeros((64, 128), F32)
        for i in range(16) if kind == 0 else reversed(range(16)):
            res[kind, i] = state.astype(BF16)
            state = jnp.exp(dr[i][0:1]) * state + rmsg[kind, i].astype(F32)
        for d, t, source, target in at.others:
            copy = remote(res.at[kind, t], rres.at[kind, chip], r["s2"].at[kind, d], r["r2"].at[kind, d], target)
            copy.start()
            copies.append(copy)
        rres[kind, pl.ds(chip, 1)] = res[kind, pl.ds(chip, 1)]

    def take_states(kind):
        for d, t, source, target in at.others:
            remote(res.at[kind, t], rres.at[kind, source], r["s2"].at[kind, d], r["r2"].at[kind, d], target).wait_recv()
        for j in range(8):
            l = slice(j * 128, j * 128 + 128)
            got = jnp.concatenate([rres[kind, 2 * j], rres[kind, 2 * j + 1]], axis=0).astype(F32)
            mine, theirs = stf[kind, own, :, l][0], pst[kind, :, l].astype(F32)
            if kind == 0:
                edge, inside = got, e0[:, l] * got + jnp.where(first, mine, theirs)
                low, high = edge, inside
            else:
                edge, inside = got, jnp.where(first, theirs, mine) + e1[:, l] * got
                low, high = inside, edge
            se[kind, own, :, l] = jnp.where(first, low, high).astype(BF16)[None]
            hs[kind, :, l] = jnp.where(first, high, low).astype(BF16)
        copy = remote(hs.at[kind], se.at[kind, c], d_sem.at[6 + 2 * kind], d_sem.at[7 + 2 * kind], mate)
        copy.start()
        copies.append(copy)

    def mate_states(kind):
        remote(hs.at[kind], se.at[kind, 1 - c], d_sem.at[6 + 2 * kind], d_sem.at[7 + 2 * kind], mate).wait_recv()

    with jax.named_scope("send_f"):
        send_states(0)
    with jax.named_scope("send_b"):
        send_states(1)

    with jax.named_scope("pairs_prep"):
        scores = dot_nt(cm, bm)
        scores_t = dot_nt(bm, cm)
        ds_acc[...] = jnp.zeros_like(ds_acc)
        for j, e in enumerate(spread(jnp.broadcast_to(jnp.concatenate([r["d_skip"][...], rowz], axis=1), (8, 128)))):
            ske[:, j * 128 : (j + 1) * 128] = e
        for h in range(32):
            cume[:, h * 128 : h * 128 + 128] = jnp.broadcast_to(cum[:, h : h + 1], (count, 128))

    def pair(j, carry):
        cols = pl.ds(pl.multiple_of(j * 128, 128), 128)
        xj = xdt[:, cols]
        gj = g_r[:, cols]
        none = jnp.zeros_like(xj)
        xx = jnp.concatenate([jnp.where(lane < 64, xj, none), jnp.where(lane < 64, none, xj)], axis=0)
        gg = jnp.concatenate([jnp.where(lane < 64, gj, none), jnp.where(lane < 64, none, gj)], axis=0)
        ww = dot_nt(gg, xj)
        mix, mix_t = [], []
        total_ds = ds_acc[...]
        for n in range(2):
            span = cume[:, pl.ds(pl.multiple_of(j * 256 + n * 128, 128), 128)] - cumt[pl.ds(2 * j + n, 1), :]
            decay = jnp.exp(jnp.where(keep, span, -1e30))
            decay_t = jnp.exp(jnp.where(keep_t, -span, -1e30))
            mix.append((scores * decay).astype(BF16))
            mix_t.append((scores_t * decay_t).astype(BF16))
            total_ds += ww[n * 128 : n * 128 + 128] * decay
        ds_acc[...] = total_ds
        yi[:, cols] = dot(jnp.concatenate(mix, axis=1), xx)
        dxi[:, cols] = dot(jnp.concatenate(mix_t, axis=1), gg)
        return carry

    with jax.named_scope("pairs1"):
        lax.fori_loop(0, 6, pair, 0)
    with jax.named_scope("scan_f"):
        scan_states(0)
    with jax.named_scope("pairs2"):
        lax.fori_loop(6, 11, pair, 0)
    with jax.named_scope("scan_b"):
        scan_states(1)
    with jax.named_scope("pairs3"):
        lax.fori_loop(11, 16, pair, 0)
        ds = ds_acc[...]
        ds_t = ds.T.astype(BF16)
        ds = ds.astype(BF16)
        grad_c = dot(ds, bm)
        grad_b = dot(ds_t, cm)
    with jax.named_scope("take_f"):
        take_states(0)
        mate_states(0)
    segment = jnp.where(
        lax.broadcasted_iota(jnp.int32, (512, 128), 0) // 64 == lax.broadcasted_iota(jnp.int32, (512, 128), 1), 1.0, 0.0
    ).astype(BF16)
    y_v = r["y_v"]

    def place_heads(arrs):
        lane8 = lax.broadcasted_iota(jnp.int32, arrs[0].shape, 1)
        out = arrs[0]
        for q in range(1, 4):
            out = jnp.where(lane8 < 8 * q, out, pltpu.roll(arrs[q], 8 * q, 1))
        return out

    with jax.named_scope("y_part"):
        p1 = []
        for q in range(4):
            half, l = q // 2, slice(q % 2 * 512, q % 2 * 512 + 512)
            cols = slice(q * 512, q * 512 + 512)
            st = se[0, half, :, l]
            xs = x_r[:, cols].astype(F32)
            yo = yi[:, cols] + ece[:, cols] * dot(cm, st)
            y_v[:, cols] = (yo + ske[0:1, cols] * xs).astype(BF16)
            p1.append(heads(g_r[:, cols].astype(F32) * yo, segment))
            grad_c += dot_nt(gec[:, cols], st)
        p1 = place_heads(p1)
        y_copy = pltpu.make_async_copy(y_v, r["y_out"], r["in_sem"].at[0])
        y_copy.start()
    with jax.named_scope("take_b"):
        take_states(1)
        mate_states(1)

    gx, gz, gy = r["gx"], r["gz"], r["gy"]
    swaps = {}

    def swap_grads(n, buf):
        copy = remote(buf.at[0], buf.at[1], r["gs_sem"].at[n], r["gr_sem"].at[n], mate)
        copy.start()
        swaps[n] = copy

    p2, p3, he = [], [], []

    def x_part(q):
        half, l = q // 2, slice(q % 2 * 512, q % 2 * 512 + 512)
        cols = slice(q * 512, q * 512 + 512)
        en = se[1, half, :, l]
        xs = x_r[:, cols].astype(F32)
        dxs = tle[:, cols] * dot(bm, en)
        dxn = dxi[:, cols] + dxs
        dx = (dte[:, cols] * dxn + ske[0:1, cols] * g_r[:, cols].astype(F32)).astype(BF16)
        if q == 0:
            gx[0, :, :512] = dx
        elif q == 1:
            gx[0, :, 512:] = dx[:, :256]
            gz[0, :, :256] = dx[:, 256:]
        elif q == 2:
            gz[0, :, 256:] = dx
        else:
            gy[0, :, :512] = dx
        p2.append(heads(xs * dxn, segment))
        p3.append(heads(xs * dxs, segment))
        both = jnp.sum(se[0, half, :, l].astype(F32) * en.astype(F32), axis=0, keepdims=True)
        he.append(heads(jnp.broadcast_to(both, (8, 512)), segment))
        return dot_nt(xt[:, cols], en)

    ring_x = Ring4(x, at.right, at.left, r["px"], r["got_x"], r["sx"], r["rx"])
    ring_y = Ring4(y, at.up, at.down, r["py"], r["got_y"], r["sy"], r["ry"])
    ring_z = Ring8(z, at.fore, at.aft, r["pz"], r["got_z"], r["sz"], r["rz"])

    def partial(p, lhs, both, piece):
        rows = p.shape[1]
        lhs = lhs[piece].reshape(rows, 2 * count)
        p[piece] = (dot(lhs[:, :count], both[0]) + dot(lhs[:, count:], both[1])).astype(BF16)

    with jax.named_scope("x_part1"):
        grad_b += x_part(0)
        grad_b += x_part(1)
        swap_grads(0, gx)
        grad_b += x_part(2)
        swap_grads(1, gz)
    with jax.named_scope("far_xz"):
        swaps[0].wait()
        partial(ring_x.src, t1, gx, (x + 2) % 4)
        ring_x.far()
        swaps[1].wait()
        partial(ring_z.src, t3, gz, (z + 4) % 8)
        ring_z.far()
    with jax.named_scope("x_part2"):
        grad_b += x_part(3)
        last = jnp.sum(dt * place_heads(p3), axis=0, keepdims=True) + jnp.exp(total) * place_heads(he)[0:1]
        p2 = place_heads(p2)
        dloga = dot(upper, p1 - dt * p2, lax.Precision.HIGHEST) + last
        draw = (p2 + decay_rate * dloga) * sig
        gy[0, :, 512:640] = grad_b.astype(BF16)
        gy[0, :, 640:768] = grad_c.astype(BF16)
        gy[0, :, 768:800] = draw[:, :32].astype(BF16)
        swap_grads(2, gy)
    with jax.named_scope("near"):
        for way in range(2):
            partial(ring_z.src, t3, gz, ring_z.piece(way, 3))
            ring_z.next_far(way)
        for step in (1, 3):
            partial(ring_x.src, t1, gx, (x + step) % 4)
            ring_x.near(step)
        swaps[2].wait()
        partial(ring_y.src, t2, gy, (y + 2) % 4)
        ring_y.far()
        for step in (1, 3):
            partial(ring_y.src, t2, gy, (y + step) % 4)
            ring_y.near(step)
        for s in (2, 1):
            for way in range(2):
                partial(ring_z.src, t3, gz, ring_z.piece(way, s))
    gt_v = r["gt_v"]

    def grad_tokens(k, carry):
        w = wbuf[k]
        cols = pl.ds(pl.multiple_of(k * 256, 256), 256)
        gt_v[:, cols] = (dot(gx[0], w[:WX]) + dot(gz[0], w[WX : WX + WZ]) + dot(gy[0], w[WX + WZ :])).astype(BF16)
        return carry

    with jax.named_scope("z3"):
        ring_z.long(3)
        partial(ring_x.src, t1, gx, x)
        partial(ring_z.src, t3, gz, z)
        partial(ring_y.src, t2, gy, y)
    with jax.named_scope("mid_x"):
        ring_x.middle()
        ring_z.short(2)
    with jax.named_scope("gt1"):
        lax.fori_loop(0, 2, grad_tokens, 0)
    with jax.named_scope("z2"):
        ring_z.long(2)
        ring_y.middle()
        ring_z.short(1)
    with jax.named_scope("gt2"):
        lax.fori_loop(2, 4, grad_tokens, 0)
    with jax.named_scope("z1"):
        ring_z.long(1)
    with jax.named_scope("gt3"):
        lax.fori_loop(4, 8, grad_tokens, 0)
        gt_copy = pltpu.make_async_copy(gt_v, r["gt_out"], r["in_sem"].at[1])
        gt_copy.start()

    ring_xy = Ring4(y, at.up, at.down, r["qx"], r["got_xy"], r["sxy"], r["rxy"])
    ring_yx = Ring4(x, at.right, at.left, r["qy"], r["got_yx"], r["syx"], r["ryx"])
    ring_zx = Ring4(x, at.right, at.left, r["qz"], r["got_zx"], r["szx"], r["rzx"])

    def onward(ring, nxt):
        q = nxt.src
        rows = q.shape[1]
        low, high = ring.end()
        for k in range(2):
            q[k] = low[k * rows : k * rows + rows].astype(BF16)
            q[k + 2] = high[k * rows : k * rows + rows].astype(BF16)
        nxt.far()
        nxt.near(1)
        nxt.near(3)

    with jax.named_scope("end_x"):
        onward(ring_x, ring_xy)
    with jax.named_scope("end_z"):
        onward(ring_z, ring_zx)
    with jax.named_scope("end_y"):
        onward(ring_y, ring_yx)
    with jax.named_scope("mids"):
        ring_xy.middle()
        ring_zx.middle()
        ring_yx.middle()
    along_z = [(d, (z + d) % 8, {"z": (z + d) % 8}) for d in range(1, 8)]
    along_y = [(d, (y + d) % 4, {"y": (y + d) % 4}) for d in range(1, 4)]
    lasts = []

    def scatter(ring, name, targets, lo):
        src, got, send, recv = (r[name + n] for n in ("_s", "_g", "_ss", "_rs"))
        low, high = ring.end()
        n = src.shape[0] // 2
        for k in range(n):
            src[k] = low[k * 8 : k * 8 + 8].astype(BF16)
            src[k + n] = high[k * 8 : k * 8 + 8].astype(BF16)
        for d, t, target in targets:
            copy = remote(src.at[t], got.at[d], send.at[d], recv.at[d], target)
            copy.start()
            copies.append(copy)
        lasts.append((src, got, send, recv, targets, lo))

    with jax.named_scope("scatter"):
        scatter(ring_xy, "fx", along_z, 0)
        scatter(ring_yx, "fy", along_z, WX + WZ)
        scatter(ring_zx, "fz", along_y, WX)
    gw = r["gw_out"]
    with jax.named_scope("finish"):
        for (src, got, send, recv, targets, lo), me in zip(lasts, (z, z, y)):
            out = src[me].astype(F32)
            for d, t, target in targets:
                remote(src.at[t], got.at[d], send.at[d], recv.at[d], target).wait_recv()
                out += got[d].astype(F32)
            gw[:, lo : lo + out.shape[1]] = out
        for ring in (ring_x, ring_y, ring_z, ring_xy, ring_yx, ring_zx):
            for copy in ring.copies:
                copy.wait_send()
        for copy in copies + gather.sends:
            copy.wait_send()
        y_copy.wait()
        gt_copy.wait()


def fused(tokens, w, a_log, dt_bias, d_skip, grad_y):
    count = tokens.shape[0]
    cols, depth = w.shape
    sd = jax.ShapeDtypeStruct
    dma = pltpu.SemaphoreType.DMA
    scratch = {
        "tok": ((count, 2048), BF16), "g": ((count, INNER), BF16), "wbuf": ((8, cols, depth), BF16), "acc": ((count, cols), F32),
        "tt": ((2, 4, 4, 64, count), F32), "tt3": ((2, 8, 128, count), F32),
        "tb": ((2, 4, 4, 64, count), BF16), "tb3": ((2, 8, 128, count), BF16),
        "tr": ((4, 4, 64, count), BF16), "tr3": ((8, 128, count), BF16),
        "t1": ((4, 4, 64, 2 * count), BF16), "t2": ((4, 4, 64, 2 * count), BF16), "t3": ((8, 128, 2 * count), BF16),
        "x": ((count, INNER), BF16), "y_v": ((count, INNER), BF16), "gt_v": ((count, 2048), BF16),
        "dte": ((count, INNER), F32), "ece": ((count, INNER), F32), "tle": ((count, INNER), F32),
        "cume": ((count, 2 * INNER), F32), "cumt": ((128, count), F32),
        "xdt": ((count, INNER), BF16), "xt": ((count, INNER), BF16), "gec": ((count, INNER), BF16),
        "yi": ((count, INNER), F32), "dxi": ((count, INNER), F32), "ds_acc": ((128, 128), F32),
        "stf": ((2, 2, 128, 1024), F32), "sst": ((2, 128, 1024), BF16), "pst": ((2, 128, 1024), BF16),
        "tot_s": ((8, 128), F32), "tot_r": ((8, 128), F32), "te": ((2, 2, 8, 1024), F32),
        "dmsg": ((8, 8, 128), F32), "dr": ((16, 8, 128), F32),
        "msg": ((2, 16, 64, 128), BF16), "rmsg": ((2, 16, 64, 128), BF16),
        "res": ((2, 16, 64, 128), BF16), "rres": ((2, 16, 64, 128), BF16),
        "se": ((2, 2, 128, 1024), BF16), "hs": ((2, 128, 1024), BF16), "ske": ((8, INNER), F32),
        "gx": ((2, count, WX), BF16), "gz": ((2, count, WZ), BF16), "gy": ((2, count, WY), BF16),
        "px": ((4, 256, WX), BF16), "py": ((4, 256, WY), BF16), "pz": ((8, 128, WZ), BF16),
        "got_x": ((6, 128, WX), BF16), "got_y": ((6, 128, WY), BF16), "got_z": ((16, 64, WZ), BF16),
        "qx": ((4, 64, WX), BF16), "qy": ((4, 64, WY), BF16), "qz": ((4, 32, WZ), BF16),
        "got_xy": ((6, 32, WX), BF16), "got_yx": ((6, 32, WY), BF16), "got_zx": ((6, 16, WZ), BF16),
        "fx_s": ((8, 8, WX), BF16), "fx_g": ((8, 8, WX), BF16), "fy_s": ((8, 8, WY), BF16), "fy_g": ((8, 8, WY), BF16),
        "fz_s": ((4, 8, WZ), BF16), "fz_g": ((4, 8, WZ), BF16),
    }
    sems = {
        "in_sem": (3,), "tok_sem": (4,), "g_send": (28,), "g_ici": (7, 4), "g_d2d_send": (7, 4), "g_d2d": (7, 4),
        "d_sem": (10,), "s0": (16,), "r0": (16,), "s1": (2, 16), "r1": (2, 16), "s2": (2, 16), "r2": (2, 16),
        "gs_sem": (3,), "gr_sem": (3,), "sx": (6,), "rx": (6,), "sy": (6,), "ry": (6,), "sz": (16,), "rz": (16,),
        "sxy": (6,), "rxy": (6,), "syx": (6,), "ryx": (6,), "szx": (6,), "rzx": (6,),
        "fx_ss": (8,), "fx_rs": (8,), "fy_ss": (8,), "fy_rs": (8,), "fz_ss": (4,), "fz_rs": (4,),
    }
    names = ["tokens", "w", "a_log", "dt_bias", "d_skip", "grad_y", "y_out", "gt_out", "gw_out", *scratch, *sems]

    def body(*refs):
        kernel(names, *refs)

    return pl.pallas_call(
        body,
        out_shape=(sd((count, INNER), BF16), sd((count, 2048), BF16), sd((8, cols), F32)),
        in_specs=[ANY, ANY, VM, VM, VM, ANY],
        out_specs=(ANY, ANY, VM),
        scratch_shapes=[pltpu.VMEM(*v) for v in scratch.values()] + [dma(v) for v in sems.values()],
        compiler_params=pltpu.CompilerParams(collective_id=0, has_side_effects=True, vmem_limit_bytes=LIMIT),
    )(tokens, w, a_log.reshape(1, -1), dt_bias.reshape(1, -1), d_skip.reshape(1, -1), grad_y)


def per_device(tokens, w_in, a_log, dt_bias, d_skip, grad_y):
    count, width = tokens.shape[1:]
    inner = grad_y.shape[2]
    y, gt, gw = fused(tokens.reshape(count, width), w_in.T, a_log, dt_bias, d_skip, grad_y.reshape(count, inner))
    return (y.reshape(1, count, inner), gt.reshape(1, count, width), gw)


def solution(mesh):
    torus = Mesh(mesh.devices.reshape(2, 8, 2, 2, 4), ("xh", "z", "c", "xl", "y"))
    placed = (P(ZERO, SEQ, None), P(ZERO, None), P(), P(), P(), P(ZERO, SEQ, None))
    return jax.shard_map(
        per_device,
        mesh=torus,
        in_specs=placed,
        out_specs=(P(ZERO, SEQ, None), P(ZERO, SEQ, None), P(SEQ + ZERO, None)),
        check_vma=False,
    )
```

```python
from types import SimpleNamespace

import jax
import jax.numpy as jnp
from jax import lax
from jax.experimental import pallas as pl
from jax.experimental.pallas import tpu as pltpu
from jax.sharding import Mesh
from jax.sharding import PartitionSpec as P

SEQ = ("xh", "z", "c")
ZERO = ("xl", "y")
MESH = pl.DeviceIdType.MESH
F32 = jnp.float32
BF16 = jnp.bfloat16
LIMIT = 62 * 1024 * 1024
VM = pl.BlockSpec(memory_space=pltpu.VMEM)
ANY = pl.BlockSpec(memory_space=pl.ANY)
INNER = 2048
EDGE_SMALL, EDGE_LARGE = 384, 400
WA, WZ, WB, WV = 1024, 384, 768, 160


def remote(src, dst, send, recv, target):
    return pltpu.make_async_remote_copy(
        src_ref=src, dst_ref=dst, send_sem=send, recv_sem=recv, device_id=target, device_id_type=MESH
    )


def sent(block, sem, target):
    remote(block, block, sem, sem, target).wait_send()


def received(block, sem, target):
    remote(block, block, sem, sem, target).wait_recv()


def along_x(x):
    return {"xh": x // 2, "xl": x % 2}


def dot(a, b, precision=None):
    return jnp.dot(a, b, preferred_element_type=F32, precision=precision)


def dot_nt(a, b):
    return lax.dot_general(a, b, (((1,), (1,)), ((), ())), preferred_element_type=F32)


class Place:
    def __init__(self):
        self.xh, self.z, self.c, self.xl, self.y = (lax.axis_index(a) for a in ("xh", "z", "c", "xl", "y"))
        self.x = self.xh * 2 + self.xl
        self.chip = self.xh * 8 + self.z
        self.right, self.left = along_x((self.x + 1) % 4), along_x((self.x + 3) % 4)
        self.up, self.down = {"y": (self.y + 1) % 4}, {"y": (self.y + 3) % 4}
        self.fore, self.aft = {"z": (self.z + 1) % 8}, {"z": (self.z + 7) % 8}
        self.mate = {"c": 1 - self.c}
        self.others = []
        for d in (4, 12, 3, 5, 11, 13, 2, 6, 10, 14, 8, 1, 7, 9, 15):
            t = (self.chip + d) % 16
            self.others.append((d, t, (self.chip + 16 - d) % 16, {"xh": t // 8, "z": t % 8}))

    def greet(self):
        barrier = pltpu.get_barrier_semaphore()
        targets = [self.mate, self.right, self.left, self.up, self.down, {"y": (self.y + 2) % 4}] + [o[3] for o in self.others]
        for target in targets:
            pl.semaphore_signal(barrier, inc=1, device_id=target, device_id_type=MESH)
        pl.semaphore_wait(barrier, len(targets))


class Gather:
    def __init__(self, at, w, wbuf, s):
        self.at, self.w, self.wbuf, self.s = at, w, wbuf, s
        self.rel = [self.shard(0, 3), self.shard(0, 1), self.shard(0, 2)] + [self.shard(1, d) for d in (0, 3, 1, 2)]
        self.mine = self.shard(0, 0)

    def shard(self, flip, dy):
        return (self.at.xl + flip) % 2 * 4 + (self.at.y + dy) % 4

    def rows(self, part, core=None):
        core = self.at.c if core is None else core
        odd = self.at.z % 2
        base = core * (2 * EDGE_SMALL + EDGE_LARGE)
        far = EDGE_SMALL + EDGE_LARGE
        if part == "a":
            start, size = base + odd * far, EDGE_SMALL
        elif part == "b":
            start, size = base + EDGE_SMALL, EDGE_LARGE
        elif part in ("a0", "a1"):
            start, size = base + odd * far + (part == "a1") * (EDGE_SMALL // 2), EDGE_SMALL // 2
        else:
            start, size = base + (1 - odd) * far, EDGE_SMALL
        return pl.ds(pl.multiple_of(start, 16), size)

    def block(self, k, part, core=None):
        return self.wbuf.at[k, self.rows(part, core)]

    def send(self, k, part, to, slot, lane):
        block = self.block(k, part)
        remote(block, block, self.s.g_send.at[0], self.s.g_ici.at[slot, lane], to).start()

    def depth_send(self, k, slot):
        self.send(k, "a0", self.at.fore, slot, 2)
        self.send(k, "a1", self.at.aft, slot, 2)

    def begin(self):
        at = self.at
        self.send(self.mine, "a", at.up, 0, 0)
        self.send(self.mine, "b", at.down, 1, 1)
        self.send(self.mine, "a", at.left, 3, 0)
        self.send(self.mine, "b", at.right, 3, 1)
        self.send(self.mine, "b", at.up, 0, 1)
        self.send(self.mine, "a", at.down, 1, 0)

    def arrive(self, slot, lane):
        block = self.block(self.rel[slot], ("a", "b", "m")[lane])
        received(block, self.s.g_ici.at[slot, lane], self.at.mate)
        remote(block, block, self.s.g_send.at[0], self.s.g_d2d.at[slot], self.at.mate).start()

    def a(self, slot, *onward):
        self.arrive(slot, 0)
        for to, there in onward:
            self.send(self.rel[slot], "a", to, there, 0)
        self.depth_send(self.rel[slot], slot)

    def b(self, slot, *onward):
        self.arrive(slot, 1)
        for to, there in onward:
            self.send(self.rel[slot], "b", to, there, 1)

    def m(self, slot):
        self.arrive(slot, 2)

    def whole(self, slot):
        half = self.wbuf.shape[1] // 2
        rows = pl.ds(pl.multiple_of((1 - self.at.c) * half, 16), half)
        received(self.wbuf.at[self.rel[slot], rows], self.s.g_d2d.at[slot], self.at.mate)

    def end(self):
        sent(self.wbuf.at[pl.ds(0, 7)], self.s.g_send.at[0], self.at.mate)


def spread(row):
    lane = lax.broadcasted_iota(jnp.int32, (row.shape[0], 128), 1)
    out = []
    for j in range(16):
        out.append(jnp.where(lane < 64, row[:, 2 * j : 2 * j + 1], row[:, 2 * j + 1 : 2 * j + 2]))
    return out


def heads(values, part):
    high = values.astype(BF16)
    low = (values - high.astype(F32)).astype(BF16)
    return dot(high, part) + dot(low, part)


class Share:
    def __init__(self, plus, minus, mate, g, lhs, acc, send, ici, d2d):
        self.plus, self.minus, self.mate, self.g, self.lhs, self.acc = plus, minus, mate, g, lhs, acc
        self.sem, self.ici, self.d2d = send, ici, d2d
        self.h = g.shape[1] // 2

    def half(self, n, part):
        return self.g.at[n, pl.ds(part * self.h, self.h)]

    def go(self, src, slot, part, to):
        remote(self.half(src, part), self.half(2 * slot, part), self.sem, self.ici.at[slot, part], to).start()

    def begin(self):
        remote(self.g.at[0], self.g.at[1], self.sem, self.d2d.at[0], self.mate).start()
        self.go(0, 3, 0, self.plus)
        self.go(0, 1, 1, self.minus)
        self.go(0, 3, 1, self.plus)
        self.go(0, 1, 0, self.minus)

    def arrive(self, slot, part):
        received(self.half(2 * slot, part), self.ici.at[slot, part], self.plus)
        block = self.half(2 * slot, part)
        remote(block, self.half(2 * slot + 1, part), self.sem, self.d2d.at[slot], self.mate).start()

    def early(self):
        self.arrive(3, 0)
        self.go(6, 2, 0, self.plus)
        self.arrive(1, 1)
        self.go(2, 2, 1, self.minus)

    def near(self):
        self.arrive(3, 1)
        self.arrive(1, 0)

    def far(self):
        self.arrive(2, 0)
        self.arrive(2, 1)

    def product(self, slot):
        received(self.g.at[2 * slot + 1], self.d2d.at[slot], self.mate)
        rhs = self.g[2 * slot : 2 * slot + 2].reshape(4 * self.h, self.g.shape[2])
        value = dot(self.lhs[slot], rhs)
        self.acc[...] = value if slot == 0 else self.acc[...] + value

    def end(self):
        h = self.acc.shape[0] // 2
        return self.acc[:h], self.acc[h:]

    def drain(self):
        sent(self.g.at[pl.ds(0, 7)], self.sem, self.mate)


class Scatter:
    def __init__(self, me, targets, src, got, send, recv):
        self.me, self.targets, self.src, self.got, self.sem, self.recv = me, targets, src, got, send, recv

    def begin(self, low, high):
        n, rows = self.src.shape[0] // 2, self.src.shape[1]
        for k in range(n):
            self.src[k] = low[k * rows : k * rows + rows].astype(BF16)
            self.src[k + n] = high[k * rows : k * rows + rows].astype(BF16)
        for d, t, target in self.targets:
            remote(self.src.at[t], self.got.at[d], self.sem, self.recv, target).start()

    def all(self):
        return self.got.at[pl.ds(1, len(self.targets))]

    def end(self):
        received(self.all(), self.recv, self.targets[0][2])
        out = self.src[self.me].astype(F32)
        for d in range(1, len(self.targets) + 1):
            out += self.got[d].astype(F32)
        return out

    def halves(self):
        out = self.end()
        h = out.shape[0] // 2
        return out[:h], out[h:]

    def drain(self):
        sent(self.all(), self.sem, self.targets[0][2])


class Ring8:
    def __init__(self, me, plus, minus, src, got, send, recv):
        self.me, self.src, self.got, self.sem, self.recv = me, src, got, send, recv
        self.to = (plus, minus)
        self.h = src.shape[1] // 2

    def piece(self, way, s):
        return (self.me + (s if way == 0 else 8 - s)) % 8

    def slot(self, way, half, s):
        return (way * 2 + half) * 4 + s

    def go(self, way, half, s):
        block = self.src.at[self.piece(way, s), pl.ds(half * self.h, self.h)]
        n = self.slot(way, half, s - 1)
        remote(block, self.got.at[n], self.sem, self.recv.at[n], self.to[way]).start()

    def landed(self, way, half, s):
        n = self.slot(way, half, s)
        received(self.got.at[n], self.recv.at[n], self.to[way])
        return self.got[n].astype(F32)

    def on(self, way, half, s):
        at = self.piece(way, s)
        rows = slice(half * self.h, half * self.h + self.h)
        self.src[at, rows] = (self.src[at, rows].astype(F32) + self.landed(way, half, s)).astype(BF16)
        self.go(way, half, s)

    def far(self):
        self.go(0, 0, 4)
        self.go(1, 1, 4)

    def next_far(self, way):
        self.go(way, 1 - way, 3)

    def long(self, s):
        self.on(0, 0, s)
        self.on(1, 1, s)

    def short(self, s):
        self.on(0, 1, s)
        self.on(1, 0, s)

    def end(self):
        low = self.src[self.me, : self.h].astype(F32) + self.landed(1, 0, 0)
        high = self.src[self.me, self.h :].astype(F32) + self.landed(0, 1, 0)
        return low + self.landed(0, 0, 0), high + self.landed(1, 1, 0)

    def drain(self):
        sent(self.got.at[pl.ds(0, 14)], self.sem, self.to[0])


def kernel(r):
    at = Place()
    c, x, y, z, chip, mate = at.c, at.x, at.y, at.z, at.chip, at.mate
    first = c == 0
    own = pl.ds(c, 1)

    tok, acc, wbuf = r.tok, r.acc, r.wbuf
    count = tok.shape[0]
    depth = wbuf.shape[2]
    gather = Gather(at, r.w, wbuf, r)
    w_copy = pltpu.make_async_copy(r.w, wbuf.at[gather.mine], r.in_sem.at[0])
    tok_copy = pltpu.make_async_copy(r.tokens, tok, r.in_sem.at[1])
    g_copy = pltpu.make_async_copy(r.grad_y, r.g, r.in_sem.at[2])
    w_copy.start()
    tok_copy.start()
    g_copy.start()
    with jax.named_scope("greet"):
        at.greet()
    w_copy.wait()
    gather.begin()
    tok_copy.wait()
    scope_tok = jax.named_scope("tok")
    scope_tok.__enter__()
    tt, tt3 = r.tt, r.tt3
    for i in range(16):
        block = tok[:, i * 128 : (i + 1) * 128].astype(F32).T
        for n in range(16):
            core, xlow, yy = n // 8, n // 4 % 2, n % 4
            rows = block[n * 8 : n * 8 + 8, :]
            xx, zz = i // 8 * 2 + xlow, i % 8
            tt[core, xx, yy, zz * 8 : zz * 8 + 8, :] = rows
            tt3[core, zz, xx * 32 + yy * 8 : xx * 32 + yy * 8 + 8, :] = rows
    tb, tb3, tr, tr3 = r.tb, r.tb3, r.tr, r.tr3
    tb[...] = tt[...].astype(BF16)
    tb3[...] = tt3[...].astype(BF16)
    swap = remote(tb.at[1 - c], tr, r.tok_sem.at[0], r.tok_sem.at[1], mate)
    swap3 = remote(tb3.at[1 - c], tr3, r.tok_sem.at[2], r.tok_sem.at[3], mate)
    swap.start()
    swap3.start()
    t1, t2, t3 = r.t1, r.t2, r.t3

    def place_rows(lo, one, three):
        t3[:, :, lo : lo + 128] = three
        for i in range(4):
            for j in range(4):
                t1[i, j * 64 : j * 64 + 64, lo : lo + 128] = one[i, j]
                t2[j, i * 64 : i * 64 + 64, lo : lo + 128] = one[i, j]

    place_rows(0, tb[own][0], tb3[own][0])
    acc[...] = jnp.zeros_like(acc)

    def multiply(*ks):
        def body(i, carry):
            k = ks[0]
            for n in range(1, len(ks)):
                k = jnp.where(i == n, ks[n], k)
            acc[...] += dot_nt(tok[:, pl.ds(pl.multiple_of(k * depth, depth), depth)], wbuf[k])
            return carry

        lax.fori_loop(0, len(ks), body, 0)

    scope_tok.__exit__(None, None, None)
    ga, gb, gm, rel = gather.a, gather.b, gather.m, gather.rel
    with jax.named_scope("g1"):
        ga(0, (at.up, 2), (at.left, 4))
        gb(1, (at.down, 2), (at.right, 5))
        ga(3)
        gb(3)
    with jax.named_scope("g2"):
        gb(0, (at.right, 4))
        ga(1, (at.left, 5))
        ga(4)
        gb(5)
        gm(0)
        gm(3)
    with jax.named_scope("g3"):
        ga(2, (at.left, 6))
        gb(2, (at.right, 6))
        gb(4)
        ga(5)
        gather.whole(0)
        gather.whole(3)
        multiply(gather.mine, rel[0], rel[3])
    with jax.named_scope("g4"):
        gm(1)
        gm(4)
        ga(6)
        gb(6)
        gm(2)
        gm(5)
        gather.whole(1)
        gather.whole(4)
        multiply(rel[1], rel[4])
    with jax.named_scope("g5"):
        gm(6)
        gather.whole(2)
        gather.whole(5)
        multiply(rel[2], rel[5])
    with jax.named_scope("g6"):
        swap.wait()
        swap3.wait()
        gather.whole(6)
    with jax.named_scope("g7"):
        multiply(rel[6])

    x_r, g_r = r.x, r.g
    dte, ece, tle, cume, cumt = r.dte, r.ece, r.tle, r.cume, r.cumt
    xdt, xt, gec, yi, dxi, ds_acc = r.xdt, r.xt, r.gec, r.yi, r.dxi, r.ds_acc
    stf, sst, pst, te, ske = r.stf, r.sst, r.pst, r.te, r.ske
    tot_s, tot_r, dmsg, dr = r.tot_s, r.tot_r, r.dmsg, r.dr
    msg, rmsg, res, rres, se, hs = r.msg, r.rmsg, r.res, r.rres, r.se, r.hs
    d_sem = r.d_sem
    copies = []
    with jax.named_scope("prep"):
        bm = acc[:, INNER : INNER + 128].astype(BF16)
        cm = acc[:, INNER + 128 : INNER + 256].astype(BF16)
        rowz = jnp.zeros((1, 96), F32)
        decay_rate = jnp.concatenate([-jnp.exp(r.a_log[...]), rowz], axis=1)
        bias = jnp.concatenate([r.dt_bias[...], rowz], axis=1)
        u = jnp.concatenate([acc[:, INNER + 256 :], jnp.zeros((count, 96), F32)], axis=1) + bias
        small = jnp.exp(-jnp.abs(u))
        dt = jnp.maximum(u, 0.0) + jnp.log1p(small)
        sig = jnp.where(u >= 0, 1.0, small) / (1.0 + small)
        ti = lax.broadcasted_iota(jnp.int32, (128, 128), 0)
        si = lax.broadcasted_iota(jnp.int32, (128, 128), 1)
        keep, keep_t = ti >= si, ti <= si
        lower = jnp.where(keep, 1.0, 0.0).astype(F32)
        upper = jnp.where(keep_t, 1.0, 0.0).astype(F32)
        cum = dot(lower, decay_rate * dt, lax.Precision.HIGHEST)
        total = cum[127:128, :]
        tot_s[...] = jnp.broadcast_to(total, (8, 128))
        tot_copy = remote(tot_s, tot_r, d_sem.at[0], d_sem.at[1], mate)
        tot_copy.start()
        lane = lax.broadcasted_iota(jnp.int32, (count, 128), 1)

        def widen(arr, dst):
            for j, e in enumerate(spread(arr)):
                dst[:, j * 128 : (j + 1) * 128] = e

        widen(jnp.exp(cum), ece)
        g_copy.wait()
        gec[...] = (g_r[...].astype(F32) * ece[...]).astype(BF16)
        ct = cm.astype(F32).T.astype(BF16)

    def local_states(kind, lhs, rhs):
        for half in range(2):
            stf[kind, half] = dot(lhs, rhs[:, half * 1024 : half * 1024 + 1024])
        sst[kind] = stf[kind, pl.ds(1 - c, 1)][0].astype(BF16)
        copy = remote(sst.at[kind], pst.at[kind], d_sem.at[2 + 2 * kind], d_sem.at[3 + 2 * kind], mate)
        copy.start()
        return copy

    with jax.named_scope("states"):
        st_b = local_states(1, ct, gec)
        widen(dt, dte)
        widen(jnp.exp(total - cum), tle)
        xs = acc[:, :INNER].astype(BF16)
        x_r[...] = xs
        xd = xs.astype(F32) * dte[...]
        xdt[...] = xd.astype(BF16)
        xt[...] = (xd * tle[...]).astype(BF16)
        bt = bm.astype(F32).T.astype(BF16)
        st_copies = [local_states(0, bt, xt), st_b]
        tot_copy.wait()
        for n, arr in enumerate((tot_s, tot_r)):
            for j, e in enumerate(spread(arr[...])):
                te[n, j // 8, :, j % 8 * 128 : j % 8 * 128 + 128] = e
        for j in range(8):
            l = slice(j * 128, j * 128 + 128)
            dmsg[j] = te[0, own, :, l][0] + te[1, own, :, l][0]
        dr[pl.ds(chip, 1)] = dmsg[pl.ds(chip // 2, 1)]
        for d, t, source, target in at.others:
            remote(dmsg.at[t // 2], dr.at[chip], r.s_scan.at[0], r.r_scan.at[0], target).start()
        e_own, e_mate = jnp.exp(te[0, own][0][0:1]), jnp.exp(te[1, own][0][0:1])
        e0 = jnp.where(first, e_own, e_mate)
        e1 = jnp.where(first, e_mate, e_own)

    def send_states(kind):
        st_copies[kind].wait()
        mine, theirs = stf[kind, own][0], pst[kind].astype(F32)
        early = jnp.where(first, mine, theirs)
        late = jnp.where(first, theirs, mine)
        whole = (e1 * early + late if kind == 0 else early + e0 * late).astype(BF16)
        for i in range(16):
            msg[kind, i] = whole[i % 2 * 64 : i % 2 * 64 + 64, i // 2 * 128 : i // 2 * 128 + 128]
        for d, t, source, target in at.others:
            remote(msg.at[kind, t], rmsg.at[kind, chip], r.s_scan.at[1 + kind], r.r_scan.at[1 + kind], target).start()
        rmsg[kind, pl.ds(chip, 1)] = msg[kind, pl.ds(chip, 1)]

    def scan_states(kind):
        if kind == 1:
            received(dr.at[pl.ds(0, 15)], r.r_scan.at[0], mate)
        received(rmsg.at[kind, pl.ds(0, 15)], r.r_scan.at[1 + kind], mate)
        state = jnp.zeros((64, 128), F32)
        for i in range(16) if kind == 0 else reversed(range(16)):
            res[kind, i] = state.astype(BF16)
            state = jnp.exp(dr[i][0:1]) * state + rmsg[kind, i].astype(F32)
        for d, t, source, target in at.others:
            remote(res.at[kind, t], rres.at[kind, chip], r.s_scan.at[3 + kind], r.r_scan.at[3 + kind], target).start()
        rres[kind, pl.ds(chip, 1)] = res[kind, pl.ds(chip, 1)]

    def take_states(kind):
        received(rres.at[kind, pl.ds(0, 15)], r.r_scan.at[3 + kind], mate)
        for j in range(8):
            l = slice(j * 128, j * 128 + 128)
            got = jnp.concatenate([rres[kind, 2 * j], rres[kind, 2 * j + 1]], axis=0).astype(F32)
            mine, theirs = stf[kind, own, :, l][0], pst[kind, :, l].astype(F32)
            if kind == 0:
                edge, inside = got, e0[:, l] * got + jnp.where(first, mine, theirs)
                low, high = edge, inside
            else:
                edge, inside = got, jnp.where(first, theirs, mine) + e1[:, l] * got
                low, high = inside, edge
            se[kind, own, :, l] = jnp.where(first, low, high).astype(BF16)[None]
            hs[kind, :, l] = jnp.where(first, high, low).astype(BF16)
        copy = remote(hs.at[kind], se.at[kind, c], d_sem.at[6 + 2 * kind], d_sem.at[7 + 2 * kind], mate)
        copy.start()
        copies.append(copy)

    def mate_states(kind):
        remote(hs.at[kind], se.at[kind, 1 - c], d_sem.at[6 + 2 * kind], d_sem.at[7 + 2 * kind], mate).wait_recv()

    with jax.named_scope("send_b"):
        send_states(1)
    with jax.named_scope("send_f"):
        send_states(0)

    with jax.named_scope("pairs_prep"):
        cumt[...] = cum.T
        scores = dot_nt(cm, bm)
        scores_t = dot_nt(bm, cm)
        ds_acc[...] = jnp.zeros_like(ds_acc)
        for j, e in enumerate(spread(jnp.broadcast_to(jnp.concatenate([r.d_skip[...], rowz], axis=1), (8, 128)))):
            ske[:, j * 128 : (j + 1) * 128] = e
        for h in range(32):
            cume[:, h * 128 : h * 128 + 128] = jnp.broadcast_to(cum[:, h : h + 1], (count, 128))

    def pair(j, carry):
        cols = pl.ds(pl.multiple_of(j * 128, 128), 128)
        xj = xdt[:, cols]
        gj = g_r[:, cols]
        none = jnp.zeros_like(xj)
        xx = jnp.concatenate([jnp.where(lane < 64, xj, none), jnp.where(lane < 64, none, xj)], axis=0)
        gg = jnp.concatenate([jnp.where(lane < 64, gj, none), jnp.where(lane < 64, none, gj)], axis=0)
        ww = dot_nt(gg, xj)
        mix, mix_t = [], []
        total_ds = ds_acc[...]
        for n in range(2):
            span = cume[:, pl.ds(pl.multiple_of(j * 256 + n * 128, 128), 128)] - cumt[pl.ds(2 * j + n, 1), :]
            decay = jnp.exp(jnp.where(keep, span, -1e30))
            decay_t = jnp.exp(jnp.where(keep_t, -span, -1e30))
            mix.append((scores * decay).astype(BF16))
            mix_t.append((scores_t * decay_t).astype(BF16))
            total_ds += ww[n * 128 : n * 128 + 128] * decay
        ds_acc[...] = total_ds
        yi[:, cols] = dot(jnp.concatenate(mix, axis=1), xx)
        dxi[:, cols] = dot(jnp.concatenate(mix_t, axis=1), gg)
        return carry

    by_y = [(d, (y + d) % 4, {"y": (y + d) % 4}) for d in (2, 1, 3)]
    by_x = [(d, (x + d) % 4, along_x((x + d) % 4)) for d in (2, 1, 3)]
    with jax.named_scope("pairs1"):
        place_rows(128, tr[...], tr3[...])
        for n, (t, l, me, targets) in enumerate(((t2, r.ly, y, by_y), (t1, r.lx, x, by_x))):
            for d, to, target in targets:
                remote(t.at[to], l.at[4 - d], r.t_sem.at[n], r.t_sem.at[2 + n], target).start()
            l[0] = t[me]
        lax.fori_loop(0, 6, pair, 0)
    with jax.named_scope("scan_b"):
        scan_states(1)
    with jax.named_scope("pairs2"):
        lax.fori_loop(6, 11, pair, 0)
    with jax.named_scope("scan_f"):
        scan_states(0)
    with jax.named_scope("pairs3"):
        lax.fori_loop(11, 16, pair, 0)
        ds = ds_acc[...]
        ds_t = ds.T.astype(BF16)
        ds = ds.astype(BF16)
        grad_c = dot(ds, bm)
        grad_b = dot(ds_t, cm)
    segment = jnp.where(
        lax.broadcasted_iota(jnp.int32, (512, 128), 0) // 64 == lax.broadcasted_iota(jnp.int32, (512, 128), 1), 1.0, 0.0
    ).astype(BF16)
    y_v = r.y_out

    def place_heads(arrs):
        lane8 = lax.broadcasted_iota(jnp.int32, arrs[0].shape, 1)
        out = arrs[0]
        for q in range(1, 4):
            out = jnp.where(lane8 < 8 * q, out, pltpu.roll(arrs[q], 8 * q, 1))
        return out

    with jax.named_scope("take_b"):
        take_states(1)
        mate_states(1)

    ga, gz, gb, gv = r.ga, r.gz, r.gb, r.gv
    p2, p3 = [], []

    def x_part(q):
        half, l = q // 2, slice(q % 2 * 512, q % 2 * 512 + 512)
        cols = slice(q * 512, q * 512 + 512)
        en = se[1, half, :, l]
        xs = x_r[:, cols].astype(F32)
        dxs = tle[:, cols] * dot(bm, en)
        dxn = dxi[:, cols] + dxs
        dx = (dte[:, cols] * dxn + ske[0:1, cols] * g_r[:, cols].astype(F32)).astype(BF16)
        if q < 2:
            ga[0, :, q * 512 : q * 512 + 512] = dx
        elif q == 2:
            gz[0, :, :] = dx[:, :WZ]
            gb[0, :, :128] = dx[:, WZ:]
        else:
            gb[0, :, 128:640] = dx
        p2.append(heads(xs * dxn, segment))
        p3.append(heads(xs * dxs, segment))
        return dot_nt(xt[:, cols], en)

    share_a = Share(at.up, at.down, mate, ga, r.ly, r.acc_a, r.s_share.at[0], r.r_share.at[0], r.d_share.at[0])
    share_b = Share(at.right, at.left, mate, gb, r.lx, r.acc_b, r.s_share.at[1], r.r_share.at[1], r.d_share.at[1])
    share_v = Share(at.up, at.down, mate, gv, r.ly, r.acc_v, r.s_share.at[2], r.r_share.at[2], r.d_share.at[2])
    ring_z = Ring8(z, at.fore, at.aft, r.pz, r.got_z, r.s_share.at[3], r.rz)

    def partial(p, lhs, both, piece):
        rows = p.shape[1]
        lhs = lhs[piece].reshape(rows, 2 * count)
        p[piece] = dot(lhs, both[...].reshape(2 * count, p.shape[2])).astype(BF16)

    with jax.named_scope("x_part"):
        grad_b += x_part(0)
        grad_b += x_part(1)
        share_a.begin()
        grad_b += x_part(2)
        swap_z = remote(gz.at[0], gz.at[1], d_sem.at[10], d_sem.at[11], mate)
        swap_z.start()
        grad_b += x_part(3)
        gb[0, :, 640:] = grad_b.astype(BF16)
        share_b.begin()
    with jax.named_scope("far_z"):
        swap_z.wait()
        partial(ring_z.src, t3, gz, (z + 4) % 8)
        ring_z.far()
        for way in range(2):
            partial(ring_z.src, t3, gz, ring_z.piece(way, 3))
            ring_z.next_far(way)
        for s in (2, 1):
            for way in range(2):
                partial(ring_z.src, t3, gz, ring_z.piece(way, s))
        partial(ring_z.src, t3, gz, z)
    with jax.named_scope("take_f"):
        take_states(0)
    with jax.named_scope("early"):
        share_a.early()
        share_b.early()
    with jax.named_scope("z3"):
        ring_z.long(3)
    with jax.named_scope("mate_f"):
        mate_states(0)
    with jax.named_scope("y_part"):
        p1, he = [], []
        for q in range(4):
            half, l = q // 2, slice(q % 2 * 512, q % 2 * 512 + 512)
            cols = slice(q * 512, q * 512 + 512)
            st = se[0, half, :, l]
            xs = x_r[:, cols].astype(F32)
            yo = yi[:, cols] + ece[:, cols] * dot(cm, st)
            y_v[:, cols] = (yo + ske[0:1, cols] * xs).astype(BF16)
            p1.append(heads(g_r[:, cols].astype(F32) * yo, segment))
            both = jnp.sum(se[1, half, :, l].astype(F32) * st.astype(F32), axis=0, keepdims=True)
            he.append(heads(jnp.broadcast_to(both, (8, 512)), segment))
            grad_c += dot_nt(gec[:, cols], st)
        p1, p2 = place_heads(p1), place_heads(p2)
        last = jnp.sum(dt * place_heads(p3), axis=0, keepdims=True) + jnp.exp(total) * place_heads(he)[0:1]
        dloga = dot(upper, p1 - dt * p2, lax.Precision.HIGHEST) + last
        draw = (p2 + decay_rate * dloga) * sig
        gv[0, :, :128] = grad_c.astype(BF16)
        gv[0, :, 128:] = draw[:, :32].astype(BF16)
        share_v.begin()
    gt_v = r.gt_out

    def grad_tokens(k, carry):
        w = wbuf[k]
        cols = pl.ds(pl.multiple_of(k * 256, 256), 256)
        out = dot(ga[0], w[:WA]) + dot(gz[0], w[WA : WA + WZ])
        out += dot(gb[0], w[WA + WZ : WA + WZ + WB]) + dot(gv[0], w[WA + WZ + WB :])
        gt_v[:, cols] = out.astype(BF16)
        return carry

    with jax.named_scope("near"):
        share_a.near()
        share_b.near()
        ring_z.short(2)
        ring_z.long(2)
    with jax.named_scope("prod"):
        for n, l in ((0, r.ly), (1, r.lx)):
            received(l.at[pl.ds(1, 3)], r.t_sem.at[2 + n], mate)
        for slot in (0, 3, 1):
            share_a.product(slot)
            share_b.product(slot)
    with jax.named_scope("far"):
        share_v.early()
        share_a.far()
        share_b.far()
        ring_z.short(1)
        share_v.near()
        ring_z.long(1)

    by_z = [(d, (z + d) % 8, {"z": (z + d) % 8}) for d in (4, 3, 5, 2, 6, 1, 7)]
    def scatter(n, me, targets, src, got):
        return Scatter(me, targets, src, got, r.s_last.at[n], r.r_last.at[n])

    mid_a = scatter(0, x, by_x, r.qa, r.got_a)
    mid_b = scatter(1, y, by_y, r.qb, r.got_b)
    mid_v = scatter(2, x, by_x, r.qv, r.got_v)
    mid_z = scatter(3, x, by_x, r.qz, r.got_zx)
    end_a = scatter(4, z, by_z, r.fa_s, r.fa_g)
    end_b = scatter(5, z, by_z, r.fb_s, r.fb_g)
    end_v = scatter(6, z, by_z, r.fv_s, r.fv_g)
    end_z = scatter(7, y, by_y, r.fz_s, r.fz_g)
    with jax.named_scope("end_a"):
        share_a.product(2)
        mid_a.begin(*share_a.end())
    with jax.named_scope("end_b"):
        share_b.product(2)
        mid_b.begin(*share_b.end())
    with jax.named_scope("end_v"):
        share_v.far()
        for slot in (0, 3, 1, 2):
            share_v.product(slot)
        mid_v.begin(*share_v.end())
    with jax.named_scope("end_z"):
        mid_z.begin(*ring_z.end())
    with jax.named_scope("gt1"):
        lax.fori_loop(0, 4, grad_tokens, 0)
    with jax.named_scope("mid_a"):
        end_a.begin(*mid_a.halves())
    with jax.named_scope("mid_b"):
        end_b.begin(*mid_b.halves())
    with jax.named_scope("mid_v"):
        end_v.begin(*mid_v.halves())
    with jax.named_scope("mid_z"):
        end_z.begin(*mid_z.halves())
    with jax.named_scope("gt2"):
        lax.fori_loop(4, 8, grad_tokens, 0)
    gw = r.gw_out
    with jax.named_scope("finish"):
        gw[:, :WA] = end_a.end()
        gw[:, WA + WZ : WA + WZ + WB] = end_b.end()
        gw[:, WA + WZ + WB :] = end_v.end()
        gw[:, WA : WA + WZ] = end_z.end()
    with jax.named_scope("drain"):
        for part in (gather, share_a, share_b, share_v, ring_z, mid_a, mid_b, mid_v, mid_z, end_a, end_b, end_v, end_z):
            part.end() if part is gather else part.drain()
        sent(dr.at[pl.ds(0, 15)], r.s_scan.at[0], mate)
        for n, l in ((0, r.ly), (1, r.lx)):
            sent(l.at[pl.ds(1, 3)], r.t_sem.at[n], mate)
        for kind in range(2):
            sent(rmsg.at[kind, pl.ds(0, 15)], r.s_scan.at[1 + kind], mate)
            sent(rres.at[kind, pl.ds(0, 15)], r.s_scan.at[3 + kind], mate)
        for copy in copies:
            copy.wait_send()


def fused(tokens, w, a_log, dt_bias, d_skip, grad_y):
    count = tokens.shape[0]
    cols, depth = w.shape
    sd = jax.ShapeDtypeStruct
    dma = pltpu.SemaphoreType.DMA
    scratch = dict(
        tok=((count, 2048), BF16), g=((count, INNER), BF16), wbuf=((8, cols, depth), BF16), acc=((count, cols), F32),
        tt=((2, 4, 4, 64, count), F32), tt3=((2, 8, 128, count), F32),
        tb=((2, 4, 4, 64, count), BF16), tb3=((2, 8, 128, count), BF16),
        tr=((4, 4, 64, count), BF16), tr3=((8, 128, count), BF16),
        t1=((4, 256, 2 * count), BF16), t2=((4, 256, 2 * count), BF16), lx=((4, 256, 2 * count), BF16), ly=((4, 256, 2 * count), BF16), t3=((8, 128, 2 * count), BF16),
        x=((count, INNER), BF16),
        dte=((count, INNER), F32), ece=((count, INNER), F32), tle=((count, INNER), F32),
        cume=((count, 2 * INNER), F32), cumt=((128, count), F32),
        xdt=((count, INNER), BF16), xt=((count, INNER), BF16), gec=((count, INNER), BF16),
        yi=((count, INNER), F32), dxi=((count, INNER), F32), ds_acc=((128, 128), F32),
        stf=((2, 2, 128, 1024), F32), sst=((2, 128, 1024), BF16), pst=((2, 128, 1024), BF16),
        tot_s=((8, 128), F32), tot_r=((8, 128), F32), te=((2, 2, 8, 1024), F32),
        dmsg=((8, 8, 128), F32), dr=((16, 8, 128), F32),
        msg=((2, 16, 64, 128), BF16), rmsg=((2, 16, 64, 128), BF16),
        res=((2, 16, 64, 128), BF16), rres=((2, 16, 64, 128), BF16),
        se=((2, 2, 128, 1024), BF16), hs=((2, 128, 1024), BF16), ske=((8, INNER), F32),
        ga=((8, count, WA), BF16), gb=((8, count, WB), BF16), gv=((8, count, WV), BF16), gz=((2, count, WZ), BF16),
        acc_a=((256, WA), F32), acc_b=((256, WB), F32), acc_v=((256, WV), F32),
        pz=((8, 128, WZ), BF16), got_z=((16, 64, WZ), BF16),
        qa=((4, 64, WA), BF16), qb=((4, 64, WB), BF16), qv=((4, 64, WV), BF16), qz=((4, 32, WZ), BF16),
        got_a=((4, 64, WA), BF16), got_b=((4, 64, WB), BF16), got_v=((4, 64, WV), BF16), got_zx=((4, 32, WZ), BF16),
        fa_s=((8, 8, WA), BF16), fa_g=((8, 8, WA), BF16), fb_s=((8, 8, WB), BF16), fb_g=((8, 8, WB), BF16),
        fv_s=((8, 8, WV), BF16), fv_g=((8, 8, WV), BF16), fz_s=((4, 8, WZ), BF16), fz_g=((4, 8, WZ), BF16),
    )
    sems = dict(
        in_sem=(3,), tok_sem=(4,), g_send=(1,), g_ici=(7, 3), g_d2d=(7,), d_sem=(12,), s_scan=(5,), r_scan=(5,),
        t_sem=(4,), s_share=(4,), r_share=(3, 4, 2), d_share=(3, 4), rz=(16,), s_last=(8,), r_last=(8,),
    )

    def body(tokens, w, a_log, dt_bias, d_skip, grad_y, y_out, gt_out, gw_out, *rest):
        r = SimpleNamespace(**dict(zip([*scratch, *sems], rest)))
        r.tokens, r.w, r.a_log, r.dt_bias, r.d_skip, r.grad_y = tokens, w, a_log, dt_bias, d_skip, grad_y
        r.y_out, r.gt_out, r.gw_out = y_out, gt_out, gw_out
        kernel(r)

    return pl.pallas_call(
        body,
        out_shape=(pltpu.VMEM((count, INNER), BF16), pltpu.VMEM((count, 2048), BF16), pltpu.VMEM((8, cols), F32)),
        in_specs=[ANY, ANY, VM, VM, VM, ANY],
        out_specs=(VM, VM, VM),
        scratch_shapes=[pltpu.VMEM(*v) for v in scratch.values()] + [dma(v) for v in sems.values()],
        compiler_params=pltpu.CompilerParams(collective_id=0, has_side_effects=True, vmem_limit_bytes=LIMIT),
    )(tokens, w, a_log.reshape(1, -1), dt_bias.reshape(1, -1), d_skip.reshape(1, -1), grad_y)


def per_device(tokens, w_in, a_log, dt_bias, d_skip, grad_y):
    count, width = tokens.shape[1:]
    inner = grad_y.shape[2]
    y, gt, gw = fused(tokens.reshape(count, width), w_in.T, a_log, dt_bias, d_skip, grad_y.reshape(count, inner))
    return (y.reshape(1, count, inner), gt.reshape(1, count, width), gw)


def solution(mesh):
    torus = Mesh(mesh.devices.reshape(2, 8, 2, 2, 4), ("xh", "z", "c", "xl", "y"))
    placed = (P(ZERO, SEQ, None), P(ZERO, None), P(), P(), P(), P(ZERO, SEQ, None))
    return jax.shard_map(
        per_device,
        mesh=torus,
        in_specs=placed,
        out_specs=(P(ZERO, SEQ, None), P(ZERO, SEQ, None), P(SEQ + ZERO, None)),
        check_vma=False,
    )
```

```python
from types import SimpleNamespace

import jax
import jax.numpy as jnp
from jax import lax
from jax.experimental import pallas as pl
from jax.experimental.pallas import tpu as pltpu
from jax.sharding import Mesh
from jax.sharding import PartitionSpec as P

SEQ = ("xh", "z", "c")
ZERO = ("xl", "y")
MESH = pl.DeviceIdType.MESH
F32 = jnp.float32
BF16 = jnp.bfloat16
LIMIT = 62 * 1024 * 1024
VM = pl.BlockSpec(memory_space=pltpu.VMEM)
ANY = pl.BlockSpec(memory_space=pl.ANY)
INNER = 2048
EDGE_SMALL, EDGE_LARGE = 384, 400
WA, WZ, WB, WV = 896, 512, 768, 160
PARTS = ((0, 0, 512), (0, 512, 896), (1, 0, 384), (1, 384, 768), (2, 0, 160))


def remote(src, dst, send, recv, target):
    return pltpu.make_async_remote_copy(
        src_ref=src, dst_ref=dst, send_sem=send, recv_sem=recv, device_id=target, device_id_type=MESH
    )


def sent(block, sem, target):
    remote(block, block, sem, sem, target).wait_send()


def received(block, sem, target):
    remote(block, block, sem, sem, target).wait_recv()


def along_x(x):
    return {"xh": x // 2, "xl": x % 2}


def dot(a, b, precision=None):
    return jnp.dot(a, b, preferred_element_type=F32, precision=precision)


def dot_nt(a, b):
    return lax.dot_general(a, b, (((1,), (1,)), ((), ())), preferred_element_type=F32)


class Place:
    def __init__(self):
        self.xh, self.z, self.c, self.xl, self.y = (lax.axis_index(a) for a in ("xh", "z", "c", "xl", "y"))
        self.x = self.xh * 2 + self.xl
        self.chip = self.xh * 8 + self.z
        self.right, self.left = along_x((self.x + 1) % 4), along_x((self.x + 3) % 4)
        self.up, self.down = {"y": (self.y + 1) % 4}, {"y": (self.y + 3) % 4}
        self.fore, self.aft = {"z": (self.z + 1) % 8}, {"z": (self.z + 7) % 8}
        self.mate = {"c": 1 - self.c}
        self.others = []
        for d in (4, 12, 3, 5, 11, 13, 2, 6, 10, 14, 8, 1, 7, 9, 15):
            t = (self.chip + d) % 16
            self.others.append((d, t, (self.chip + 16 - d) % 16, {"xh": t // 8, "z": t % 8}))

    def greet(self):
        barrier = pltpu.get_barrier_semaphore()
        targets = [self.mate, self.right, self.left, self.up, self.down, {"y": (self.y + 2) % 4}] + [o[3] for o in self.others]
        for target in targets:
            pl.semaphore_signal(barrier, inc=1, device_id=target, device_id_type=MESH)
        pl.semaphore_wait(barrier, len(targets))


class Gather:
    def __init__(self, at, w, wbuf, s):
        self.at, self.w, self.wbuf, self.s = at, w, wbuf, s
        self.rel = [self.shard(0, 3), self.shard(0, 1), self.shard(0, 2)] + [self.shard(1, d) for d in (0, 3, 1, 2)]
        self.mine = self.shard(0, 0)

    def shard(self, flip, dy):
        return (self.at.xl + flip) % 2 * 4 + (self.at.y + dy) % 4

    def rows(self, part, core=None):
        core = self.at.c if core is None else core
        odd = self.at.z % 2
        base = core * (2 * EDGE_SMALL + EDGE_LARGE)
        far = EDGE_SMALL + EDGE_LARGE
        if part == "a":
            start, size = base + odd * far, EDGE_SMALL
        elif part == "b":
            start, size = base + EDGE_SMALL, EDGE_LARGE
        elif part in ("a0", "a1"):
            start, size = base + odd * far + (part == "a1") * (EDGE_SMALL // 2), EDGE_SMALL // 2
        else:
            start, size = base + (1 - odd) * far, EDGE_SMALL
        return pl.ds(pl.multiple_of(start, 16), size)

    def block(self, k, part, core=None):
        return self.wbuf.at[k, self.rows(part, core)]

    def send(self, k, part, to, slot, lane):
        block = self.block(k, part)
        remote(block, block, self.s.g_send.at[0], self.s.g_ici.at[slot, lane], to).start()

    def depth_send(self, k, slot):
        self.send(k, "a0", self.at.fore, slot, 2)
        self.send(k, "a1", self.at.aft, slot, 2)

    def begin(self):
        at = self.at
        self.send(self.mine, "a", at.up, 0, 0)
        self.send(self.mine, "b", at.down, 1, 1)
        self.send(self.mine, "a", at.left, 3, 0)
        self.send(self.mine, "b", at.right, 3, 1)
        self.send(self.mine, "b", at.up, 0, 1)
        self.send(self.mine, "a", at.down, 1, 0)

    def arrive(self, slot, lane):
        block = self.block(self.rel[slot], ("a", "b", "m")[lane])
        received(block, self.s.g_ici.at[slot, lane], self.at.mate)
        remote(block, block, self.s.g_send.at[0], self.s.g_d2d.at[slot], self.at.mate).start()

    def a(self, slot, *onward):
        self.arrive(slot, 0)
        for to, there in onward:
            self.send(self.rel[slot], "a", to, there, 0)
        self.depth_send(self.rel[slot], slot)

    def b(self, slot, *onward):
        self.arrive(slot, 1)
        for to, there in onward:
            self.send(self.rel[slot], "b", to, there, 1)

    def m(self, slot):
        self.arrive(slot, 2)

    def whole(self, slot):
        half = self.wbuf.shape[1] // 2
        rows = pl.ds(pl.multiple_of((1 - self.at.c) * half, 16), half)
        received(self.wbuf.at[self.rel[slot], rows], self.s.g_d2d.at[slot], self.at.mate)

    def end(self):
        sent(self.wbuf.at[pl.ds(0, 7)], self.s.g_send.at[0], self.at.mate)


def spread(row):
    lane = lax.broadcasted_iota(jnp.int32, (row.shape[0], 128), 1)
    out = []
    for j in range(16):
        out.append(jnp.where(lane < 64, row[:, 2 * j : 2 * j + 1], row[:, 2 * j + 1 : 2 * j + 2]))
    return out


def heads(values, part):
    high = values.astype(BF16)
    low = (values - high.astype(F32)).astype(BF16)
    return dot(high, part) + dot(low, part)


class Share:
    def __init__(self, plus, minus, mate, g, lhs, acc, send, ici, d2d):
        self.plus, self.minus, self.mate, self.g, self.lhs, self.acc = plus, minus, mate, g, lhs, acc
        self.sem, self.ici, self.d2d = send, ici, d2d
        self.h = g.shape[1] // 2

    def half(self, n, part):
        return self.g.at[n, pl.ds(part * self.h, self.h)]

    def go(self, src, slot, part, to):
        remote(self.half(src, part), self.half(2 * slot, part), self.sem, self.ici.at[slot, part], to).start()

    def begin(self):
        remote(self.g.at[0], self.g.at[1], self.sem, self.d2d.at[0], self.mate).start()
        self.go(0, 3, 0, self.plus)
        self.go(0, 1, 1, self.minus)
        self.go(0, 3, 1, self.plus)
        self.go(0, 1, 0, self.minus)

    def arrive(self, slot, part):
        received(self.half(2 * slot, part), self.ici.at[slot, part], self.plus)
        block = self.half(2 * slot, part)
        remote(block, self.half(2 * slot + 1, part), self.sem, self.d2d.at[slot], self.mate).start()

    def early(self):
        self.arrive(3, 0)
        self.go(6, 2, 0, self.plus)
        self.arrive(1, 1)
        self.go(2, 2, 1, self.minus)

    def near(self):
        self.arrive(3, 1)
        self.arrive(1, 0)

    def far(self):
        self.arrive(2, 0)
        self.arrive(2, 1)

    def product(self, slot):
        received(self.g.at[2 * slot + 1], self.d2d.at[slot], self.mate)
        rhs = self.g[2 * slot : 2 * slot + 2].reshape(4 * self.h, self.g.shape[2])
        value = dot(self.lhs[slot], rhs)
        self.acc[...] = value if slot == 0 else self.acc[...] + value

    def end(self, lo, hi):
        h = self.acc.shape[0] // 2
        return self.acc[:h, lo:hi], self.acc[h:, lo:hi]

    def drain(self):
        sent(self.g.at[pl.ds(0, 7)], self.sem, self.mate)


class Scatter:
    def __init__(self, me, targets, src, got, send, recv):
        self.me, self.targets, self.src, self.got, self.sem, self.recv = me, targets, src, got, send, recv

    def begin(self, low, high):
        n, rows = self.src.shape[0] // 2, self.src.shape[1]
        for k in range(n):
            self.src[k] = low[k * rows : k * rows + rows].astype(BF16)
            self.src[k + n] = high[k * rows : k * rows + rows].astype(BF16)
        for d, t, target in self.targets:
            remote(self.src.at[t], self.got.at[d], self.sem, self.recv, target).start()

    def all(self):
        return self.got.at[pl.ds(1, len(self.targets))]

    def end(self):
        received(self.all(), self.recv, self.targets[0][2])
        out = self.src[self.me].astype(F32)
        for d in range(1, len(self.targets) + 1):
            out += self.got[d].astype(F32)
        return out

    def halves(self):
        out = self.end()
        h = out.shape[0] // 2
        return out[:h], out[h:]

    def drain(self):
        sent(self.all(), self.sem, self.targets[0][2])


class Ring8:
    def __init__(self, me, plus, minus, src, got, send, recv):
        self.me, self.src, self.got, self.sem, self.recv = me, src, got, send, recv
        self.to = (plus, minus)
        self.h = src.shape[1] // 2

    def piece(self, way, s):
        return (self.me + (s if way == 0 else 8 - s)) % 8

    def slot(self, way, half, s):
        return (way * 2 + half) * 4 + s

    def go(self, way, half, s):
        block = self.src.at[self.piece(way, s), pl.ds(half * self.h, self.h)]
        n = self.slot(way, half, s - 1)
        remote(block, self.got.at[n], self.sem, self.recv.at[n], self.to[way]).start()

    def landed(self, way, half, s):
        n = self.slot(way, half, s)
        received(self.got.at[n], self.recv.at[n], self.to[way])
        return self.got[n].astype(F32)

    def on(self, way, half, s):
        at = self.piece(way, s)
        rows = slice(half * self.h, half * self.h + self.h)
        self.src[at, rows] = (self.src[at, rows].astype(F32) + self.landed(way, half, s)).astype(BF16)
        self.go(way, half, s)

    def far(self):
        self.go(0, 0, 4)
        self.go(1, 1, 4)

    def next_far(self, way):
        self.go(way, 1 - way, 3)

    def long(self, s):
        self.on(0, 0, s)
        self.on(1, 1, s)

    def short(self, s):
        self.on(0, 1, s)
        self.on(1, 0, s)

    def end(self):
        low = self.src[self.me, : self.h].astype(F32) + self.landed(1, 0, 0)
        high = self.src[self.me, self.h :].astype(F32) + self.landed(0, 1, 0)
        return low + self.landed(0, 0, 0), high + self.landed(1, 1, 0)

    def drain(self):
        sent(self.got.at[pl.ds(0, 14)], self.sem, self.to[0])


def kernel(r):
    at = Place()
    c, x, y, z, chip, mate = at.c, at.x, at.y, at.z, at.chip, at.mate
    first = c == 0
    own = pl.ds(c, 1)

    tok, acc, wbuf = r.tok, r.acc, r.wbuf
    count = tok.shape[0]
    depth = wbuf.shape[2]
    gather = Gather(at, r.w, wbuf, r)
    w_copy = pltpu.make_async_copy(r.w, wbuf.at[gather.mine], r.in_sem.at[0])
    tok_copy = pltpu.make_async_copy(r.tokens, tok, r.in_sem.at[1])
    g_copy = pltpu.make_async_copy(r.grad_y, r.g, r.in_sem.at[2])
    w_copy.start()
    tok_copy.start()
    g_copy.start()
    with jax.named_scope("greet"):
        at.greet()
    w_copy.wait()
    gather.begin()
    tok_copy.wait()
    scope_tok = jax.named_scope("tok")
    scope_tok.__enter__()
    tt, tt3 = r.tt, r.tt3
    for i in range(16):
        block = tok[:, i * 128 : (i + 1) * 128].astype(F32).T
        for n in range(16):
            core, xlow, yy = n // 8, n // 4 % 2, n % 4
            rows = block[n * 8 : n * 8 + 8, :]
            xx, zz = i // 8 * 2 + xlow, i % 8
            tt[core, xx, yy, zz * 8 : zz * 8 + 8, :] = rows
            tt3[core, zz, xx * 32 + yy * 8 : xx * 32 + yy * 8 + 8, :] = rows
    tb, tb3, tr, tr3 = r.tb, r.tb3, r.tr, r.tr3
    tb[...] = tt[...].astype(BF16)
    tb3[...] = tt3[...].astype(BF16)
    swap = remote(tb.at[1 - c], tr, r.tok_sem.at[0], r.tok_sem.at[1], mate)
    swap3 = remote(tb3.at[1 - c], tr3, r.tok_sem.at[2], r.tok_sem.at[3], mate)
    swap.start()
    swap3.start()
    t1, t2, t3 = r.t1, r.t2, r.t3

    def place_rows(lo, one, three):
        t3[:, :, lo : lo + 128] = three
        for i in range(4):
            for j in range(4):
                t1[i, j * 64 : j * 64 + 64, lo : lo + 128] = one[i, j]
                t2[j, i * 64 : i * 64 + 64, lo : lo + 128] = one[i, j]

    place_rows(0, tb[own][0], tb3[own][0])
    acc[...] = jnp.zeros_like(acc)

    def multiply(*ks):
        def body(i, carry):
            k = ks[0]
            for n in range(1, len(ks)):
                k = jnp.where(i == n, ks[n], k)
            acc[...] += dot_nt(tok[:, pl.ds(pl.multiple_of(k * depth, depth), depth)], wbuf[k])
            return carry

        lax.fori_loop(0, len(ks), body, 0)

    scope_tok.__exit__(None, None, None)
    ga, gb, gm, rel = gather.a, gather.b, gather.m, gather.rel
    with jax.named_scope("g1"):
        ga(0, (at.up, 2), (at.left, 4))
        gb(1, (at.down, 2), (at.right, 5))
        ga(3)
        gb(3)
    with jax.named_scope("g2"):
        gb(0, (at.right, 4))
        ga(1, (at.left, 5))
        ga(4)
        gb(5)
        gm(0)
        gm(3)
    with jax.named_scope("g3"):
        ga(2, (at.left, 6))
        gb(2, (at.right, 6))
        swap.wait()
        swap3.wait()
        place_rows(128, tr[...], tr3[...])
        gb(4)
        ga(5)
        gather.whole(0)
        gather.whole(3)
        multiply(gather.mine, rel[0], rel[3])
    with jax.named_scope("g4"):
        gm(1)
        gm(4)
        ga(6)
        gb(6)
        by_y = [(d, (y + d) % 4, {"y": (y + d) % 4}) for d in (2, 1, 3)]
        by_x = [(d, (x + d) % 4, along_x((x + d) % 4)) for d in (2, 1, 3)]
        for n, (t, l, me, targets) in enumerate(((t2, r.ly, y, by_y), (t1, r.lx, x, by_x))):
            for d, to, target in targets:
                remote(t.at[to], l.at[4 - d], r.t_sem.at[n], r.t_sem.at[2 + n], target).start()
            l[0] = t[me]
        gm(2)
        gm(5)
        gather.whole(1)
        gather.whole(4)
        multiply(rel[1], rel[4])
    with jax.named_scope("g5"):
        gm(6)
        gather.whole(2)
        gather.whole(5)
        multiply(rel[2], rel[5])
    with jax.named_scope("g6"):
        gather.whole(6)
    last_tok = tok[:, pl.ds(pl.multiple_of(rel[6] * depth, depth), depth)]
    with jax.named_scope("g7"):
        acc[:, INNER:] += dot_nt(last_tok, wbuf[rel[6], INNER:])

    x_r, g_r = r.x, r.g
    dte, ece, tle, cume, cumt = r.dte, r.ece, r.tle, r.cume, r.cumt
    xdt, xt, gec, yi, dxi, ds_acc = r.xdt, r.xt, r.gec, r.yi, r.dxi, r.ds_acc
    stf, sst, pst, te, ske = r.stf, r.sst, r.pst, r.te, r.ske
    tot_s, tot_r, dmsg, dr = r.tot_s, r.tot_r, r.dmsg, r.dr
    msg, rmsg, res, rres, se, hs = r.msg, r.rmsg, r.res, r.rres, r.se, r.hs
    d_sem = r.d_sem
    copies = []
    with jax.named_scope("prep"):
        bm = acc[:, INNER : INNER + 128].astype(BF16)
        cm = acc[:, INNER + 128 : INNER + 256].astype(BF16)
        rowz = jnp.zeros((1, 96), F32)
        decay_rate = jnp.concatenate([-jnp.exp(r.a_log[...]), rowz], axis=1)
        bias = jnp.concatenate([r.dt_bias[...], rowz], axis=1)
        u = jnp.concatenate([acc[:, INNER + 256 :], jnp.zeros((count, 96), F32)], axis=1) + bias
        small = jnp.exp(-jnp.abs(u))
        dt = jnp.maximum(u, 0.0) + jnp.log1p(small)
        sig = jnp.where(u >= 0, 1.0, small) / (1.0 + small)
        ti = lax.broadcasted_iota(jnp.int32, (128, 128), 0)
        si = lax.broadcasted_iota(jnp.int32, (128, 128), 1)
        keep, keep_t = ti >= si, ti <= si
        lower = jnp.where(keep, 1.0, 0.0).astype(F32)
        upper = jnp.where(keep_t, 1.0, 0.0).astype(F32)
        cum = dot(lower, decay_rate * dt, lax.Precision.HIGHEST)
        total = cum[127:128, :]
        tot_s[...] = jnp.broadcast_to(total, (8, 128))
        tot_copy = remote(tot_s, tot_r, d_sem.at[0], d_sem.at[1], mate)
        tot_copy.start()
        lane = lax.broadcasted_iota(jnp.int32, (count, 128), 1)

        def widen(arr, dst):
            for j, e in enumerate(spread(arr)):
                dst[:, j * 128 : (j + 1) * 128] = e

        widen(jnp.exp(cum), ece)
        g_copy.wait()
        gec[...] = (g_r[...].astype(F32) * ece[...]).astype(BF16)
        ct = cm.astype(F32).T.astype(BF16)

    def local_states(kind, lhs, rhs):
        for half in range(2):
            stf[kind, half] = dot(lhs, rhs[:, half * 1024 : half * 1024 + 1024])
        sst[kind] = stf[kind, pl.ds(1 - c, 1)][0].astype(BF16)
        copy = remote(sst.at[kind], pst.at[kind], d_sem.at[2 + 2 * kind], d_sem.at[3 + 2 * kind], mate)
        copy.start()
        return copy

    with jax.named_scope("states"):
        st_b = local_states(1, ct, gec)
        widen(dt, dte)
        widen(jnp.exp(total - cum), tle)
        xs = (acc[:, :INNER] + dot_nt(last_tok, wbuf[rel[6], :INNER])).astype(BF16)
        x_r[...] = xs
        xd = xs.astype(F32) * dte[...]
        xdt[...] = xd.astype(BF16)
        xt[...] = (xd * tle[...]).astype(BF16)
        bt = bm.astype(F32).T.astype(BF16)
        st_copies = [local_states(0, bt, xt), st_b]
        tot_copy.wait()
        for n, arr in enumerate((tot_s, tot_r)):
            for j, e in enumerate(spread(arr[...])):
                te[n, j // 8, :, j % 8 * 128 : j % 8 * 128 + 128] = e
        for j in range(8):
            l = slice(j * 128, j * 128 + 128)
            dmsg[j] = te[0, own, :, l][0] + te[1, own, :, l][0]
        dr[pl.ds(chip, 1)] = dmsg[pl.ds(chip // 2, 1)]
        for d, t, source, target in at.others:
            remote(dmsg.at[t // 2], dr.at[chip], r.s_scan.at[0], r.r_scan.at[0], target).start()
        e_own, e_mate = jnp.exp(te[0, own][0][0:1]), jnp.exp(te[1, own][0][0:1])
        e0 = jnp.where(first, e_own, e_mate)
        e1 = jnp.where(first, e_mate, e_own)

    def send_states(kind):
        st_copies[kind].wait()
        mine, theirs = stf[kind, own][0], pst[kind].astype(F32)
        early = jnp.where(first, mine, theirs)
        late = jnp.where(first, theirs, mine)
        whole = (e1 * early + late if kind == 0 else early + e0 * late).astype(BF16)
        for i in range(16):
            msg[kind, i] = whole[i % 2 * 64 : i % 2 * 64 + 64, i // 2 * 128 : i // 2 * 128 + 128]
        for d, t, source, target in at.others:
            remote(msg.at[kind, t], rmsg.at[kind, chip], r.s_scan.at[1 + kind], r.r_scan.at[1 + kind], target).start()
        rmsg[kind, pl.ds(chip, 1)] = msg[kind, pl.ds(chip, 1)]

    def scan_states(kind):
        if kind == 1:
            received(dr.at[pl.ds(0, 15)], r.r_scan.at[0], mate)
        received(rmsg.at[kind, pl.ds(0, 15)], r.r_scan.at[1 + kind], mate)
        state = jnp.zeros((64, 128), F32)
        for i in range(16) if kind == 0 else reversed(range(16)):
            res[kind, i] = state.astype(BF16)
            state = jnp.exp(dr[i][0:1]) * state + rmsg[kind, i].astype(F32)
        for d, t, source, target in at.others:
            remote(res.at[kind, t], rres.at[kind, chip], r.s_scan.at[3 + kind], r.r_scan.at[3 + kind], target).start()
        rres[kind, pl.ds(chip, 1)] = res[kind, pl.ds(chip, 1)]

    def take_states(kind):
        received(rres.at[kind, pl.ds(0, 15)], r.r_scan.at[3 + kind], mate)
        for j in range(8):
            l = slice(j * 128, j * 128 + 128)
            got = jnp.concatenate([rres[kind, 2 * j], rres[kind, 2 * j + 1]], axis=0).astype(F32)
            mine, theirs = stf[kind, own, :, l][0], pst[kind, :, l].astype(F32)
            if kind == 0:
                edge, inside = got, e0[:, l] * got + jnp.where(first, mine, theirs)
                low, high = edge, inside
            else:
                edge, inside = got, jnp.where(first, theirs, mine) + e1[:, l] * got
                low, high = inside, edge
            se[kind, own, :, l] = jnp.where(first, low, high).astype(BF16)[None]
            hs[kind, :, l] = jnp.where(first, high, low).astype(BF16)
        copy = remote(hs.at[kind], se.at[kind, c], d_sem.at[6 + 2 * kind], d_sem.at[7 + 2 * kind], mate)
        copy.start()
        copies.append(copy)

    def mate_states(kind):
        remote(hs.at[kind], se.at[kind, 1 - c], d_sem.at[6 + 2 * kind], d_sem.at[7 + 2 * kind], mate).wait_recv()

    with jax.named_scope("send_b"):
        send_states(1)
    with jax.named_scope("pairs_prep"):
        cumt[...] = cum.T
        scores = dot_nt(cm, bm)
        scores_t = dot_nt(bm, cm)
        ds_acc[...] = jnp.zeros_like(ds_acc)
        for j, e in enumerate(spread(jnp.broadcast_to(jnp.concatenate([r.d_skip[...], rowz], axis=1), (8, 128)))):
            ske[:, j * 128 : (j + 1) * 128] = e
        for h in range(32):
            cume[:, h * 128 : h * 128 + 128] = jnp.broadcast_to(cum[:, h : h + 1], (count, 128))

    def pair(j, carry):
        cols = pl.ds(pl.multiple_of(j * 128, 128), 128)
        xj = xdt[:, cols]
        gj = g_r[:, cols]
        none = jnp.zeros_like(xj)
        xx = jnp.concatenate([jnp.where(lane < 64, xj, none), jnp.where(lane < 64, none, xj)], axis=0)
        gg = jnp.concatenate([jnp.where(lane < 64, gj, none), jnp.where(lane < 64, none, gj)], axis=0)
        ww = dot_nt(gg, xj)
        mix, mix_t = [], []
        total_ds = ds_acc[...]
        for n in range(2):
            span = cume[:, pl.ds(pl.multiple_of(j * 256 + n * 128, 128), 128)] - cumt[pl.ds(2 * j + n, 1), :]
            decay = jnp.exp(jnp.where(keep, span, -1e30))
            decay_t = jnp.exp(jnp.where(keep_t, -span, -1e30))
            mix.append((scores * decay).astype(BF16))
            mix_t.append((scores_t * decay_t).astype(BF16))
            total_ds += ww[n * 128 : n * 128 + 128] * decay
        ds_acc[...] = total_ds
        yi[:, cols] = dot(jnp.concatenate(mix, axis=1), xx)
        dxi[:, cols] = dot(jnp.concatenate(mix_t, axis=1), gg)
        return carry

    with jax.named_scope("pairs1"):
        lax.fori_loop(0, 5, pair, 0)
    with jax.named_scope("send_f"):
        send_states(0)
    with jax.named_scope("scan_b"):
        scan_states(1)
    with jax.named_scope("pairs2"):
        lax.fori_loop(5, 11, pair, 0)
    with jax.named_scope("scan_f"):
        scan_states(0)
    with jax.named_scope("pairs3"):
        lax.fori_loop(11, 16, pair, 0)
        ds = ds_acc[...]
        ds_t = ds.T.astype(BF16)
        ds = ds.astype(BF16)
        grad_c = dot(ds, bm)
        grad_b = dot(ds_t, cm)
    segment = jnp.where(
        lax.broadcasted_iota(jnp.int32, (512, 128), 0) // 64 == lax.broadcasted_iota(jnp.int32, (512, 128), 1), 1.0, 0.0
    ).astype(BF16)
    y_v = r.y_out

    def place_heads(arrs):
        lane8 = lax.broadcasted_iota(jnp.int32, arrs[0].shape, 1)
        out = arrs[0]
        for q in range(1, 4):
            out = jnp.where(lane8 < 8 * q, out, pltpu.roll(arrs[q], 8 * q, 1))
        return out

    with jax.named_scope("take_b"):
        take_states(1)
        mate_states(1)

    ga, gz, gb, gv = r.ga, r.gz, r.gb, r.gv
    p2, p3 = [], []

    def x_part(q):
        half, l = q // 2, slice(q % 2 * 512, q % 2 * 512 + 512)
        cols = slice(q * 512, q * 512 + 512)
        en = se[1, half, :, l]
        xs = x_r[:, cols].astype(F32)
        dxs = tle[:, cols] * dot(bm, en)
        dxn = dxi[:, cols] + dxs
        dx = (dte[:, cols] * dxn + ske[0:1, cols] * g_r[:, cols].astype(F32)).astype(BF16)
        if q == 0:
            ga[0, :, :512] = dx
        elif q == 1:
            ga[0, :, 512:] = dx[:, :384]
            gz[0, :, :128] = dx[:, 384:]
        elif q == 2:
            gz[0, :, 128:] = dx[:, :384]
            gb[0, :, :128] = dx[:, 384:]
        else:
            gb[0, :, 128:640] = dx
        p2.append(heads(xs * dxn, segment))
        p3.append(heads(xs * dxs, segment))
        return dot_nt(xt[:, cols], en)

    share_a = Share(at.up, at.down, mate, ga, r.ly, r.acc_a, r.s_share.at[0], r.r_share.at[0], r.d_share.at[0])
    share_b = Share(at.right, at.left, mate, gb, r.lx, r.acc_b, r.s_share.at[1], r.r_share.at[1], r.d_share.at[1])
    share_v = Share(at.up, at.down, mate, gv, r.ly, r.acc_v, r.s_share.at[2], r.r_share.at[2], r.d_share.at[2])
    ring_z = Ring8(z, at.fore, at.aft, r.pz, r.got_z, r.s_share.at[3], r.rz)

    def partial(p, lhs, both, piece):
        rows = p.shape[1]
        lhs = lhs[piece].reshape(rows, 2 * count)
        p[piece] = dot(lhs, both[...].reshape(2 * count, p.shape[2])).astype(BF16)

    with jax.named_scope("x_part"):
        grad_b += x_part(0)
        grad_b += x_part(1)
        share_a.begin()
        grad_b += x_part(2)
        swap_z = remote(gz.at[0], gz.at[1], d_sem.at[10], d_sem.at[11], mate)
        swap_z.start()
        grad_b += x_part(3)
        gb[0, :, 640:] = grad_b.astype(BF16)
        share_b.begin()
    with jax.named_scope("far_z"):
        swap_z.wait()
        partial(ring_z.src, t3, gz, (z + 4) % 8)
        ring_z.far()
        for way in range(2):
            partial(ring_z.src, t3, gz, ring_z.piece(way, 3))
            ring_z.next_far(way)
        for s in (2, 1):
            for way in range(2):
                partial(ring_z.src, t3, gz, ring_z.piece(way, s))
        partial(ring_z.src, t3, gz, z)
    with jax.named_scope("take_f"):
        take_states(0)
    with jax.named_scope("early"):
        share_a.early()
        share_b.early()
    with jax.named_scope("z3"):
        ring_z.long(3)
    with jax.named_scope("mate_f"):
        mate_states(0)
    with jax.named_scope("y_part"):
        p1, he = [], []
        for q in range(4):
            half, l = q // 2, slice(q % 2 * 512, q % 2 * 512 + 512)
            cols = slice(q * 512, q * 512 + 512)
            st = se[0, half, :, l]
            xs = x_r[:, cols].astype(F32)
            yo = yi[:, cols] + ece[:, cols] * dot(cm, st)
            y_v[:, cols] = (yo + ske[0:1, cols] * xs).astype(BF16)
            p1.append(heads(g_r[:, cols].astype(F32) * yo, segment))
            both = jnp.sum(se[1, half, :, l].astype(F32) * st.astype(F32), axis=0, keepdims=True)
            he.append(heads(jnp.broadcast_to(both, (8, 512)), segment))
            grad_c += dot_nt(gec[:, cols], st)
        p1, p2 = place_heads(p1), place_heads(p2)
        last = jnp.sum(dt * place_heads(p3), axis=0, keepdims=True) + jnp.exp(total) * place_heads(he)[0:1]
        dloga = dot(upper, p1 - dt * p2, lax.Precision.HIGHEST) + last
        draw = (p2 + decay_rate * dloga) * sig
        gv[0, :, :128] = grad_c.astype(BF16)
        gv[0, :, 128:] = draw[:, :32].astype(BF16)
        share_v.begin()
    gt_v = r.gt_out

    def grad_tokens(k, carry):
        w = wbuf[k]
        cols = pl.ds(pl.multiple_of(k * 256, 256), 256)
        out = dot(ga[0], w[:WA]) + dot(gz[0], w[WA : WA + WZ])
        out += dot(gb[0], w[WA + WZ : WA + WZ + WB]) + dot(gv[0], w[WA + WZ + WB :])
        gt_v[:, cols] = out.astype(BF16)
        return carry

    with jax.named_scope("near"):
        share_a.near()
        share_b.near()
        ring_z.short(2)
        ring_z.long(2)
    with jax.named_scope("prod"):
        for n, l in ((0, r.ly), (1, r.lx)):
            received(l.at[pl.ds(1, 3)], r.t_sem.at[2 + n], mate)
        for slot in (0, 3, 1):
            share_a.product(slot)
            share_b.product(slot)
    with jax.named_scope("far"):
        share_v.early()
        share_a.far()
        share_b.far()
        ring_z.short(1)
        share_v.near()
        ring_z.long(1)

    by_z = [(d, (z + d) % 8, {"z": (z + d) % 8}) for d in (4, 3, 5, 2, 6, 1, 7)]
    def scatter(n, me, targets, src, got):
        return Scatter(me, targets, src, got, r.s_last.at[n], r.r_last.at[n])

    shares = ((share_a, x, by_x, 0), (share_b, y, by_y, WA + WZ), (share_v, x, by_x, WA + WZ + WB))
    stages = []
    for n, (k, lo, hi) in enumerate(PARTS):
        q, got, fs, fg = r.extra[4 * n : 4 * n + 4]
        share, me, targets, base = shares[k]
        mid, end = scatter(2 * n, me, targets, q, got), scatter(2 * n + 1, z, by_z, fs, fg)
        stages.append((mid, end, share, lo, hi, base))
    mid_z = scatter(10, x, by_x, r.qz, r.got_zx)
    end_z = scatter(11, y, by_y, r.fz_s, r.fz_g)

    def enter(n):
        mid, end, share, lo, hi, base = stages[n]
        mid.begin(*share.end(lo, hi))

    with jax.named_scope("end_a"):
        share_a.product(2)
        enter(0)
        enter(1)
    with jax.named_scope("end_b"):
        share_b.product(2)
        enter(2)
        enter(3)
    with jax.named_scope("end_v"):
        share_v.far()
        for slot in (0, 3, 1, 2):
            share_v.product(slot)
        enter(4)
    with jax.named_scope("end_z"):
        mid_z.begin(*ring_z.end())
    with jax.named_scope("gt1"):
        lax.fori_loop(0, 4, grad_tokens, 0)
    with jax.named_scope("mid_1"):
        for n in (0, 2):
            stages[n][1].begin(*stages[n][0].halves())
    with jax.named_scope("mid_2"):
        for n in (1, 3):
            stages[n][1].begin(*stages[n][0].halves())
    with jax.named_scope("mid_v"):
        stages[4][1].begin(*stages[4][0].halves())
    with jax.named_scope("mid_z"):
        end_z.begin(*mid_z.halves())
    with jax.named_scope("gt2"):
        lax.fori_loop(4, 8, grad_tokens, 0)
    gw = r.gw_out
    with jax.named_scope("finish"):
        for n in (0, 2, 1, 3, 4):
            mid, end, share, lo, hi, base = stages[n]
            gw[:, base + lo : base + hi] = end.end()
        gw[:, WA : WA + WZ] = end_z.end()
    with jax.named_scope("drain"):
        gather.end()
        for part in (share_a, share_b, share_v, ring_z, mid_z, end_z):
            part.drain()
        for mid, end, *rest in stages:
            mid.drain()
            end.drain()
        sent(dr.at[pl.ds(0, 15)], r.s_scan.at[0], mate)
        for n, l in ((0, r.ly), (1, r.lx)):
            sent(l.at[pl.ds(1, 3)], r.t_sem.at[n], mate)
        for kind in range(2):
            sent(rmsg.at[kind, pl.ds(0, 15)], r.s_scan.at[1 + kind], mate)
            sent(rres.at[kind, pl.ds(0, 15)], r.s_scan.at[3 + kind], mate)
        for copy in copies:
            copy.wait_send()


def fused(tokens, w, a_log, dt_bias, d_skip, grad_y):
    count = tokens.shape[0]
    cols, depth = w.shape
    sd = jax.ShapeDtypeStruct
    dma = pltpu.SemaphoreType.DMA
    scratch = dict(
        tok=((count, 2048), BF16), g=((count, INNER), BF16), wbuf=((8, cols, depth), BF16), acc=((count, cols), F32),
        tt=((2, 4, 4, 64, count), F32), tt3=((2, 8, 128, count), F32),
        tb=((2, 4, 4, 64, count), BF16), tb3=((2, 8, 128, count), BF16),
        tr=((4, 4, 64, count), BF16), tr3=((8, 128, count), BF16),
        t1=((4, 256, 2 * count), BF16), t2=((4, 256, 2 * count), BF16), lx=((4, 256, 2 * count), BF16), ly=((4, 256, 2 * count), BF16), t3=((8, 128, 2 * count), BF16),
        x=((count, INNER), BF16),
        dte=((count, INNER), F32), ece=((count, INNER), F32), tle=((count, INNER), F32),
        cume=((count, 2 * INNER), F32), cumt=((128, count), F32),
        xdt=((count, INNER), BF16), xt=((count, INNER), BF16), gec=((count, INNER), BF16),
        yi=((count, INNER), F32), dxi=((count, INNER), F32), ds_acc=((128, 128), F32),
        stf=((2, 2, 128, 1024), F32), sst=((2, 128, 1024), BF16), pst=((2, 128, 1024), BF16),
        tot_s=((8, 128), F32), tot_r=((8, 128), F32), te=((2, 2, 8, 1024), F32),
        dmsg=((8, 8, 128), F32), dr=((16, 8, 128), F32),
        msg=((2, 16, 64, 128), BF16), rmsg=((2, 16, 64, 128), BF16),
        res=((2, 16, 64, 128), BF16), rres=((2, 16, 64, 128), BF16),
        se=((2, 2, 128, 1024), BF16), hs=((2, 128, 1024), BF16), ske=((8, INNER), F32),
        ga=((8, count, WA), BF16), gb=((8, count, WB), BF16), gv=((8, count, WV), BF16), gz=((2, count, WZ), BF16),
        acc_a=((256, WA), F32), acc_b=((256, WB), F32), acc_v=((256, WV), F32),
        pz=((8, 128, WZ), BF16), got_z=((16, 64, WZ), BF16),
        qz=((4, 32, WZ), BF16), got_zx=((4, 32, WZ), BF16), fz_s=((4, 8, WZ), BF16), fz_g=((4, 8, WZ), BF16),
    )
    sems = dict(
        in_sem=(3,), tok_sem=(4,), g_send=(1,), g_ici=(7, 3), g_d2d=(7,), d_sem=(12,), s_scan=(5,), r_scan=(5,),
        t_sem=(4,), s_share=(4,), r_share=(3, 4, 2), d_share=(3, 4), rz=(16,), s_last=(12,), r_last=(12,),
    )

    extra = []
    for k, lo, hi in PARTS:
        extra += [pltpu.VMEM((4, 64, hi - lo), BF16)] * 2 + [pltpu.VMEM((8, 8, hi - lo), BF16)] * 2

    def body(tokens, w, a_log, dt_bias, d_skip, grad_y, y_out, gt_out, gw_out, *rest):
        r = SimpleNamespace(**dict(zip([*scratch, *sems], rest)))
        r.extra = rest[len(scratch) + len(sems) :]
        r.tokens, r.w, r.a_log, r.dt_bias, r.d_skip, r.grad_y = tokens, w, a_log, dt_bias, d_skip, grad_y
        r.y_out, r.gt_out, r.gw_out = y_out, gt_out, gw_out
        kernel(r)

    return pl.pallas_call(
        body,
        out_shape=(pltpu.VMEM((count, INNER), BF16), pltpu.VMEM((count, 2048), BF16), pltpu.VMEM((8, cols), F32)),
        in_specs=[ANY, ANY, VM, VM, VM, ANY],
        out_specs=(VM, VM, VM),
        scratch_shapes=[pltpu.VMEM(*v) for v in scratch.values()] + [dma(v) for v in sems.values()] + extra,
        compiler_params=pltpu.CompilerParams(collective_id=0, has_side_effects=True, vmem_limit_bytes=LIMIT),
    )(tokens, w, a_log.reshape(1, -1), dt_bias.reshape(1, -1), d_skip.reshape(1, -1), grad_y)


def per_device(tokens, w_in, a_log, dt_bias, d_skip, grad_y):
    count, width = tokens.shape[1:]
    inner = grad_y.shape[2]
    y, gt, gw = fused(tokens.reshape(count, width), w_in.T, a_log, dt_bias, d_skip, grad_y.reshape(count, inner))
    return (y.reshape(1, count, inner), gt.reshape(1, count, width), gw)


def solution(mesh):
    torus = Mesh(mesh.devices.reshape(2, 8, 2, 2, 4), ("xh", "z", "c", "xl", "y"))
    placed = (P(ZERO, SEQ, None), P(ZERO, None), P(), P(), P(), P(ZERO, SEQ, None))
    return jax.shard_map(
        per_device,
        mesh=torus,
        in_specs=placed,
        out_specs=(P(ZERO, SEQ, None), P(ZERO, SEQ, None), P(SEQ + ZERO, None)),
        check_vma=False,
    )
```

```python
from types import SimpleNamespace

import jax
import jax.numpy as jnp
from jax import lax
from jax.experimental import pallas as pl
from jax.experimental.pallas import tpu as pltpu
from jax.sharding import Mesh
from jax.sharding import PartitionSpec as P

SEQ = ("xh", "z", "c")
ZERO = ("xl", "y")
MESH = pl.DeviceIdType.MESH
F32 = jnp.float32
BF16 = jnp.bfloat16
LIMIT = 62 * 1024 * 1024
VM = pl.BlockSpec(memory_space=pltpu.VMEM)
ANY = pl.BlockSpec(memory_space=pl.ANY)
INNER = 2048
EDGE_SMALL, EDGE_LARGE = 384, 400
WA, WZ, WB, WV = 896, 512, 768, 160
PARTS = ((0, 0, 512), (0, 512, 896), (1, 0, 384), (1, 384, 768), (2, 0, 160))


def remote(src, dst, send, recv, target):
    return pltpu.make_async_remote_copy(
        src_ref=src, dst_ref=dst, send_sem=send, recv_sem=recv, device_id=target, device_id_type=MESH
    )


def sent(block, sem, target):
    remote(block, block, sem, sem, target).wait_send()


def received(block, sem, target):
    remote(block, block, sem, sem, target).wait_recv()


def along_x(x):
    return {"xh": x // 2, "xl": x % 2}


def dot(a, b, precision=None):
    return jnp.dot(a, b, preferred_element_type=F32, precision=precision)


def dot_nt(a, b):
    return lax.dot_general(a, b, (((1,), (1,)), ((), ())), preferred_element_type=F32)


class Place:
    def __init__(self):
        self.xh, self.z, self.c, self.xl, self.y = (lax.axis_index(a) for a in ("xh", "z", "c", "xl", "y"))
        self.x = self.xh * 2 + self.xl
        self.chip = self.xh * 8 + self.z
        self.right, self.left = along_x((self.x + 1) % 4), along_x((self.x + 3) % 4)
        self.up, self.down = {"y": (self.y + 1) % 4}, {"y": (self.y + 3) % 4}
        self.fore, self.aft = {"z": (self.z + 1) % 8}, {"z": (self.z + 7) % 8}
        self.mate = {"c": 1 - self.c}
        self.others = []
        for d in (4, 12, 3, 5, 11, 13, 2, 6, 10, 14, 8, 1, 7, 9, 15):
            t = (self.chip + d) % 16
            self.others.append((d, t, (self.chip + 16 - d) % 16, {"xh": t // 8, "z": t % 8}))

    def greet(self):
        barrier = pltpu.get_barrier_semaphore()
        targets = [self.mate, self.right, self.left, self.up, self.down, {"y": (self.y + 2) % 4}] + [o[3] for o in self.others]
        for target in targets:
            pl.semaphore_signal(barrier, inc=1, device_id=target, device_id_type=MESH)
        pl.semaphore_wait(barrier, len(targets))


class Gather:
    def __init__(self, at, w, wbuf, s):
        self.at, self.w, self.wbuf, self.s = at, w, wbuf, s
        self.rel = [self.shard(0, 3), self.shard(0, 1), self.shard(0, 2)] + [self.shard(1, d) for d in (0, 3, 1, 2)]
        self.mine = self.shard(0, 0)

    def shard(self, flip, dy):
        return (self.at.xl + flip) % 2 * 4 + (self.at.y + dy) % 4

    def rows(self, part, core=None):
        core = self.at.c if core is None else core
        odd = self.at.z % 2
        base = core * (2 * EDGE_SMALL + EDGE_LARGE)
        far = EDGE_SMALL + EDGE_LARGE
        if part == "a":
            start, size = base + odd * far, EDGE_SMALL
        elif part == "b":
            start, size = base + EDGE_SMALL, EDGE_LARGE
        elif part in ("a0", "a1"):
            start, size = base + odd * far + (part == "a1") * (EDGE_SMALL // 2), EDGE_SMALL // 2
        else:
            start, size = base + (1 - odd) * far, EDGE_SMALL
        return pl.ds(pl.multiple_of(start, 16), size)

    def block(self, k, part, core=None):
        return self.wbuf.at[k, self.rows(part, core)]

    def send(self, k, part, to, slot, lane):
        block = self.block(k, part)
        remote(block, block, self.s.g_send.at[0], self.s.g_ici.at[slot, lane], to).start()

    def depth_send(self, k, slot):
        self.send(k, "a0", self.at.fore, slot, 2)
        self.send(k, "a1", self.at.aft, slot, 2)

    def begin(self):
        at = self.at
        self.send(self.mine, "a", at.up, 0, 0)
        self.send(self.mine, "b", at.down, 1, 1)
        self.send(self.mine, "a", at.left, 3, 0)
        self.send(self.mine, "b", at.right, 3, 1)
        self.send(self.mine, "b", at.up, 0, 1)
        self.send(self.mine, "a", at.down, 1, 0)

    def arrive(self, slot, lane):
        block = self.block(self.rel[slot], ("a", "b", "m")[lane])
        received(block, self.s.g_ici.at[slot, lane], self.at.mate)
        remote(block, block, self.s.g_send.at[0], self.s.g_d2d.at[slot], self.at.mate).start()

    def a(self, slot, *onward):
        self.arrive(slot, 0)
        for to, there in onward:
            self.send(self.rel[slot], "a", to, there, 0)
        self.depth_send(self.rel[slot], slot)

    def b(self, slot, *onward):
        self.arrive(slot, 1)
        for to, there in onward:
            self.send(self.rel[slot], "b", to, there, 1)

    def m(self, slot):
        self.arrive(slot, 2)

    def whole(self, slot):
        half = self.wbuf.shape[1] // 2
        rows = pl.ds(pl.multiple_of((1 - self.at.c) * half, 16), half)
        received(self.wbuf.at[self.rel[slot], rows], self.s.g_d2d.at[slot], self.at.mate)

    def end(self):
        sent(self.wbuf.at[pl.ds(0, 7)], self.s.g_send.at[0], self.at.mate)


def spread(row):
    lane = lax.broadcasted_iota(jnp.int32, (row.shape[0], 128), 1)
    out = []
    for j in range(16):
        out.append(jnp.where(lane < 64, row[:, 2 * j : 2 * j + 1], row[:, 2 * j + 1 : 2 * j + 2]))
    return out


def heads(values, part):
    high = values.astype(BF16)
    low = (values - high.astype(F32)).astype(BF16)
    return dot(high, part) + dot(low, part)


class Share:
    def __init__(self, plus, minus, mate, g, lhs, acc, send, ici, d2d):
        self.plus, self.minus, self.mate, self.g, self.lhs, self.acc = plus, minus, mate, g, lhs, acc
        self.sem, self.ici, self.d2d = send, ici, d2d
        self.h = g.shape[1] // 2

    def half(self, n, part):
        return self.g.at[n, pl.ds(part * self.h, self.h)]

    def go(self, src, slot, part, to):
        remote(self.half(src, part), self.half(2 * slot, part), self.sem, self.ici.at[slot, part], to).start()

    def begin(self):
        remote(self.g.at[0], self.g.at[1], self.sem, self.d2d.at[0], self.mate).start()
        self.go(0, 3, 0, self.plus)
        self.go(0, 1, 1, self.minus)
        self.go(0, 3, 1, self.plus)
        self.go(0, 1, 0, self.minus)

    def arrive(self, slot, part):
        received(self.half(2 * slot, part), self.ici.at[slot, part], self.plus)
        block = self.half(2 * slot, part)
        remote(block, self.half(2 * slot + 1, part), self.sem, self.d2d.at[slot], self.mate).start()

    def early(self):
        self.arrive(3, 0)
        self.go(6, 2, 0, self.plus)
        self.arrive(1, 1)
        self.go(2, 2, 1, self.minus)

    def near(self):
        self.arrive(3, 1)
        self.arrive(1, 0)

    def far(self):
        self.arrive(2, 0)
        self.arrive(2, 1)

    def product(self, slot):
        received(self.g.at[2 * slot + 1], self.d2d.at[slot], self.mate)
        rhs = self.g[2 * slot : 2 * slot + 2].reshape(4 * self.h, self.g.shape[2])
        value = dot(self.lhs[slot], rhs)
        self.acc[...] = value if slot == 0 else self.acc[...] + value

    def end(self, lo, hi):
        h = self.acc.shape[0] // 2
        return self.acc[:h, lo:hi], self.acc[h:, lo:hi]

    def drain(self):
        sent(self.g.at[pl.ds(0, 7)], self.sem, self.mate)


class Scatter:
    def __init__(self, me, targets, src, got, send, recv):
        self.me, self.targets, self.src, self.got, self.sem, self.recv = me, targets, src, got, send, recv

    def begin(self, low, high):
        n, rows = self.src.shape[0] // 2, self.src.shape[1]
        for k in range(n):
            self.src[k] = low[k * rows : k * rows + rows].astype(BF16)
            self.src[k + n] = high[k * rows : k * rows + rows].astype(BF16)
        for d, t, target in self.targets:
            remote(self.src.at[t], self.got.at[d], self.sem, self.recv, target).start()

    def all(self):
        return self.got.at[pl.ds(1, len(self.targets))]

    def end(self):
        received(self.all(), self.recv, self.targets[0][2])
        out = self.src[self.me].astype(F32)
        for d in range(1, len(self.targets) + 1):
            out += self.got[d].astype(F32)
        return out

    def halves(self):
        out = self.end()
        h = out.shape[0] // 2
        return out[:h], out[h:]

    def drain(self):
        sent(self.all(), self.sem, self.targets[0][2])


class Ring8:
    def __init__(self, me, plus, minus, src, got, send, recv):
        self.me, self.src, self.got, self.sem, self.recv = me, src, got, send, recv
        self.to = (plus, minus)
        self.h = src.shape[1] // 2

    def piece(self, way, s):
        return (self.me + (s if way == 0 else 8 - s)) % 8

    def slot(self, way, half, s):
        return (way * 2 + half) * 4 + s

    def go(self, way, half, s):
        block = self.src.at[self.piece(way, s), pl.ds(half * self.h, self.h)]
        n = self.slot(way, half, s - 1)
        remote(block, self.got.at[n], self.sem, self.recv.at[n], self.to[way]).start()

    def landed(self, way, half, s):
        n = self.slot(way, half, s)
        received(self.got.at[n], self.recv.at[n], self.to[way])
        return self.got[n].astype(F32)

    def on(self, way, half, s):
        at = self.piece(way, s)
        rows = slice(half * self.h, half * self.h + self.h)
        self.src[at, rows] = (self.src[at, rows].astype(F32) + self.landed(way, half, s)).astype(BF16)
        self.go(way, half, s)

    def far(self):
        self.go(0, 0, 4)
        self.go(1, 1, 4)

    def next_far(self, way):
        self.go(way, 1 - way, 3)

    def long(self, s):
        self.on(0, 0, s)
        self.on(1, 1, s)

    def short(self, s):
        self.on(0, 1, s)
        self.on(1, 0, s)

    def end(self):
        low = self.src[self.me, : self.h].astype(F32) + self.landed(1, 0, 0)
        high = self.src[self.me, self.h :].astype(F32) + self.landed(0, 1, 0)
        return low + self.landed(0, 0, 0), high + self.landed(1, 1, 0)

    def drain(self):
        sent(self.got.at[pl.ds(0, 14)], self.sem, self.to[0])


def kernel(r):
    at = Place()
    c, x, y, z, chip, mate = at.c, at.x, at.y, at.z, at.chip, at.mate
    first = c == 0
    own = pl.ds(c, 1)

    tok, acc, wbuf = r.tok, r.acc, r.wbuf
    count = tok.shape[0]
    depth = wbuf.shape[2]
    gather = Gather(at, r.w, wbuf, r)
    w_copy = pltpu.make_async_copy(r.w, wbuf.at[gather.mine], r.in_sem.at[0])
    tok_copy = pltpu.make_async_copy(r.tokens, tok, r.in_sem.at[1])
    g_copy = pltpu.make_async_copy(r.grad_y, r.g, r.in_sem.at[2])
    w_copy.start()
    tok_copy.start()
    g_copy.start()
    with jax.named_scope("greet"):
        at.greet()
    w_copy.wait()
    gather.begin()
    tok_copy.wait()
    scope_tok = jax.named_scope("tok")
    scope_tok.__enter__()
    tt, tt3 = r.tt, r.tt3
    for i in range(16):
        block = tok[:, i * 128 : (i + 1) * 128].astype(F32).T
        for n in range(16):
            core, xlow, yy = n // 8, n // 4 % 2, n % 4
            rows = block[n * 8 : n * 8 + 8, :]
            xx, zz = i // 8 * 2 + xlow, i % 8
            tt[core, xx, yy, zz * 8 : zz * 8 + 8, :] = rows
            tt3[core, zz, xx * 32 + yy * 8 : xx * 32 + yy * 8 + 8, :] = rows
    tb, tb3, tr, tr3 = r.tb, r.tb3, r.tr, r.tr3
    tb[...] = tt[...].astype(BF16)
    tb3[...] = tt3[...].astype(BF16)
    swap = remote(tb.at[1 - c], tr, r.tok_sem.at[0], r.tok_sem.at[1], mate)
    swap3 = remote(tb3.at[1 - c], tr3, r.tok_sem.at[2], r.tok_sem.at[3], mate)
    swap.start()
    swap3.start()
    t1, t2, t3 = r.t1, r.t2, r.t3

    def place_rows(lo, one, three):
        t3[:, :, lo : lo + 128] = three
        for i in range(4):
            for j in range(4):
                t1[i, j * 64 : j * 64 + 64, lo : lo + 128] = one[i, j]
                t2[j, i * 64 : i * 64 + 64, lo : lo + 128] = one[i, j]

    place_rows(0, tb[own][0], tb3[own][0])
    acc[...] = jnp.zeros_like(acc)

    def multiply(*ks):
        def body(i, carry):
            k = ks[0]
            for n in range(1, len(ks)):
                k = jnp.where(i == n, ks[n], k)
            acc[...] += dot_nt(tok[:, pl.ds(pl.multiple_of(k * depth, depth), depth)], wbuf[k])
            return carry

        lax.fori_loop(0, len(ks), body, 0)

    scope_tok.__exit__(None, None, None)
    ga, gb, gm, rel = gather.a, gather.b, gather.m, gather.rel
    with jax.named_scope("g1"):
        ga(0, (at.up, 2), (at.left, 4))
        gb(1, (at.down, 2), (at.right, 5))
        ga(3)
        gb(3)
    with jax.named_scope("g2"):
        gb(0, (at.right, 4))
        ga(1, (at.left, 5))
        ga(4)
        gb(5)
        gm(0)
        gm(3)
    with jax.named_scope("g3"):
        ga(2, (at.left, 6))
        gb(2, (at.right, 6))
        swap.wait()
        swap3.wait()
        place_rows(128, tr[...], tr3[...])
        gb(4)
        ga(5)
        gather.whole(0)
        gather.whole(3)
        multiply(gather.mine, rel[0], rel[3])
    with jax.named_scope("g4"):
        gm(1)
        gm(4)
        ga(6)
        gb(6)
        by_y = [(d, (y + d) % 4, {"y": (y + d) % 4}) for d in (2, 1, 3)]
        by_x = [(d, (x + d) % 4, along_x((x + d) % 4)) for d in (2, 1, 3)]
        for n, (t, l, me, targets) in enumerate(((t2, r.ly, y, by_y), (t1, r.lx, x, by_x))):
            for d, to, target in targets:
                remote(t.at[to], l.at[4 - d], r.t_sem.at[n], r.t_sem.at[2 + n], target).start()
            l[0] = t[me]
        gm(2)
        gm(5)
        gather.whole(1)
        gather.whole(4)
        multiply(rel[1], rel[4])
    with jax.named_scope("g5"):
        gm(6)
        gather.whole(2)
        gather.whole(5)
        multiply(rel[2], rel[5])
    with jax.named_scope("g6"):
        gather.whole(6)
    last_tok = tok[:, pl.ds(pl.multiple_of(rel[6] * depth, depth), depth)]
    with jax.named_scope("g7"):
        acc[:, INNER:] += dot_nt(last_tok, wbuf[rel[6], INNER:])

    x_r, g_r = r.x, r.g
    dte, ece, tle, cume, cumt = r.dte, r.ece, r.tle, r.cume, r.cumt
    xdt, xt, gec, yi, dxi, ds_acc = r.xdt, r.xt, r.gec, r.yi, r.dxi, r.ds_acc
    stf, sst, pst, te, ske = r.stf, r.sst, r.pst, r.te, r.ske
    tot_s, tot_r, dmsg, dr = r.tot_s, r.tot_r, r.dmsg, r.dr
    msg, rmsg, res, rres, se, hs = r.msg, r.rmsg, r.res, r.rres, r.se, r.hs
    d_sem = r.d_sem
    copies = []
    with jax.named_scope("prep"):
        bm = acc[:, INNER : INNER + 128].astype(BF16)
        cm = acc[:, INNER + 128 : INNER + 256].astype(BF16)
        rowz = jnp.zeros((1, 96), F32)
        decay_rate = jnp.concatenate([-jnp.exp(r.a_log[...]), rowz], axis=1)
        bias = jnp.concatenate([r.dt_bias[...], rowz], axis=1)
        u = jnp.concatenate([acc[:, INNER + 256 :], jnp.zeros((count, 96), F32)], axis=1) + bias
        small = jnp.exp(-jnp.abs(u))
        dt = jnp.maximum(u, 0.0) + jnp.log1p(small)
        sig = jnp.where(u >= 0, 1.0, small) / (1.0 + small)
        ti = lax.broadcasted_iota(jnp.int32, (128, 128), 0)
        si = lax.broadcasted_iota(jnp.int32, (128, 128), 1)
        keep, keep_t = ti >= si, ti <= si
        lower = jnp.where(keep, 1.0, 0.0).astype(F32)
        upper = jnp.where(keep_t, 1.0, 0.0).astype(F32)
        cum = dot(lower, decay_rate * dt, lax.Precision.HIGHEST)
        total = cum[127:128, :]
        tot_s[...] = jnp.broadcast_to(total, (8, 128))
        tot_copy = remote(tot_s, tot_r, d_sem.at[0], d_sem.at[1], mate)
        tot_copy.start()
        lane = lax.broadcasted_iota(jnp.int32, (count, 128), 1)

        def widen(arr, dst):
            for j, e in enumerate(spread(arr)):
                dst[:, j * 128 : (j + 1) * 128] = e

        widen(jnp.exp(cum), ece)
        g_copy.wait()
        gec[...] = (g_r[...].astype(F32) * ece[...]).astype(BF16)
        ct = cm.astype(F32).T.astype(BF16)

    def local_states(kind, lhs, rhs):
        for half in range(2):
            stf[kind, half] = dot(lhs, rhs[:, half * 1024 : half * 1024 + 1024])
        sst[kind] = stf[kind, pl.ds(1 - c, 1)][0].astype(BF16)
        copy = remote(sst.at[kind], pst.at[kind], d_sem.at[2 + 2 * kind], d_sem.at[3 + 2 * kind], mate)
        copy.start()
        return copy

    with jax.named_scope("states"):
        st_b = local_states(1, ct, gec)
        widen(dt, dte)
        widen(jnp.exp(total - cum), tle)
        xs = (acc[:, :INNER] + dot_nt(last_tok, wbuf[rel[6], :INNER])).astype(BF16)
        x_r[...] = xs
        xd = xs.astype(F32) * dte[...]
        xdt[...] = xd.astype(BF16)
        xt[...] = (xd * tle[...]).astype(BF16)
        bt = bm.astype(F32).T.astype(BF16)
        st_copies = [local_states(0, bt, xt), st_b]
        tot_copy.wait()
        for n, arr in enumerate((tot_s, tot_r)):
            for j, e in enumerate(spread(arr[...])):
                te[n, j // 8, :, j % 8 * 128 : j % 8 * 128 + 128] = e
        for j in range(8):
            l = slice(j * 128, j * 128 + 128)
            dmsg[j] = te[0, own, :, l][0] + te[1, own, :, l][0]
        dr[pl.ds(chip, 1)] = dmsg[pl.ds(chip // 2, 1)]
        for d, t, source, target in at.others:
            remote(dmsg.at[t // 2], dr.at[chip], r.s_scan.at[0], r.r_scan.at[0], target).start()
        e_own, e_mate = jnp.exp(te[0, own][0][0:1]), jnp.exp(te[1, own][0][0:1])
        e0 = jnp.where(first, e_own, e_mate)
        e1 = jnp.where(first, e_mate, e_own)

    def send_states(kind):
        st_copies[kind].wait()
        mine, theirs = stf[kind, own][0], pst[kind].astype(F32)
        early = jnp.where(first, mine, theirs)
        late = jnp.where(first, theirs, mine)
        whole = (e1 * early + late if kind == 0 else early + e0 * late).astype(BF16)
        for i in range(16):
            msg[kind, i] = whole[i % 2 * 64 : i % 2 * 64 + 64, i // 2 * 128 : i // 2 * 128 + 128]
        for d, t, source, target in at.others:
            remote(msg.at[kind, t], rmsg.at[kind, chip], r.s_scan.at[1 + kind], r.r_scan.at[1 + kind], target).start()
        rmsg[kind, pl.ds(chip, 1)] = msg[kind, pl.ds(chip, 1)]

    def scan_states(kind):
        if kind == 1:
            received(dr.at[pl.ds(0, 15)], r.r_scan.at[0], mate)
        received(rmsg.at[kind, pl.ds(0, 15)], r.r_scan.at[1 + kind], mate)
        state = jnp.zeros((64, 128), F32)
        for i in range(16) if kind == 0 else reversed(range(16)):
            res[kind, i] = state.astype(BF16)
            state = jnp.exp(dr[i][0:1]) * state + rmsg[kind, i].astype(F32)
        for d, t, source, target in at.others:
            remote(res.at[kind, t], rres.at[kind, chip], r.s_scan.at[3 + kind], r.r_scan.at[3 + kind], target).start()
        rres[kind, pl.ds(chip, 1)] = res[kind, pl.ds(chip, 1)]

    def take_states(kind):
        received(rres.at[kind, pl.ds(0, 15)], r.r_scan.at[3 + kind], mate)
        for j in range(8):
            l = slice(j * 128, j * 128 + 128)
            got = jnp.concatenate([rres[kind, 2 * j], rres[kind, 2 * j + 1]], axis=0).astype(F32)
            mine, theirs = stf[kind, own, :, l][0], pst[kind, :, l].astype(F32)
            if kind == 0:
                edge, inside = got, e0[:, l] * got + jnp.where(first, mine, theirs)
                low, high = edge, inside
            else:
                edge, inside = got, jnp.where(first, theirs, mine) + e1[:, l] * got
                low, high = inside, edge
            se[kind, own, :, l] = jnp.where(first, low, high).astype(BF16)[None]
            hs[kind, :, l] = jnp.where(first, high, low).astype(BF16)
        copy = remote(hs.at[kind], se.at[kind, c], d_sem.at[6 + 2 * kind], d_sem.at[7 + 2 * kind], mate)
        copy.start()
        copies.append(copy)

    def mate_states(kind):
        remote(hs.at[kind], se.at[kind, 1 - c], d_sem.at[6 + 2 * kind], d_sem.at[7 + 2 * kind], mate).wait_recv()

    with jax.named_scope("send_b"):
        send_states(1)
    with jax.named_scope("pairs_prep"):
        cumt[...] = cum.T
        scores = dot_nt(cm, bm)
        scores_t = dot_nt(bm, cm)
        ds_acc[...] = jnp.zeros_like(ds_acc)
        for j, e in enumerate(spread(jnp.broadcast_to(jnp.concatenate([r.d_skip[...], rowz], axis=1), (8, 128)))):
            ske[:, j * 128 : (j + 1) * 128] = e
        for h in range(32):
            cume[:, h * 128 : h * 128 + 128] = jnp.broadcast_to(cum[:, h : h + 1], (count, 128))

    def pair(j, carry):
        cols = pl.ds(pl.multiple_of(j * 128, 128), 128)
        xj = xdt[:, cols]
        gj = g_r[:, cols]
        none = jnp.zeros_like(xj)
        xx = jnp.concatenate([jnp.where(lane < 64, xj, none), jnp.where(lane < 64, none, xj)], axis=0)
        gg = jnp.concatenate([jnp.where(lane < 64, gj, none), jnp.where(lane < 64, none, gj)], axis=0)
        ww = dot_nt(gg, xj)
        mix, mix_t = [], []
        total_ds = ds_acc[...]
        for n in range(2):
            span = cume[:, pl.ds(pl.multiple_of(j * 256 + n * 128, 128), 128)] - cumt[pl.ds(2 * j + n, 1), :]
            decay = jnp.exp(jnp.where(keep, span, -1e30))
            decay_t = jnp.exp(jnp.where(keep_t, -span, -1e30))
            mix.append((scores * decay).astype(BF16))
            mix_t.append((scores_t * decay_t).astype(BF16))
            total_ds += ww[n * 128 : n * 128 + 128] * decay
        ds_acc[...] = total_ds
        yi[:, cols] = dot(jnp.concatenate(mix, axis=1), xx)
        dxi[:, cols] = dot(jnp.concatenate(mix_t, axis=1), gg)
        return carry

    with jax.named_scope("pairs1"):
        lax.fori_loop(0, 5, pair, 0)
    with jax.named_scope("send_f"):
        send_states(0)
    with jax.named_scope("scan_b"):
        scan_states(1)
    with jax.named_scope("pairs2"):
        lax.fori_loop(5, 11, pair, 0)
    with jax.named_scope("scan_f"):
        scan_states(0)
    with jax.named_scope("pairs3"):
        lax.fori_loop(11, 16, pair, 0)
        ds = ds_acc[...]
        ds_t = ds.T.astype(BF16)
        ds = ds.astype(BF16)
        grad_c = dot(ds, bm)
        grad_b = dot(ds_t, cm)
    segment = jnp.where(
        lax.broadcasted_iota(jnp.int32, (512, 128), 0) // 64 == lax.broadcasted_iota(jnp.int32, (512, 128), 1), 1.0, 0.0
    ).astype(BF16)
    y_v = r.y_out

    def place_heads(arrs):
        lane8 = lax.broadcasted_iota(jnp.int32, arrs[0].shape, 1)
        out = arrs[0]
        for q in range(1, 4):
            out = jnp.where(lane8 < 8 * q, out, pltpu.roll(arrs[q], 8 * q, 1))
        return out

    with jax.named_scope("take_b"):
        take_states(1)
        mate_states(1)

    ga, gz, gb, gv = r.ga, r.gz, r.gb, r.gv
    p2, p3 = [], []

    def x_part(q):
        half, l = q // 2, slice(q % 2 * 512, q % 2 * 512 + 512)
        cols = slice(q * 512, q * 512 + 512)
        en = se[1, half, :, l]
        xs = x_r[:, cols].astype(F32)
        dxs = tle[:, cols] * dot(bm, en)
        dxn = dxi[:, cols] + dxs
        dx = (dte[:, cols] * dxn + ske[0:1, cols] * g_r[:, cols].astype(F32)).astype(BF16)
        if q == 0:
            ga[0, :, :512] = dx
        elif q == 1:
            ga[0, :, 512:] = dx[:, :384]
            gz[0, :, :128] = dx[:, 384:]
        elif q == 2:
            gz[0, :, 128:] = dx[:, :384]
            gb[0, :, :128] = dx[:, 384:]
        else:
            gb[0, :, 128:640] = dx
        p2.append(heads(xs * dxn, segment))
        p3.append(heads(xs * dxs, segment))
        return dot_nt(xt[:, cols], en)

    share_a = Share(at.up, at.down, mate, ga, r.ly, r.acc_a, r.s_share.at[0], r.r_share.at[0], r.d_share.at[0])
    share_b = Share(at.right, at.left, mate, gb, r.lx, r.acc_b, r.s_share.at[1], r.r_share.at[1], r.d_share.at[1])
    share_v = Share(at.up, at.down, mate, gv, r.ly, r.acc_v, r.s_share.at[2], r.r_share.at[2], r.d_share.at[2])
    ring_z = Ring8(z, at.fore, at.aft, r.pz, r.got_z, r.s_share.at[3], r.rz)

    def partial(p, lhs, both, piece):
        rows = p.shape[1]
        lhs = lhs[piece].reshape(rows, 2 * count)
        p[piece] = dot(lhs, both[...].reshape(2 * count, p.shape[2])).astype(BF16)

    with jax.named_scope("x_part"):
        grad_b += x_part(0)
        grad_b += x_part(1)
        share_a.begin()
        grad_b += x_part(2)
        swap_z = remote(gz.at[0], gz.at[1], d_sem.at[10], d_sem.at[11], mate)
        swap_z.start()
        grad_b += x_part(3)
        gb[0, :, 640:] = grad_b.astype(BF16)
        share_b.begin()
    with jax.named_scope("far_z"):
        swap_z.wait()
        partial(ring_z.src, t3, gz, (z + 4) % 8)
        ring_z.far()
        for way in range(2):
            partial(ring_z.src, t3, gz, ring_z.piece(way, 3))
            ring_z.next_far(way)
        for s in (2, 1):
            for way in range(2):
                partial(ring_z.src, t3, gz, ring_z.piece(way, s))
        partial(ring_z.src, t3, gz, z)
    with jax.named_scope("take_f"):
        take_states(0)
    with jax.named_scope("early"):
        share_a.early()
        share_b.early()
    with jax.named_scope("z3"):
        ring_z.long(3)
    with jax.named_scope("mate_f"):
        mate_states(0)
    with jax.named_scope("y_part"):
        p1, he = [], []
        for q in range(4):
            half, l = q // 2, slice(q % 2 * 512, q % 2 * 512 + 512)
            cols = slice(q * 512, q * 512 + 512)
            st = se[0, half, :, l]
            xs = x_r[:, cols].astype(F32)
            yo = yi[:, cols] + ece[:, cols] * dot(cm, st)
            y_v[:, cols] = (yo + ske[0:1, cols] * xs).astype(BF16)
            p1.append(heads(g_r[:, cols].astype(F32) * yo, segment))
            both = jnp.sum(se[1, half, :, l].astype(F32) * st.astype(F32), axis=0, keepdims=True)
            he.append(heads(jnp.broadcast_to(both, (8, 512)), segment))
            grad_c += dot_nt(gec[:, cols], st)
        p1, p2 = place_heads(p1), place_heads(p2)
        last = jnp.sum(dt * place_heads(p3), axis=0, keepdims=True) + jnp.exp(total) * place_heads(he)[0:1]
        dloga = dot(upper, p1 - dt * p2, lax.Precision.HIGHEST) + last
        draw = (p2 + decay_rate * dloga) * sig
        gv[0, :, :128] = grad_c.astype(BF16)
        gv[0, :, 128:] = draw[:, :32].astype(BF16)
        share_v.begin()
    gt_v = r.gt_out

    def grad_tokens(k, carry):
        w = wbuf[k]
        cols = pl.ds(pl.multiple_of(k * 256, 256), 256)
        out = dot(ga[0], w[:WA]) + dot(gz[0], w[WA : WA + WZ])
        out += dot(gb[0], w[WA + WZ : WA + WZ + WB]) + dot(gv[0], w[WA + WZ + WB :])
        gt_v[:, cols] = out.astype(BF16)
        return carry

    with jax.named_scope("near"):
        share_a.near()
        share_b.near()
        ring_z.short(2)
        ring_z.long(2)
    with jax.named_scope("prod"):
        for n, l in ((0, r.ly), (1, r.lx)):
            received(l.at[pl.ds(1, 3)], r.t_sem.at[2 + n], mate)
        for slot in (0, 3, 1):
            share_a.product(slot)
            share_b.product(slot)
    with jax.named_scope("far"):
        share_v.early()
        share_a.far()
        share_b.far()
        ring_z.short(1)
        share_v.near()
        ring_z.long(1)

    by_z = [(d, (z + d) % 8, {"z": (z + d) % 8}) for d in (4, 3, 5, 2, 6, 1, 7)]
    def scatter(n, me, targets, src, got):
        return Scatter(me, targets, src, got, r.s_last.at[n], r.r_last.at[n])

    shares = ((share_a, x, by_x, 0), (share_b, y, by_y, WA + WZ), (share_v, x, by_x, WA + WZ + WB))
    stages = []
    for n, (k, lo, hi) in enumerate(PARTS):
        q, got, fs, fg = r.extra[4 * n : 4 * n + 4]
        share, me, targets, base = shares[k]
        mid, end = scatter(2 * n, me, targets, q, got), scatter(2 * n + 1, z, by_z, fs, fg)
        stages.append((mid, end, share, lo, hi, base))
    mid_z = scatter(10, x, by_x, r.qz, r.got_zx)
    end_z = scatter(11, y, by_y, r.fz_s, r.fz_g)

    def enter(n):
        mid, end, share, lo, hi, base = stages[n]
        mid.begin(*share.end(lo, hi))

    with jax.named_scope("end_a"):
        share_a.product(2)
        enter(0)
        enter(1)
    with jax.named_scope("end_b"):
        share_b.product(2)
        enter(2)
        enter(3)
    with jax.named_scope("end_v"):
        share_v.far()
        for slot in (0, 3, 1, 2):
            share_v.product(slot)
        enter(4)
    with jax.named_scope("end_z"):
        mid_z.begin(*ring_z.end())
    with jax.named_scope("gt1"):
        lax.fori_loop(0, 4, grad_tokens, 0)
    with jax.named_scope("mid_1"):
        for n in (0, 2):
            stages[n][1].begin(*stages[n][0].halves())
    with jax.named_scope("mid_2"):
        for n in (1, 3):
            stages[n][1].begin(*stages[n][0].halves())
    with jax.named_scope("mid_v"):
        stages[4][1].begin(*stages[4][0].halves())
    with jax.named_scope("mid_z"):
        end_z.begin(*mid_z.halves())
    with jax.named_scope("gt2"):
        lax.fori_loop(4, 8, grad_tokens, 0)
    gw = r.gw_out
    with jax.named_scope("finish"):
        for n in (0, 2, 1, 3, 4):
            mid, end, share, lo, hi, base = stages[n]
            gw[:, base + lo : base + hi] = end.end()
        gw[:, WA : WA + WZ] = end_z.end()
    with jax.named_scope("drain"):
        gather.end()
        for part in (share_a, share_b, share_v, ring_z, mid_z, end_z):
            part.drain()
        for mid, end, *rest in stages:
            mid.drain()
            end.drain()
        sent(dr.at[pl.ds(0, 15)], r.s_scan.at[0], mate)
        for n, l in ((0, r.ly), (1, r.lx)):
            sent(l.at[pl.ds(1, 3)], r.t_sem.at[n], mate)
        for kind in range(2):
            sent(rmsg.at[kind, pl.ds(0, 15)], r.s_scan.at[1 + kind], mate)
            sent(rres.at[kind, pl.ds(0, 15)], r.s_scan.at[3 + kind], mate)
        for copy in copies:
            copy.wait_send()


def fused(tokens, w, a_log, dt_bias, d_skip, grad_y):
    count = tokens.shape[0]
    cols, depth = w.shape
    sd = jax.ShapeDtypeStruct
    dma = pltpu.SemaphoreType.DMA
    scratch = dict(
        tok=((count, 2048), BF16), g=((count, INNER), BF16), wbuf=((8, cols, depth), BF16), acc=((count, cols), F32),
        tt=((2, 4, 4, 64, count), F32), tt3=((2, 8, 128, count), F32),
        tb=((2, 4, 4, 64, count), BF16), tb3=((2, 8, 128, count), BF16),
        tr=((4, 4, 64, count), BF16), tr3=((8, 128, count), BF16),
        t1=((4, 256, 2 * count), BF16), t2=((4, 256, 2 * count), BF16), lx=((4, 256, 2 * count), BF16), ly=((4, 256, 2 * count), BF16), t3=((8, 128, 2 * count), BF16),
        x=((count, INNER), BF16),
        dte=((count, INNER), F32), ece=((count, INNER), F32), tle=((count, INNER), F32),
        cume=((count, 2 * INNER), F32), cumt=((128, count), F32),
        xdt=((count, INNER), BF16), xt=((count, INNER), BF16), gec=((count, INNER), BF16),
        yi=((count, INNER), F32), dxi=((count, INNER), F32), ds_acc=((128, 128), F32),
        stf=((2, 2, 128, 1024), F32), sst=((2, 128, 1024), BF16), pst=((2, 128, 1024), BF16),
        tot_s=((8, 128), F32), tot_r=((8, 128), F32), te=((2, 2, 8, 1024), F32),
        dmsg=((8, 8, 128), F32), dr=((16, 8, 128), F32),
        msg=((2, 16, 64, 128), BF16), rmsg=((2, 16, 64, 128), BF16),
        res=((2, 16, 64, 128), BF16), rres=((2, 16, 64, 128), BF16),
        se=((2, 2, 128, 1024), BF16), hs=((2, 128, 1024), BF16), ske=((8, INNER), F32),
        ga=((8, count, WA), BF16), gb=((8, count, WB), BF16), gv=((8, count, WV), BF16), gz=((2, count, WZ), BF16),
        acc_a=((256, WA), F32), acc_b=((256, WB), F32), acc_v=((256, WV), F32),
        pz=((8, 128, WZ), BF16), got_z=((16, 64, WZ), BF16),
        qz=((4, 32, WZ), BF16), got_zx=((4, 32, WZ), BF16), fz_s=((4, 8, WZ), BF16), fz_g=((4, 8, WZ), BF16),
    )
    sems = dict(
        in_sem=(3,), tok_sem=(4,), g_send=(1,), g_ici=(7, 3), g_d2d=(7,), d_sem=(12,), s_scan=(5,), r_scan=(5,),
        t_sem=(4,), s_share=(4,), r_share=(3, 4, 2), d_share=(3, 4), rz=(16,), s_last=(12,), r_last=(12,),
    )

    extra = []
    for k, lo, hi in PARTS:
        extra += [pltpu.VMEM((4, 64, hi - lo), BF16)] * 2 + [pltpu.VMEM((8, 8, hi - lo), BF16)] * 2

    def body(tokens, w, a_log, dt_bias, d_skip, grad_y, y_out, gt_out, gw_out, *rest):
        r = SimpleNamespace(**dict(zip([*scratch, *sems], rest)))
        r.extra = rest[len(scratch) + len(sems) :]
        r.tokens, r.w, r.a_log, r.dt_bias, r.d_skip, r.grad_y = tokens, w, a_log, dt_bias, d_skip, grad_y
        r.y_out, r.gt_out, r.gw_out = y_out, gt_out, gw_out
        kernel(r)

    return pl.pallas_call(
        body,
        out_shape=(pltpu.VMEM((count, INNER), BF16), pltpu.VMEM((count, 2048), BF16), pltpu.VMEM((8, cols), F32)),
        in_specs=[ANY, ANY, VM, VM, VM, ANY],
        out_specs=(VM, VM, VM),
        scratch_shapes=[pltpu.VMEM(*v) for v in scratch.values()] + [dma(v) for v in sems.values()] + extra,
        compiler_params=pltpu.CompilerParams(collective_id=0, has_side_effects=True, vmem_limit_bytes=LIMIT),
    )(tokens, w, a_log.reshape(1, -1), dt_bias.reshape(1, -1), d_skip.reshape(1, -1), grad_y)


def leave_kernel(*refs):
    copies = [pltpu.make_async_copy(refs[n], refs[3 + n], refs[6].at[n]) for n in range(3)]
    for copy in copies:
        copy.start()
    for copy in copies:
        copy.wait()


def leave(*arrays):
    return pl.pallas_call(
        leave_kernel,
        out_shape=tuple(jax.ShapeDtypeStruct(a.shape, a.dtype) for a in arrays),
        in_specs=[VM] * 3,
        out_specs=(ANY,) * 3,
        scratch_shapes=[pltpu.SemaphoreType.DMA((3,))],
    )(*(pltpu.with_memory_space_constraint(a, pltpu.VMEM) for a in arrays))


def per_device(tokens, w_in, a_log, dt_bias, d_skip, grad_y):
    count, width = tokens.shape[1:]
    inner = grad_y.shape[2]
    y, gt, gw = fused(tokens.reshape(count, width), w_in.T, a_log, dt_bias, d_skip, grad_y.reshape(count, inner))
    y, gt, gw = leave(y, gt, gw)
    return (y.reshape(1, count, inner), gt.reshape(1, count, width), gw)


def solution(mesh):
    torus = Mesh(mesh.devices.reshape(2, 8, 2, 2, 4), ("xh", "z", "c", "xl", "y"))
    placed = (P(ZERO, SEQ, None), P(ZERO, None), P(), P(), P(), P(ZERO, SEQ, None))
    return jax.shard_map(
        per_device,
        mesh=torus,
        in_specs=placed,
        out_specs=(P(ZERO, SEQ, None), P(ZERO, SEQ, None), P(SEQ + ZERO, None)),
        check_vma=False,
    )
```

```python
from types import SimpleNamespace

import jax
import jax.numpy as jnp
from jax import lax
from jax.experimental import pallas as pl
from jax.experimental.pallas import tpu as pltpu
from jax.sharding import Mesh
from jax.sharding import PartitionSpec as P

SEQ = ("xh", "z", "c")
ZERO = ("xl", "y")
MESH = pl.DeviceIdType.MESH
F32 = jnp.float32
BF16 = jnp.bfloat16
LIMIT = 62 * 1024 * 1024
VM = pl.BlockSpec(memory_space=pltpu.VMEM)
ANY = pl.BlockSpec(memory_space=pl.ANY)
INNER = 2048
EDGE_SMALL, EDGE_LARGE = 384, 400
WA, WZ, WB, WV = 896, 512, 768, 160
PARTS = ((0, 0, 512), (0, 512, 896), (1, 0, 384), (1, 384, 768), (2, 0, 160))


def remote(src, dst, send, recv, target):
    return pltpu.make_async_remote_copy(
        src_ref=src, dst_ref=dst, send_sem=send, recv_sem=recv, device_id=target, device_id_type=MESH
    )


def sent(block, sem, target):
    remote(block, block, sem, sem, target).wait_send()


def received(block, sem, target):
    remote(block, block, sem, sem, target).wait_recv()


def along_x(x):
    return {"xh": x // 2, "xl": x % 2}


def dot(a, b, precision=None):
    return jnp.dot(a, b, preferred_element_type=F32, precision=precision)


def dot_nt(a, b):
    return lax.dot_general(a, b, (((1,), (1,)), ((), ())), preferred_element_type=F32)


class Place:
    def __init__(self):
        self.xh, self.z, self.c, self.xl, self.y = (lax.axis_index(a) for a in ("xh", "z", "c", "xl", "y"))
        self.x = self.xh * 2 + self.xl
        self.chip = self.xh * 8 + self.z
        self.right, self.left = along_x((self.x + 1) % 4), along_x((self.x + 3) % 4)
        self.up, self.down = {"y": (self.y + 1) % 4}, {"y": (self.y + 3) % 4}
        self.fore, self.aft = {"z": (self.z + 1) % 8}, {"z": (self.z + 7) % 8}
        self.mate = {"c": 1 - self.c}
        self.others = []
        for d in (4, 12, 3, 5, 11, 13, 2, 6, 10, 14, 8, 1, 7, 9, 15):
            t = (self.chip + d) % 16
            self.others.append((d, t, (self.chip + 16 - d) % 16, {"xh": t // 8, "z": t % 8}))

    def greet(self):
        barrier = pltpu.get_barrier_semaphore()
        targets = [self.mate, self.right, self.left, self.up, self.down, {"y": (self.y + 2) % 4}] + [o[3] for o in self.others]
        for target in targets:
            pl.semaphore_signal(barrier, inc=1, device_id=target, device_id_type=MESH)
        pl.semaphore_wait(barrier, len(targets))


class Gather:
    def __init__(self, at, w, wbuf, s):
        self.at, self.w, self.wbuf, self.s = at, w, wbuf, s
        self.rel = [self.shard(0, 3), self.shard(0, 1), self.shard(0, 2)] + [self.shard(1, d) for d in (0, 3, 1, 2)]
        self.mine = self.shard(0, 0)

    def shard(self, flip, dy):
        return (self.at.xl + flip) % 2 * 4 + (self.at.y + dy) % 4

    def rows(self, part, core=None):
        core = self.at.c if core is None else core
        odd = self.at.z % 2
        base = core * (2 * EDGE_SMALL + EDGE_LARGE)
        far = EDGE_SMALL + EDGE_LARGE
        if part == "a":
            start, size = base + odd * far, EDGE_SMALL
        elif part == "b":
            start, size = base + EDGE_SMALL, EDGE_LARGE
        elif part in ("a0", "a1"):
            start, size = base + odd * far + (part == "a1") * (EDGE_SMALL // 2), EDGE_SMALL // 2
        else:
            start, size = base + (1 - odd) * far, EDGE_SMALL
        return pl.ds(pl.multiple_of(start, 16), size)

    def block(self, k, part, core=None):
        return self.wbuf.at[k, self.rows(part, core)]

    def send(self, k, part, to, slot, lane):
        block = self.block(k, part)
        remote(block, block, self.s.g_send.at[0], self.s.g_ici.at[slot, lane], to).start()

    def depth_send(self, k, slot):
        self.send(k, "a0", self.at.fore, slot, 2)
        self.send(k, "a1", self.at.aft, slot, 2)

    def begin(self):
        at = self.at
        self.send(self.mine, "a", at.up, 0, 0)
        self.send(self.mine, "b", at.down, 1, 1)
        self.send(self.mine, "a", at.left, 3, 0)
        self.send(self.mine, "b", at.right, 3, 1)
        self.send(self.mine, "b", at.up, 0, 1)
        self.send(self.mine, "a", at.down, 1, 0)

    def arrive(self, slot, lane):
        block = self.block(self.rel[slot], ("a", "b", "m")[lane])
        received(block, self.s.g_ici.at[slot, lane], self.at.mate)
        remote(block, block, self.s.g_send.at[0], self.s.g_d2d.at[slot], self.at.mate).start()

    def a(self, slot, *onward):
        self.arrive(slot, 0)
        for to, there in onward:
            self.send(self.rel[slot], "a", to, there, 0)
        self.depth_send(self.rel[slot], slot)

    def b(self, slot, *onward):
        self.arrive(slot, 1)
        for to, there in onward:
            self.send(self.rel[slot], "b", to, there, 1)

    def m(self, slot):
        self.arrive(slot, 2)

    def whole(self, slot):
        half = self.wbuf.shape[1] // 2
        rows = pl.ds(pl.multiple_of((1 - self.at.c) * half, 16), half)
        received(self.wbuf.at[self.rel[slot], rows], self.s.g_d2d.at[slot], self.at.mate)

    def end(self):
        sent(self.wbuf.at[pl.ds(0, 7)], self.s.g_send.at[0], self.at.mate)


def spread(row):
    lane = lax.broadcasted_iota(jnp.int32, (row.shape[0], 128), 1)
    out = []
    for j in range(16):
        out.append(jnp.where(lane < 64, row[:, 2 * j : 2 * j + 1], row[:, 2 * j + 1 : 2 * j + 2]))
    return out


def heads(values, part):
    high = values.astype(BF16)
    low = (values - high.astype(F32)).astype(BF16)
    return dot(high, part) + dot(low, part)


class Share:
    def __init__(self, plus, minus, mate, g, lhs, acc, send, ici, d2d):
        self.plus, self.minus, self.mate, self.g, self.lhs, self.acc = plus, minus, mate, g, lhs, acc
        self.sem, self.ici, self.d2d = send, ici, d2d
        self.h = g.shape[1] // 2

    def half(self, n, part):
        return self.g.at[n, pl.ds(part * self.h, self.h)]

    def go(self, src, slot, part, to):
        remote(self.half(src, part), self.half(2 * slot, part), self.sem, self.ici.at[slot, part], to).start()

    def begin(self):
        remote(self.g.at[0], self.g.at[1], self.sem, self.d2d.at[0], self.mate).start()
        self.go(0, 3, 0, self.plus)
        self.go(0, 1, 1, self.minus)
        self.go(0, 3, 1, self.plus)
        self.go(0, 1, 0, self.minus)

    def arrive(self, slot, part):
        received(self.half(2 * slot, part), self.ici.at[slot, part], self.plus)
        block = self.half(2 * slot, part)
        remote(block, self.half(2 * slot + 1, part), self.sem, self.d2d.at[slot], self.mate).start()

    def early(self):
        self.arrive(3, 0)
        self.go(6, 2, 0, self.plus)
        self.arrive(1, 1)
        self.go(2, 2, 1, self.minus)

    def near(self):
        self.arrive(3, 1)
        self.arrive(1, 0)

    def far(self):
        self.arrive(2, 0)
        self.arrive(2, 1)

    def product(self, slot):
        received(self.g.at[2 * slot + 1], self.d2d.at[slot], self.mate)
        rhs = self.g[2 * slot : 2 * slot + 2].reshape(4 * self.h, self.g.shape[2])
        value = dot(self.lhs[slot], rhs)
        self.acc[...] = value if slot == 0 else self.acc[...] + value

    def end(self, lo, hi):
        h = self.acc.shape[0] // 2
        return self.acc[:h, lo:hi], self.acc[h:, lo:hi]

    def drain(self):
        sent(self.g.at[pl.ds(0, 7)], self.sem, self.mate)


class Scatter:
    def __init__(self, me, targets, src, got, send, recv):
        self.me, self.targets, self.src, self.got, self.sem, self.recv = me, targets, src, got, send, recv

    def begin(self, low, high):
        n, rows = self.src.shape[0] // 2, self.src.shape[1]
        for k in range(n):
            self.src[k] = low[k * rows : k * rows + rows].astype(BF16)
            self.src[k + n] = high[k * rows : k * rows + rows].astype(BF16)
        for d, t, target in self.targets:
            remote(self.src.at[t], self.got.at[d], self.sem, self.recv, target).start()

    def all(self):
        return self.got.at[pl.ds(1, len(self.targets))]

    def end(self):
        received(self.all(), self.recv, self.targets[0][2])
        out = self.src[self.me].astype(F32)
        for d in range(1, len(self.targets) + 1):
            out += self.got[d].astype(F32)
        return out

    def halves(self):
        out = self.end()
        h = out.shape[0] // 2
        return out[:h], out[h:]

    def drain(self):
        sent(self.all(), self.sem, self.targets[0][2])


class Ring8:
    def __init__(self, me, plus, minus, src, got, send, recv):
        self.me, self.src, self.got, self.sem, self.recv = me, src, got, send, recv
        self.to = (plus, minus)
        self.h = src.shape[1] // 2

    def piece(self, way, s):
        return (self.me + (s if way == 0 else 8 - s)) % 8

    def slot(self, way, half, s):
        return (way * 2 + half) * 4 + s

    def go(self, way, half, s):
        block = self.src.at[self.piece(way, s), pl.ds(half * self.h, self.h)]
        n = self.slot(way, half, s - 1)
        remote(block, self.got.at[n], self.sem, self.recv.at[n], self.to[way]).start()

    def landed(self, way, half, s):
        n = self.slot(way, half, s)
        received(self.got.at[n], self.recv.at[n], self.to[way])
        return self.got[n].astype(F32)

    def on(self, way, half, s):
        at = self.piece(way, s)
        rows = slice(half * self.h, half * self.h + self.h)
        self.src[at, rows] = (self.src[at, rows].astype(F32) + self.landed(way, half, s)).astype(BF16)
        self.go(way, half, s)

    def far(self):
        self.go(0, 0, 4)
        self.go(1, 1, 4)

    def next_far(self, way):
        self.go(way, 1 - way, 3)

    def long(self, s):
        self.on(0, 0, s)
        self.on(1, 1, s)

    def short(self, s):
        self.on(0, 1, s)
        self.on(1, 0, s)

    def end(self):
        low = self.src[self.me, : self.h].astype(F32) + self.landed(1, 0, 0)
        high = self.src[self.me, self.h :].astype(F32) + self.landed(0, 1, 0)
        return low + self.landed(0, 0, 0), high + self.landed(1, 1, 0)

    def drain(self):
        sent(self.got.at[pl.ds(0, 14)], self.sem, self.to[0])


def kernel(r):
    at = Place()
    c, x, y, z, chip, mate = at.c, at.x, at.y, at.z, at.chip, at.mate
    first = c == 0
    own = pl.ds(c, 1)

    tok, acc, wbuf = r.tok, r.acc, r.wbuf
    count = tok.shape[0]
    depth = wbuf.shape[2]
    gather = Gather(at, r.w, wbuf, r)
    w_copy = pltpu.make_async_copy(r.w, wbuf.at[gather.mine], r.in_sem.at[0])
    tok_copy = pltpu.make_async_copy(r.tokens, tok, r.in_sem.at[1])
    g_copy = pltpu.make_async_copy(r.grad_y, r.g, r.in_sem.at[2])
    w_copy.start()
    tok_copy.start()
    g_copy.start()
    with jax.named_scope("greet"):
        at.greet()
    w_copy.wait()
    gather.begin()
    tok_copy.wait()
    scope_tok = jax.named_scope("tok")
    scope_tok.__enter__()
    tt, tt3 = r.tt, r.tt3
    for i in range(16):
        block = tok[:, i * 128 : (i + 1) * 128].astype(F32).T
        for n in range(16):
            core, xlow, yy = n // 8, n // 4 % 2, n % 4
            rows = block[n * 8 : n * 8 + 8, :]
            xx, zz = i // 8 * 2 + xlow, i % 8
            tt[core, xx, yy, zz * 8 : zz * 8 + 8, :] = rows
            tt3[core, zz, xx * 32 + yy * 8 : xx * 32 + yy * 8 + 8, :] = rows
    tb, tb3, tr, tr3 = r.tb, r.tb3, r.tr, r.tr3
    tb[...] = tt[...].astype(BF16)
    tb3[...] = tt3[...].astype(BF16)
    swap = remote(tb.at[1 - c], tr, r.tok_sem.at[0], r.tok_sem.at[1], mate)
    swap3 = remote(tb3.at[1 - c], tr3, r.tok_sem.at[2], r.tok_sem.at[3], mate)
    swap.start()
    swap3.start()
    t1, t2, t3 = r.t1, r.t2, r.t3

    def place_rows(lo, one, three):
        t3[:, :, lo : lo + 128] = three
        for i in range(4):
            for j in range(4):
                t1[i, j * 64 : j * 64 + 64, lo : lo + 128] = one[i, j]
                t2[j, i * 64 : i * 64 + 64, lo : lo + 128] = one[i, j]

    place_rows(0, tb[own][0], tb3[own][0])
    acc[...] = jnp.zeros_like(acc)

    def multiply(*ks):
        def body(i, carry):
            k = ks[0]
            for n in range(1, len(ks)):
                k = jnp.where(i == n, ks[n], k)
            acc[...] += dot_nt(tok[:, pl.ds(pl.multiple_of(k * depth, depth), depth)], wbuf[k])
            return carry

        lax.fori_loop(0, len(ks), body, 0)

    scope_tok.__exit__(None, None, None)
    ga, gb, gm, rel = gather.a, gather.b, gather.m, gather.rel
    with jax.named_scope("g1"):
        ga(0, (at.up, 2), (at.left, 4))
        gb(1, (at.down, 2), (at.right, 5))
        ga(3)
        gb(3)
    with jax.named_scope("g2"):
        gb(0, (at.right, 4))
        ga(1, (at.left, 5))
        ga(4)
        gb(5)
        gm(0)
        gm(3)
    with jax.named_scope("g3"):
        ga(2, (at.left, 6))
        gb(2, (at.right, 6))
        swap.wait()
        swap3.wait()
        place_rows(128, tr[...], tr3[...])
        gb(4)
        ga(5)
        gather.whole(0)
        gather.whole(3)
        multiply(gather.mine, rel[0], rel[3])
    with jax.named_scope("g4"):
        gm(1)
        gm(4)
        ga(6)
        gb(6)
        by_y = [(d, (y + d) % 4, {"y": (y + d) % 4}) for d in (2, 1, 3)]
        by_x = [(d, (x + d) % 4, along_x((x + d) % 4)) for d in (2, 1, 3)]
        for n, (t, l, me, targets) in enumerate(((t2, r.ly, y, by_y), (t1, r.lx, x, by_x))):
            for d, to, target in targets:
                remote(t.at[to], l.at[4 - d], r.t_sem.at[n], r.t_sem.at[2 + n], target).start()
            l[0] = t[me]
        gm(2)
        gm(5)
        gather.whole(1)
        gather.whole(4)
        multiply(rel[1], rel[4])
    with jax.named_scope("g5"):
        gm(6)
        gather.whole(2)
        gather.whole(5)
        multiply(rel[2], rel[5])
    with jax.named_scope("g6"):
        gather.whole(6)
    last_tok = tok[:, pl.ds(pl.multiple_of(rel[6] * depth, depth), depth)]
    with jax.named_scope("g7"):
        acc[:, INNER:] += dot_nt(last_tok, wbuf[rel[6], INNER:])

    x_r, g_r = r.x, r.g
    dte, ece, tle, cume, cumt = r.dte, r.ece, r.tle, r.cume, r.cumt
    xdt, xt, gec, yi, dxi, ds_acc = r.xdt, r.xt, r.gec, r.yi, r.dxi, r.ds_acc
    stf, sst, pst, te, ske = r.stf, r.sst, r.pst, r.te, r.ske
    tot_s, tot_r, dmsg, dr = r.tot_s, r.tot_r, r.dmsg, r.dr
    msg, rmsg, res, rres, se, hs = r.msg, r.rmsg, r.res, r.rres, r.se, r.hs
    d_sem = r.d_sem
    copies = []
    with jax.named_scope("prep"):
        bm = acc[:, INNER : INNER + 128].astype(BF16)
        cm = acc[:, INNER + 128 : INNER + 256].astype(BF16)
        rowz = jnp.zeros((1, 96), F32)
        decay_rate = jnp.concatenate([-jnp.exp(r.a_log[...]), rowz], axis=1)
        bias = jnp.concatenate([r.dt_bias[...], rowz], axis=1)
        u = jnp.concatenate([acc[:, INNER + 256 :], jnp.zeros((count, 96), F32)], axis=1) + bias
        small = jnp.exp(-jnp.abs(u))
        dt = jnp.maximum(u, 0.0) + jnp.log1p(small)
        sig = jnp.where(u >= 0, 1.0, small) / (1.0 + small)
        ti = lax.broadcasted_iota(jnp.int32, (128, 128), 0)
        si = lax.broadcasted_iota(jnp.int32, (128, 128), 1)
        keep, keep_t = ti >= si, ti <= si
        lower = jnp.where(keep, 1.0, 0.0).astype(F32)
        upper = jnp.where(keep_t, 1.0, 0.0).astype(F32)
        cum = dot(lower, decay_rate * dt, lax.Precision.HIGHEST)
        total = cum[127:128, :]
        tot_s[...] = jnp.broadcast_to(total, (8, 128))
        tot_copy = remote(tot_s, tot_r, d_sem.at[0], d_sem.at[1], mate)
        tot_copy.start()
        lane = lax.broadcasted_iota(jnp.int32, (count, 128), 1)

        def widen(arr, dst):
            for j, e in enumerate(spread(arr)):
                dst[:, j * 128 : (j + 1) * 128] = e

        widen(jnp.exp(cum), ece)
        g_copy.wait()
        gec[...] = (g_r[...].astype(F32) * ece[...]).astype(BF16)
        ct = cm.astype(F32).T.astype(BF16)

    def local_states(kind, lhs, rhs):
        for half in range(2):
            stf[kind, half] = dot(lhs, rhs[:, half * 1024 : half * 1024 + 1024])
        sst[kind] = stf[kind, pl.ds(1 - c, 1)][0].astype(BF16)
        copy = remote(sst.at[kind], pst.at[kind], d_sem.at[2 + 2 * kind], d_sem.at[3 + 2 * kind], mate)
        copy.start()
        return copy

    with jax.named_scope("states"):
        st_b = local_states(1, ct, gec)
        widen(dt, dte)
        widen(jnp.exp(total - cum), tle)
        xs = (acc[:, :INNER] + dot_nt(last_tok, wbuf[rel[6], :INNER])).astype(BF16)
        x_r[...] = xs
        st_copies = [None, st_b]
        tot_copy.wait()
        for n, arr in enumerate((tot_s, tot_r)):
            for j, e in enumerate(spread(arr[...])):
                te[n, j // 8, :, j % 8 * 128 : j % 8 * 128 + 128] = e
        for j in range(8):
            l = slice(j * 128, j * 128 + 128)
            dmsg[j] = te[0, own, :, l][0] + te[1, own, :, l][0]
        dr[pl.ds(chip, 1)] = dmsg[pl.ds(chip // 2, 1)]
        for d, t, source, target in at.others:
            remote(dmsg.at[t // 2], dr.at[chip], r.s_scan.at[0], r.r_scan.at[0], target).start()
        e_own, e_mate = jnp.exp(te[0, own][0][0:1]), jnp.exp(te[1, own][0][0:1])
        e0 = jnp.where(first, e_own, e_mate)
        e1 = jnp.where(first, e_mate, e_own)

    def send_states(kind):
        st_copies[kind].wait()
        mine, theirs = stf[kind, own][0], pst[kind].astype(F32)
        early = jnp.where(first, mine, theirs)
        late = jnp.where(first, theirs, mine)
        whole = (e1 * early + late if kind == 0 else early + e0 * late).astype(BF16)
        for i in range(16):
            msg[kind, i] = whole[i % 2 * 64 : i % 2 * 64 + 64, i // 2 * 128 : i // 2 * 128 + 128]
        for d, t, source, target in at.others:
            remote(msg.at[kind, t], rmsg.at[kind, chip], r.s_scan.at[1 + kind], r.r_scan.at[1 + kind], target).start()
        rmsg[kind, pl.ds(chip, 1)] = msg[kind, pl.ds(chip, 1)]

    def scan_states(kind):
        if kind == 1:
            received(dr.at[pl.ds(0, 15)], r.r_scan.at[0], mate)
        received(rmsg.at[kind, pl.ds(0, 15)], r.r_scan.at[1 + kind], mate)
        state = jnp.zeros((64, 128), F32)
        for i in range(16) if kind == 0 else reversed(range(16)):
            res[kind, i] = state.astype(BF16)
            state = jnp.exp(dr[i][0:1]) * state + rmsg[kind, i].astype(F32)
        for d, t, source, target in at.others:
            remote(res.at[kind, t], rres.at[kind, chip], r.s_scan.at[3 + kind], r.r_scan.at[3 + kind], target).start()
        rres[kind, pl.ds(chip, 1)] = res[kind, pl.ds(chip, 1)]

    def take_states(kind):
        received(rres.at[kind, pl.ds(0, 15)], r.r_scan.at[3 + kind], mate)
        for j in range(8):
            l = slice(j * 128, j * 128 + 128)
            got = jnp.concatenate([rres[kind, 2 * j], rres[kind, 2 * j + 1]], axis=0).astype(F32)
            mine, theirs = stf[kind, own, :, l][0], pst[kind, :, l].astype(F32)
            if kind == 0:
                edge, inside = got, e0[:, l] * got + jnp.where(first, mine, theirs)
                low, high = edge, inside
            else:
                edge, inside = got, jnp.where(first, theirs, mine) + e1[:, l] * got
                low, high = inside, edge
            se[kind, own, :, l] = jnp.where(first, low, high).astype(BF16)[None]
            hs[kind, :, l] = jnp.where(first, high, low).astype(BF16)
        copy = remote(hs.at[kind], se.at[kind, c], d_sem.at[6 + 2 * kind], d_sem.at[7 + 2 * kind], mate)
        copy.start()
        copies.append(copy)

    def mate_states(kind):
        remote(hs.at[kind], se.at[kind, 1 - c], d_sem.at[6 + 2 * kind], d_sem.at[7 + 2 * kind], mate).wait_recv()

    with jax.named_scope("send_b"):
        send_states(1)
        xd = x_r[...].astype(F32) * dte[...]
        xdt[...] = xd.astype(BF16)
        xt[...] = (xd * tle[...]).astype(BF16)
        bt = bm.astype(F32).T.astype(BF16)
        st_copies[0] = local_states(0, bt, xt)
    with jax.named_scope("pairs_prep"):
        cumt[...] = cum.T
        scores = dot_nt(cm, bm)
        scores_t = dot_nt(bm, cm)
        ds_acc[...] = jnp.zeros_like(ds_acc)
        for j, e in enumerate(spread(jnp.broadcast_to(jnp.concatenate([r.d_skip[...], rowz], axis=1), (8, 128)))):
            ske[:, j * 128 : (j + 1) * 128] = e
        for h in range(32):
            cume[:, h * 128 : h * 128 + 128] = jnp.broadcast_to(cum[:, h : h + 1], (count, 128))

    def pair(j, carry):
        cols = pl.ds(pl.multiple_of(j * 128, 128), 128)
        xj = xdt[:, cols]
        gj = g_r[:, cols]
        none = jnp.zeros_like(xj)
        xx = jnp.concatenate([jnp.where(lane < 64, xj, none), jnp.where(lane < 64, none, xj)], axis=0)
        gg = jnp.concatenate([jnp.where(lane < 64, gj, none), jnp.where(lane < 64, none, gj)], axis=0)
        ww = dot_nt(gg, xj)
        mix, mix_t = [], []
        total_ds = ds_acc[...]
        for n in range(2):
            span = cume[:, pl.ds(pl.multiple_of(j * 256 + n * 128, 128), 128)] - cumt[pl.ds(2 * j + n, 1), :]
            decay = jnp.exp(jnp.where(keep, span, -1e30))
            decay_t = jnp.exp(jnp.where(keep_t, -span, -1e30))
            mix.append((scores * decay).astype(BF16))
            mix_t.append((scores_t * decay_t).astype(BF16))
            total_ds += ww[n * 128 : n * 128 + 128] * decay
        ds_acc[...] = total_ds
        yi[:, cols] = dot(jnp.concatenate(mix, axis=1), xx)
        dxi[:, cols] = dot(jnp.concatenate(mix_t, axis=1), gg)
        return carry

    with jax.named_scope("pairs1"):
        lax.fori_loop(0, 5, pair, 0)
    with jax.named_scope("send_f"):
        send_states(0)
    with jax.named_scope("scan_b"):
        scan_states(1)
    with jax.named_scope("pairs2"):
        lax.fori_loop(5, 11, pair, 0)
    with jax.named_scope("scan_f"):
        scan_states(0)
    with jax.named_scope("pairs3"):
        lax.fori_loop(11, 16, pair, 0)
        ds = ds_acc[...]
        ds_t = ds.T.astype(BF16)
        ds = ds.astype(BF16)
        grad_c = dot(ds, bm)
        grad_b = dot(ds_t, cm)
    segment = jnp.where(
        lax.broadcasted_iota(jnp.int32, (512, 128), 0) // 64 == lax.broadcasted_iota(jnp.int32, (512, 128), 1), 1.0, 0.0
    ).astype(BF16)
    y_v = r.y_out

    def place_heads(arrs):
        lane8 = lax.broadcasted_iota(jnp.int32, arrs[0].shape, 1)
        out = arrs[0]
        for q in range(1, 4):
            out = jnp.where(lane8 < 8 * q, out, pltpu.roll(arrs[q], 8 * q, 1))
        return out

    with jax.named_scope("take_b"):
        take_states(1)
        mate_states(1)

    ga, gz, gb, gv = r.ga, r.gz, r.gb, r.gv
    p2, p3 = [], []

    def x_part(q):
        half, l = q // 2, slice(q % 2 * 512, q % 2 * 512 + 512)
        cols = slice(q * 512, q * 512 + 512)
        en = se[1, half, :, l]
        xs = x_r[:, cols].astype(F32)
        dxs = tle[:, cols] * dot(bm, en)
        dxn = dxi[:, cols] + dxs
        dx = (dte[:, cols] * dxn + ske[0:1, cols] * g_r[:, cols].astype(F32)).astype(BF16)
        if q == 0:
            ga[0, :, :512] = dx
        elif q == 1:
            ga[0, :, 512:] = dx[:, :384]
            gz[0, :, :128] = dx[:, 384:]
        elif q == 2:
            gz[0, :, 128:] = dx[:, :384]
            gb[0, :, :128] = dx[:, 384:]
        else:
            gb[0, :, 128:640] = dx
        p2.append(heads(xs * dxn, segment))
        p3.append(heads(xs * dxs, segment))
        return dot_nt(xt[:, cols], en)

    share_a = Share(at.up, at.down, mate, ga, r.ly, r.acc_a, r.s_share.at[0], r.r_share.at[0], r.d_share.at[0])
    share_b = Share(at.right, at.left, mate, gb, r.lx, r.acc_b, r.s_share.at[1], r.r_share.at[1], r.d_share.at[1])
    share_v = Share(at.up, at.down, mate, gv, r.ly, r.acc_v, r.s_share.at[2], r.r_share.at[2], r.d_share.at[2])
    ring_z = Ring8(z, at.fore, at.aft, r.pz, r.got_z, r.s_share.at[3], r.rz)

    def partial(p, lhs, both, piece):
        rows = p.shape[1]
        lhs = lhs[piece].reshape(rows, 2 * count)
        p[piece] = dot(lhs, both[...].reshape(2 * count, p.shape[2])).astype(BF16)

    with jax.named_scope("x_part"):
        grad_b += x_part(0)
        grad_b += x_part(1)
        share_a.begin()
        grad_b += x_part(2)
        swap_z = remote(gz.at[0], gz.at[1], d_sem.at[10], d_sem.at[11], mate)
        swap_z.start()
        grad_b += x_part(3)
        gb[0, :, 640:] = grad_b.astype(BF16)
        share_b.begin()
    with jax.named_scope("far_z"):
        swap_z.wait()
        partial(ring_z.src, t3, gz, (z + 4) % 8)
        ring_z.far()
        for way in range(2):
            partial(ring_z.src, t3, gz, ring_z.piece(way, 3))
            ring_z.next_far(way)
        for s in (2, 1):
            for way in range(2):
                partial(ring_z.src, t3, gz, ring_z.piece(way, s))
        partial(ring_z.src, t3, gz, z)
    with jax.named_scope("take_f"):
        take_states(0)
    with jax.named_scope("early"):
        share_a.early()
        share_b.early()
    with jax.named_scope("z3"):
        ring_z.long(3)
    with jax.named_scope("mate_f"):
        mate_states(0)
    with jax.named_scope("y_part"):
        p1, he = [], []
        for q in range(4):
            half, l = q // 2, slice(q % 2 * 512, q % 2 * 512 + 512)
            cols = slice(q * 512, q * 512 + 512)
            st = se[0, half, :, l]
            xs = x_r[:, cols].astype(F32)
            yo = yi[:, cols] + ece[:, cols] * dot(cm, st)
            y_v[:, cols] = (yo + ske[0:1, cols] * xs).astype(BF16)
            p1.append(heads(g_r[:, cols].astype(F32) * yo, segment))
            both = jnp.sum(se[1, half, :, l].astype(F32) * st.astype(F32), axis=0, keepdims=True)
            he.append(heads(jnp.broadcast_to(both, (8, 512)), segment))
            grad_c += dot_nt(gec[:, cols], st)
        p1, p2 = place_heads(p1), place_heads(p2)
        last = jnp.sum(dt * place_heads(p3), axis=0, keepdims=True) + jnp.exp(total) * place_heads(he)[0:1]
        dloga = dot(upper, p1 - dt * p2, lax.Precision.HIGHEST) + last
        draw = (p2 + decay_rate * dloga) * sig
        gv[0, :, :128] = grad_c.astype(BF16)
        gv[0, :, 128:] = draw[:, :32].astype(BF16)
        share_v.begin()
    gt_v = r.gt_out

    def grad_tokens(k, carry):
        w = wbuf[k]
        cols = pl.ds(pl.multiple_of(k * 256, 256), 256)
        out = dot(ga[0], w[:WA]) + dot(gz[0], w[WA : WA + WZ])
        out += dot(gb[0], w[WA + WZ : WA + WZ + WB]) + dot(gv[0], w[WA + WZ + WB :])
        gt_v[:, cols] = out.astype(BF16)
        return carry

    with jax.named_scope("near"):
        share_a.near()
        share_b.near()
        ring_z.short(2)
        ring_z.long(2)
    with jax.named_scope("prod"):
        for n, l in ((0, r.ly), (1, r.lx)):
            received(l.at[pl.ds(1, 3)], r.t_sem.at[2 + n], mate)
        for slot in (0, 3, 1):
            share_a.product(slot)
            share_b.product(slot)
    with jax.named_scope("far"):
        share_a.far()
        share_b.far()
        share_v.early()
        ring_z.short(1)
        share_v.near()
        ring_z.long(1)

    by_z = [(d, (z + d) % 8, {"z": (z + d) % 8}) for d in (4, 3, 5, 2, 6, 1, 7)]
    def scatter(n, me, targets, src, got):
        return Scatter(me, targets, src, got, r.s_last.at[n], r.r_last.at[n])

    shares = ((share_a, x, by_x, 0), (share_b, y, by_y, WA + WZ), (share_v, x, by_x, WA + WZ + WB))
    stages = []
    for n, (k, lo, hi) in enumerate(PARTS):
        q, got, fs, fg = r.extra[4 * n : 4 * n + 4]
        share, me, targets, base = shares[k]
        mid, end = scatter(2 * n, me, targets, q, got), scatter(2 * n + 1, z, by_z, fs, fg)
        stages.append((mid, end, share, lo, hi, base))
    mid_z = scatter(10, x, by_x, r.qz, r.got_zx)
    end_z = scatter(11, y, by_y, r.fz_s, r.fz_g)

    def enter(n):
        mid, end, share, lo, hi, base = stages[n]
        mid.begin(*share.end(lo, hi))

    with jax.named_scope("end_a"):
        share_a.product(2)
        enter(0)
        enter(1)
    with jax.named_scope("end_b"):
        share_b.product(2)
        enter(2)
        enter(3)
    with jax.named_scope("end_v"):
        share_v.far()
        for slot in (0, 3, 1, 2):
            share_v.product(slot)
        enter(4)
    with jax.named_scope("end_z"):
        mid_z.begin(*ring_z.end())
    with jax.named_scope("gt1"):
        lax.fori_loop(0, 4, grad_tokens, 0)
    with jax.named_scope("mid_1"):
        for n in (0, 2):
            stages[n][1].begin(*stages[n][0].halves())
    with jax.named_scope("mid_2"):
        for n in (1, 3):
            stages[n][1].begin(*stages[n][0].halves())
    with jax.named_scope("mid_v"):
        stages[4][1].begin(*stages[4][0].halves())
    with jax.named_scope("mid_z"):
        end_z.begin(*mid_z.halves())
    with jax.named_scope("gt2"):
        lax.fori_loop(4, 8, grad_tokens, 0)
    gw = r.gw_out
    with jax.named_scope("finish"):
        for n in (0, 2, 1, 3, 4):
            mid, end, share, lo, hi, base = stages[n]
            gw[:, base + lo : base + hi] = end.end()
        gw[:, WA : WA + WZ] = end_z.end()
    with jax.named_scope("drain"):
        gather.end()
        for part in (share_a, share_b, share_v, ring_z, mid_z, end_z):
            part.drain()
        for mid, end, *rest in stages:
            mid.drain()
            end.drain()
        sent(dr.at[pl.ds(0, 15)], r.s_scan.at[0], mate)
        for n, l in ((0, r.ly), (1, r.lx)):
            sent(l.at[pl.ds(1, 3)], r.t_sem.at[n], mate)
        for kind in range(2):
            sent(rmsg.at[kind, pl.ds(0, 15)], r.s_scan.at[1 + kind], mate)
            sent(rres.at[kind, pl.ds(0, 15)], r.s_scan.at[3 + kind], mate)
        for copy in copies:
            copy.wait_send()


def fused(tokens, w, a_log, dt_bias, d_skip, grad_y):
    count = tokens.shape[0]
    cols, depth = w.shape
    sd = jax.ShapeDtypeStruct
    dma = pltpu.SemaphoreType.DMA
    scratch = dict(
        tok=((count, 2048), BF16), g=((count, INNER), BF16), wbuf=((8, cols, depth), BF16), acc=((count, cols), F32),
        tt=((2, 4, 4, 64, count), F32), tt3=((2, 8, 128, count), F32),
        tb=((2, 4, 4, 64, count), BF16), tb3=((2, 8, 128, count), BF16),
        tr=((4, 4, 64, count), BF16), tr3=((8, 128, count), BF16),
        t1=((4, 256, 2 * count), BF16), t2=((4, 256, 2 * count), BF16), lx=((4, 256, 2 * count), BF16), ly=((4, 256, 2 * count), BF16), t3=((8, 128, 2 * count), BF16),
        x=((count, INNER), BF16),
        dte=((count, INNER), F32), ece=((count, INNER), F32), tle=((count, INNER), F32),
        cume=((count, 2 * INNER), F32), cumt=((128, count), F32),
        xdt=((count, INNER), BF16), xt=((count, INNER), BF16), gec=((count, INNER), BF16),
        yi=((count, INNER), F32), dxi=((count, INNER), F32), ds_acc=((128, 128), F32),
        stf=((2, 2, 128, 1024), F32), sst=((2, 128, 1024), BF16), pst=((2, 128, 1024), BF16),
        tot_s=((8, 128), F32), tot_r=((8, 128), F32), te=((2, 2, 8, 1024), F32),
        dmsg=((8, 8, 128), F32), dr=((16, 8, 128), F32),
        msg=((2, 16, 64, 128), BF16), rmsg=((2, 16, 64, 128), BF16),
        res=((2, 16, 64, 128), BF16), rres=((2, 16, 64, 128), BF16),
        se=((2, 2, 128, 1024), BF16), hs=((2, 128, 1024), BF16), ske=((8, INNER), F32),
        ga=((8, count, WA), BF16), gb=((8, count, WB), BF16), gv=((8, count, WV), BF16), gz=((2, count, WZ), BF16),
        acc_a=((256, WA), F32), acc_b=((256, WB), F32), acc_v=((256, WV), F32),
        pz=((8, 128, WZ), BF16), got_z=((16, 64, WZ), BF16),
        qz=((4, 32, WZ), BF16), got_zx=((4, 32, WZ), BF16), fz_s=((4, 8, WZ), BF16), fz_g=((4, 8, WZ), BF16),
    )
    sems = dict(
        in_sem=(3,), tok_sem=(4,), g_send=(1,), g_ici=(7, 3), g_d2d=(7,), d_sem=(12,), s_scan=(5,), r_scan=(5,),
        t_sem=(4,), s_share=(4,), r_share=(3, 4, 2), d_share=(3, 4), rz=(16,), s_last=(12,), r_last=(12,),
    )

    extra = []
    for k, lo, hi in PARTS:
        extra += [pltpu.VMEM((4, 64, hi - lo), BF16)] * 2 + [pltpu.VMEM((8, 8, hi - lo), BF16)] * 2

    def body(tokens, w, a_log, dt_bias, d_skip, grad_y, y_out, gt_out, gw_out, *rest):
        r = SimpleNamespace(**dict(zip([*scratch, *sems], rest)))
        r.extra = rest[len(scratch) + len(sems) :]
        r.tokens, r.w, r.a_log, r.dt_bias, r.d_skip, r.grad_y = tokens, w, a_log, dt_bias, d_skip, grad_y
        r.y_out, r.gt_out, r.gw_out = y_out, gt_out, gw_out
        kernel(r)

    return pl.pallas_call(
        body,
        out_shape=(pltpu.VMEM((count, INNER), BF16), pltpu.VMEM((count, 2048), BF16), pltpu.VMEM((8, cols), F32)),
        in_specs=[ANY, ANY, VM, VM, VM, ANY],
        out_specs=(VM, VM, VM),
        scratch_shapes=[pltpu.VMEM(*v) for v in scratch.values()] + [dma(v) for v in sems.values()] + extra,
        compiler_params=pltpu.CompilerParams(collective_id=0, has_side_effects=True, vmem_limit_bytes=LIMIT),
    )(tokens, w, a_log.reshape(1, -1), dt_bias.reshape(1, -1), d_skip.reshape(1, -1), grad_y)


def leave_kernel(*refs):
    copies = [pltpu.make_async_copy(refs[n], refs[3 + n], refs[6].at[n]) for n in range(3)]
    for copy in copies:
        copy.start()
    for copy in copies:
        copy.wait()


def leave(*arrays):
    return pl.pallas_call(
        leave_kernel,
        out_shape=tuple(jax.ShapeDtypeStruct(a.shape, a.dtype) for a in arrays),
        in_specs=[VM] * 3,
        out_specs=(ANY,) * 3,
        scratch_shapes=[pltpu.SemaphoreType.DMA((3,))],
    )(*(pltpu.with_memory_space_constraint(a, pltpu.VMEM) for a in arrays))


def per_device(tokens, w_in, a_log, dt_bias, d_skip, grad_y):
    count, width = tokens.shape[1:]
    inner = grad_y.shape[2]
    y, gt, gw = fused(tokens.reshape(count, width), w_in.T, a_log, dt_bias, d_skip, grad_y.reshape(count, inner))
    y, gt, gw = leave(y, gt, gw)
    return (y.reshape(1, count, inner), gt.reshape(1, count, width), gw)


def solution(mesh):
    torus = Mesh(mesh.devices.reshape(2, 8, 2, 2, 4), ("xh", "z", "c", "xl", "y"))
    placed = (P(ZERO, SEQ, None), P(ZERO, None), P(), P(), P(), P(ZERO, SEQ, None))
    return jax.shard_map(
        per_device,
        mesh=torus,
        in_specs=placed,
        out_specs=(P(ZERO, SEQ, None), P(ZERO, SEQ, None), P(SEQ + ZERO, None)),
        check_vma=False,
    )
```
